32 devices in a mesh: frame: 8 (over z, core), mp: 2 (over x), dp: 2 (over y).
Axes of the slice: x: 2, y: 2, z: 4, core: 2. Of those that a mesh axis runs over, the one named last changes fastest.
Arguments:
- tokens: bfloat16 [4, 8, 160, 5120], P('dp', 'frame', None, 'mp'), may hold values from -30 to 30
- token_mask: int32 [4, 8, 160], P('dp', 'frame'), may hold values 0 or 1
- mask_embed: bfloat16 [5120], P('mp'), may hold values from -6 to 6
- w_qkv: bfloat16 [5120, 3, 3072], P('frame', None, 'mp'), may hold values from -0.078125 to 0.078125
- w_out: bfloat16 [3072, 5120], P('mp'), may hold values from -0.109375 to 0.109375
- action_idx: int32 [4, 8], P('dp', 'frame'), may hold values from 0 to 7
- codebook: float32 [8, 32], replicated, may hold values from -6 to 6
- act_proj: float32 [32, 5120], P(None, 'mp'), may hold values from -1 to 1
- cotangent: bfloat16 [4, 8, 160, 5120], P('dp', 'frame', None, 'mp'), may hold values from -6 to 6
Outputs:
- next_state: bfloat16 [4, 8, 160, 5120], P('dp', 'frame', None, 'mp')
- grad_proj: float32 [32, 5120], P(None, 'mp')
The draws below stay inside these ranges and needn't reach their ends.
All inputs are finite; a program needn't handle non-finite values. No bound on the sum of `token_mask` on one device may be relied on, other than what follows from the above.
Results may differ from the reference program's by a relative error of at most 0.0098.
Values may be sent and summed in bfloat16 or wider, within the bound.
A program may use at most 128 MiB of HBM per device.

```python
import jax
import jax.numpy as jnp
from jax import lax

D = 5120
HEADS = 24
HS = 128
CODES = 8
D_ACT = 32
P_SIZE = 160
CLIPS = 4
FRAMES = 8


def draw_tokens(key, part):
    shape = (CLIPS, FRAMES, P_SIZE, D)
    return jax.random.truncated_normal(key, -6.0, 6.0, shape, jnp.float32).astype(jnp.bfloat16)


def touch_ends(result, rng, low, largest):
    longest = result.shape.index(max(result.shape))
    spots = []
    for shift in (0, 1):
        where = [jax.random.randint(jax.random.fold_in(rng, axis), (), 0, length) for axis, length in enumerate(result.shape)]
        where[longest] = (where[longest] + shift) % result.shape[longest]
        spots.append(tuple(where))
    return result.at[spots[0]].set(low).at[spots[1]].set(largest)


def block_scale(key, shape, cuts, smallest, high):
    factor_of, own = 1.0, jax.random.fold_in(key, 6)
    for axis_at, parts in cuts:
        heights = jnp.exp(jax.random.uniform(jax.random.fold_in(own, axis_at), (parts,), jnp.float32, smallest / len(cuts), high / len(cuts)))
        factor_of = factor_of * jnp.repeat(heights, shape[axis_at] // parts).reshape([-1 if axis == axis_at else 1 for axis in range(len(shape))])
    return factor_of


def centred(key, dims, scale, bound, cuts=(), dtype=jnp.bfloat16):
    factor_of = block_scale(key, dims, cuts, -0.22, 0.18) if cuts else 1.0
    array = jax.random.normal(key, dims, jnp.float32) * scale * factor_of
    return jnp.minimum(jnp.maximum(array, -bound), bound).astype(dtype)


def setup_inputs(seed: int = 0) -> dict:
    splits = jax.random.split(jax.random.key(seed), 10)
    tokens = draw_tokens(jax.random.fold_in(splits[9], 71), 0)
    token_mask = touch_ends((jax.random.randint(splits[1], (CLIPS, FRAMES, P_SIZE), 0, 2) < 1).astype(jnp.int32), jax.random.fold_in(splits[1], 1), 0, 1)
    mask_embed = centred(splits[2], (D,), 1.0, 6.0, ((0, 2),))
    w_qkv = centred(splits[3], (D, 3, HEADS * HS), D ** -0.5, 0.078125, ((0, 8), (2, 2)))
    w_out = centred(splits[4], (HEADS * HS, D), (HEADS * HS) ** -0.5, 0.109375, ((0, 2),))
    action_idx = touch_ends(jax.random.randint(splits[5], (CLIPS, FRAMES), 0, CODES), jax.random.fold_in(splits[5], 1), 0, CODES - 1).astype(jnp.int32)
    codebook = centred(splits[6], (CODES, D_ACT), 1.0, 6.0, (), jnp.float32)
    act_proj = centred(splits[7], (D_ACT, D), D_ACT ** -0.5, 1.0, ((1, 2),), jnp.float32)
    cotangent = centred(splits[8], (CLIPS, FRAMES, P_SIZE, D), 1.0, 6.0, ((0, 2), (1, 8), (3, 2)))
    return dict(tokens=tokens, token_mask=token_mask, mask_embed=mask_embed, w_qkv=w_qkv, w_out=w_out, action_idx=action_idx, codebook=codebook, act_proj=act_proj, cotangent=cotangent)


def reference(tokens, token_mask, mask_embed, w_qkv, w_out, action_idx, codebook, act_proj, cotangent):
    xin = jnp.where(token_mask[..., None] == 1, mask_embed, tokens)
    width_heads = HEADS * HS
    flat = xin.reshape(-1, D)
    qkv = jnp.dot(flat, w_qkv.reshape(D, 3 * width_heads), preferred_element_type=jnp.float32).astype(jnp.bfloat16)
    qkv = qkv.reshape(CLIPS, FRAMES, P_SIZE, 3, HEADS, HS)
    query = qkv[:, :, :, 0].astype(jnp.float32)
    keys = qkv[:, :, :, 1].astype(jnp.float32)
    values = qkv[:, :, :, 2].astype(jnp.float32)
    scores = jnp.einsum('cfphd,cuphd->cfphu', query, keys, precision=lax.Precision.HIGHEST) / jnp.sqrt(jnp.float32(HS))
    causal = (jnp.arange(FRAMES)[:, None] >= jnp.arange(FRAMES)[None, :])[None, :, None, None, :]
    peak = lax.optimization_barrier(jnp.max(jnp.where(causal, scores, -jnp.inf), axis=-1))
    weights = jnp.where(causal, jnp.exp(scores - peak[..., None]), 0.0)
    total = lax.optimization_barrier(jnp.sum(weights, axis=-1))
    accum = jnp.einsum('cfphu,cuphd->cfphd', weights, values, precision=lax.Precision.HIGHEST)
    attn = (accum / total[..., None]).astype(jnp.bfloat16).reshape(-1, width_heads)
    mixed = jnp.dot(attn, w_out, preferred_element_type=jnp.float32).reshape(CLIPS, FRAMES, P_SIZE, D)
    codevec = codebook[action_idx].reshape(-1, D_ACT)
    gate = jnp.dot(codevec, act_proj, precision=lax.Precision.HIGHEST).reshape(CLIPS, FRAMES, 1, D)
    next_state = (xin.astype(jnp.float32) + gate * mixed).astype(jnp.bfloat16)
    dgate = lax.optimization_barrier(jnp.sum(cotangent.astype(jnp.float32) * mixed, axis=2)).reshape(-1, D)
    grad_proj = jnp.dot(codevec.T, dgate, precision=lax.Precision.HIGHEST)
    return (next_state, grad_proj)
```

```python
import functools
import math

import jax
import jax.numpy as jnp
from jax import lax
from jax.experimental import pallas as pl
from jax.experimental.pallas import tpu as pltpu
from jax.sharding import PartitionSpec as P

HS = 128


def attend_kernel(frames, q_ref, k_ref, v_ref, o_ref):
    scale = 1.0 / math.sqrt(HS)
    for t in range(frames):
        q = q_ref[t].astype(jnp.float32) * scale
        scores = [
            jnp.sum(q * k_ref[u].astype(jnp.float32), axis=-1, keepdims=True) for u in range(t + 1)
        ]
        peak = functools.reduce(jnp.maximum, scores)
        weights = [jnp.exp(s - peak) for s in scores]
        total = functools.reduce(jnp.add, weights)
        accum = functools.reduce(
            jnp.add, [w * v_ref[u].astype(jnp.float32) for u, w in enumerate(weights)]
        )
        o_ref[t] = (accum / total).astype(o_ref.dtype)


def attend(qkv, frames, heads_width):
    rows = qkv.shape[1]
    heads = heads_width // HS
    spec = lambda part: pl.BlockSpec((frames, rows, HS), lambda h, part=part: (0, 0, part * heads + h))
    return pl.pallas_call(
        functools.partial(attend_kernel, frames),
        grid=(heads,),
        in_specs=[spec(0), spec(1), spec(2)],
        out_specs=spec(0),
        out_shape=jax.ShapeDtypeStruct((frames, rows, heads_width), jnp.bfloat16),
        cost_estimate=pl.CostEstimate(flops=4 * frames * frames * rows * heads_width,
                                      bytes_accessed=8 * frames * rows * heads_width,
                                      transcendentals=0),
        name="attend",
    )(qkv, qkv, qkv)


def spread_kernel(frames, dps, x_ref, o_ref, send_sem, recv_sem, own_sem):
    count = frames * dps
    me = lax.axis_index("frame") * dps + lax.axis_index("dp")
    barrier = pltpu.get_barrier_semaphore()

    def peer(shift):
        other = lax.rem(me + shift, count)
        return {"frame": other // dps, "dp": lax.rem(other, dps)}

    for shift in range(1, count):
        pl.semaphore_signal(barrier, inc=1, device_id=peer(shift),
                            device_id_type=pl.DeviceIdType.MESH)
    own = pltpu.make_async_copy(x_ref, o_ref.at[me], own_sem)
    own.start()
    pl.semaphore_wait(barrier, count - 1)
    copies = []
    for shift in range(1, count):
        copy = pltpu.make_async_remote_copy(
            src_ref=x_ref, dst_ref=o_ref.at[me], send_sem=send_sem.at[shift],
            recv_sem=recv_sem.at[shift], device_id=peer(shift),
            device_id_type=pl.DeviceIdType.MESH)
        copy.start()
        copies.append(copy)
    own.wait()
    for copy in copies:
        copy.wait()


def spread_terms(terms, frames, dps):
    count = frames * dps
    return pl.pallas_call(
        functools.partial(spread_kernel, frames, dps),
        in_specs=[pl.BlockSpec(memory_space=pltpu.VMEM)],
        out_specs=pl.BlockSpec(memory_space=pltpu.VMEM),
        out_shape=jax.ShapeDtypeStruct((count, *terms.shape), terms.dtype),
        scratch_shapes=[pltpu.SemaphoreType.DMA((count,)), pltpu.SemaphoreType.DMA((count,)),
                        pltpu.SemaphoreType.DMA],
        compiler_params=pltpu.CompilerParams(collective_id=1, has_side_effects=True),
        name="spread_terms",
    )(terms)


def fused_kernel(x_ref, w_ref, o_ref, attn_ref, wo_ref, xbuf, wbuf, acc, qkv, abuf, x_recv,
                 x_send, w_recv, w_send, o_recv, o_send, a_recv, a_send, e_recv, e_send, own_sem):
    mps, frames, spots, width = xbuf.shape
    per_group, _, _, _ = wbuf.shape
    depth = w_ref.shape[1]
    lines = frames // 2
    half = lines // 2
    part = depth // 2
    quarter = o_ref.shape[0] // 4
    f, m, d = lax.axis_index("frame"), lax.axis_index("mp"), lax.axis_index("dp")
    z, c = f // 2, f % 2
    hi, lo = z // 2, z % 2
    mine = hi * 2 + c
    inner = hi != lo
    pair, near, far = z + 1 - 2 * lo, half - hi, (lines - 1) * (1 - hi)
    other_core = 2 * z + 1 - c

    def remote(source, target, send_sem, recv_sem, frame=f, mp=m, dp=d):
        return pltpu.make_async_remote_copy(
            src_ref=source, dst_ref=target, send_sem=send_sem, recv_sem=recv_sem,
            device_id={"frame": frame, "mp": mp, "dp": dp},
            device_id_type=pl.DeviceIdType.MESH)

    def arrived(target, recv_sem):
        pltpu.make_async_copy(target, target, recv_sem).wait()

    def rows_of(owner, which):
        return pl.ds(pl.multiple_of(owner * depth + which * part, part), part)

    def whole_rows(owner):
        return pl.ds(pl.multiple_of(owner * depth, depth), depth)

    def columns(group, head):
        return pl.ds(pl.multiple_of((group * per_group + head) * HS, HS), HS)

    def line(j):
        return jnp.where(j == 0, pair, jnp.where(j == 1, near, far))

    def source_of(j):
        return 2 * line(j // 2) + j % 2

    def w_direct(h, k):
        target = jnp.where(k < 2, pair, near)
        group = jnp.where(k < 2, hi, 1 - hi) * 2 + k % 2
        return remote(w_ref.at[:, pl.ds(pl.multiple_of(d * part, part), part), columns(group, h)],
                      wbuf.at[h, :, rows_of(f, d), :], w_send.at[h, k], w_recv.at[h, f, d],
                      frame=2 * target + k % 2)

    def w_partner(h):
        return remote(w_ref.at[:, :, columns(hi * 2 + 1 - c, h)], wbuf.at[h, :, whole_rows(f), :],
                      w_send.at[h, 4], w_recv.at[h, f, 0], frame=other_core)

    def w_own(h):
        return pltpu.make_async_copy(w_ref.at[:, :, columns(mine, h)],
                                     wbuf.at[h, :, whole_rows(f), :], own_sem.at[h])

    def w_block(h, owner, which):
        return wbuf.at[h, :, rows_of(owner, which), :]

    def w_share(h, j):
        owner = source_of(j)
        block = w_block(h, owner, d)
        return remote(block, block, w_send.at[h, 5 + j], w_recv.at[h, owner, d], dp=1 - d)

    def w_relay(h, j):
        owner = source_of(j)
        block = w_block(h, owner, d)
        return remote(block, block, w_send.at[h, 9 + j], w_recv.at[h, owner, d],
                      frame=2 * pair + c)

    def forward_w(h, j):
        owner = source_of(j)
        arrived(w_block(h, owner, d), w_recv.at[h, owner, d])

        @pl.when(jnp.logical_and(inner, j >= 2))
        def _():
            w_relay(h, j).start()

        w_share(h, j).start()

    def x_direct(k):
        target = (z + k) % lines
        return remote(x_ref.at[target % 2], xbuf.at[m, f], x_send.at[k], x_recv.at[m, f],
                      frame=2 * target + c)

    def x_across(owner, source, k):
        return remote(source, xbuf.at[m, owner], x_send.at[4 + k], x_recv.at[m, owner],
                      mp=1 - m)

    def x_core(owner, source, which, k, slot):
        return remote(source, xbuf.at[which, owner], x_send.at[slot + k], x_recv.at[which, owner],
                      frame=other_core)

    def x_owner(k):
        return f if k == 0 else 2 * line(k - 1) + c

    def o_rows(which):
        return pl.ds(pl.multiple_of(which * quarter, quarter), quarter)

    def attn_block(which, owner, h):
        group = (owner // 4) * 2 + owner % 2
        clip = (owner // 2) % 2
        return attn_ref.at[which, pl.ds(pl.multiple_of(clip * spots, spots), spots),
                           columns(group, h)]

    def a_direct(h, k):
        target = (f + k) % frames
        return remote(abuf.at[h, target], attn_block(m, f, h), a_send.at[h, k], a_recv.at[h, f],
                      frame=target)

    def a_own(h):
        return pltpu.make_async_copy(abuf.at[h, f], attn_block(m, f, h), a_recv.at[h, f])

    def a_across(h, k):
        owner = (f + k) % frames
        block = attn_block(m, owner, h)
        return remote(block, block, e_send.at[h, k], e_recv.at[h, owner], mp=1 - m)

    def forward_attn(h):
        @pl.loop(0, frames)
        def _(k):
            owner = (f + k) % frames
            arrived(attn_block(m, owner, h), a_recv.at[h, owner])
            a_across(h, k).start()

    barrier = pltpu.get_barrier_semaphore()
    for k in range(1, frames):
        pl.semaphore_signal(barrier, inc=1, device_id={"frame": (f + k) % frames, "mp": m, "dp": d},
                            device_id_type=pl.DeviceIdType.MESH)
    pl.semaphore_signal(barrier, inc=1, device_id={"frame": f, "mp": 1 - m, "dp": d},
                        device_id_type=pl.DeviceIdType.MESH)
    pl.semaphore_signal(barrier, inc=1, device_id={"frame": f, "mp": m, "dp": 1 - d},
                        device_id_type=pl.DeviceIdType.MESH)
    own_x = pltpu.make_async_copy(x_ref.at[lo], xbuf.at[m, f], own_sem.at[per_group])
    own_x.start()
    for h in range(per_group):
        w_own(h).start()
    pl.semaphore_wait(barrier, frames + 1)

    for k in range(4):
        w_direct(0, k).start()
    for k in range(1, lines):
        x_direct(k).start()
    q0, q1 = d * 2 + c, (1 - d) * 2 + c
    o_across = remote(o_ref.at[o_rows(q0), pl.ds(pl.multiple_of((1 - m) * width, width), width)],
                      wo_ref.at[o_rows(q0), :], o_send.at[0], o_recv.at[q0], mp=1 - m)
    x_across(f, x_ref.at[lo], 0).start()
    x_core(f, x_ref.at[lo], m, 0, 8).start()
    o_across.start()
    for h in range(per_group):
        w_partner(h).start()

    @pl.loop(0, 6)
    def _(j):
        forward_w(0, j)

    for k in range(4):
        w_direct(1, k).start()

    o_q0 = wo_ref.at[o_rows(q0), :]
    o_q1 = wo_ref.at[o_rows(q1), :]
    o_share = remote(o_q0, o_q0, o_send.at[1], o_recv.at[q0], dp=1 - d)
    o_core0 = remote(o_q0, o_q0, o_send.at[2], o_recv.at[q0], frame=other_core)
    o_core1 = remote(o_q1, o_q1, o_send.at[3], o_recv.at[q1], frame=other_core)

    for k in range(1, lines + 1):
        if k < lines:
            owner = x_owner(k)
            block = xbuf.at[m, owner]
            arrived(block, x_recv.at[m, owner])
            x_across(owner, block, k).start()
            x_core(owner, block, m, k, 8).start()
        if k == 1:
            arrived(o_q0, o_recv.at[q0])
            o_share.start()
            o_core0.start()
        before = x_owner(k - 1)
        block = xbuf.at[1 - m, before]
        arrived(block, x_recv.at[1 - m, before])
        x_core(before, block, 1 - m, k - 1, 12).start()
    for h in range(2, per_group):
        for k in range(4):
            w_direct(h, k).start()
    own_x.wait()
    for k in range(lines):
        owner = x_owner(k) + 1 - 2 * c
        for which in range(mps):
            arrived(xbuf.at[which, owner], x_recv.at[which, owner])

    chunks = frames
    marks = []
    for h in range(1, per_group):
        begin = h * chunks
        ahead = h == 1 and per_group > 2
        marks += [begin + at for at in ((-8, -4, 0, 2, 4, 6) if ahead else (0, 2, 3, 4, 5, 6))]
    finals = per_group * chunks

    def matmul(h, owner, first):
        side = owner // (frames // mps)
        col = pl.multiple_of((owner % (frames // mps)) * depth, depth)
        w = jnp.concatenate([wbuf[h, p, whole_rows(owner), :] for p in range(3)], axis=1)
        step = frames // 2

        @pl.loop(0, 2)
        def _(i):
            x = xbuf[side, pl.ds(i * step, step), :, pl.ds(col, depth)].reshape(step * spots, depth)
            y = jnp.dot(x, w, preferred_element_type=jnp.float32).reshape(step, spots, 3 * HS)

            @pl.when(first)
            def _():
                acc[pl.ds(i * step, step)] = y

            @pl.when(jnp.logical_not(first))
            def _():
                acc[pl.ds(i * step, step)] += y

    def attention(h):
        scale = 1.0 / math.sqrt(HS)

        @pl.loop(0, frames)
        def _(t):
            for p in range(3):
                qkv[p, t] = acc[t, :, p * HS:(p + 1) * HS].astype(qkv.dtype)

        rows = math.gcd(spots, 32)

        @pl.loop(0, spots // rows)
        def _(i):
            at = pl.ds(pl.multiple_of(i * rows, rows), rows)
            for t in range(frames):
                q = qkv[0, t, at, :].astype(jnp.float32) * scale
                scores = [jnp.sum(q * qkv[1, u, at, :].astype(jnp.float32), axis=-1, keepdims=True)
                          for u in range(t + 1)]
                peak = functools.reduce(jnp.maximum, scores)
                weights = [jnp.exp(s - peak) for s in scores]
                total = functools.reduce(jnp.add, weights)
                accum = functools.reduce(
                    jnp.add,
                    [w * qkv[2, u, at, :].astype(jnp.float32) for u, w in enumerate(weights)])
                abuf[h, t, at, :] = (accum / total).astype(abuf.dtype)

        a_own(h).start()

        @pl.loop(1, frames)
        def _(k):
            a_direct(h, k).start()

    @pl.loop(0, finals)
    def _(i):
        h, jj = i // chunks, i % chunks
        event = functools.reduce(jnp.add, [jnp.where(i > mark, 1, 0) for mark in marks])
        fires = functools.reduce(jnp.logical_or, [i == mark for mark in marks])

        @pl.when(fires)
        def _():
            forward_w(1 + event // 6, event % 6)

        @pl.when(i == 6)
        def _():
            arrived(o_q1, o_recv.at[q1])
            o_core1.start()

        owner = jnp.where(jj == 0, f, jnp.where(jj == 1, other_core, source_of(jnp.maximum(jj - 2, 0))))

        @pl.when(jj == 0)
        def _():
            w_own(h).wait()

        @pl.when(jj == 1)
        def _():
            arrived(wbuf.at[h, :, whole_rows(owner), :], w_recv.at[h, owner, 0])

        @pl.when(jj >= 2)
        def _():
            arrived(w_block(h, owner, 1 - d), w_recv.at[h, owner, 1 - d])

        matmul(h, owner, jj == 0)

        for ready in range(per_group - 1):
            @pl.when(i == (ready + 1) * chunks + 5)
            def _():
                forward_attn(ready)

        @pl.when(jj == chunks - 1)
        def _():
            attention(h)

    forward_attn(per_group - 1)
    for which in (d * 2 + 1 - c, (1 - d) * 2 + 1 - c):
        arrived(wo_ref.at[o_rows(which), :], o_recv.at[which])
    for copy in (o_across, o_share, o_core0, o_core1):
        copy.wait_send()
    for k in range(1, lines):
        x_direct(k).wait_send()
    for k in range(lines):
        owner = x_owner(k)
        block = xbuf.at[m, owner]
        x_across(owner, block, k).wait_send()
        x_core(owner, block, m, k, 8).wait_send()
        x_core(owner, xbuf.at[1 - m, owner], 1 - m, k, 12).wait_send()

    @pl.loop(0, per_group)
    def _(h):
        for k in range(4):
            w_direct(h, k).wait_send()
        w_partner(h).wait_send()
        for j in range(6):
            w_share(h, j).wait_send()

        @pl.when(inner)
        def _():
            for j in range(2, 6):
                w_relay(h, j).wait_send()

        @pl.loop(1, frames)
        def _(k):
            a_direct(h, k).wait_send()

        @pl.loop(0, frames)
        def _(k):
            a_across(h, k).wait_send()
            owner = (f + k) % frames
            arrived(attn_block(1 - m, owner, h), e_recv.at[h, owner])


def fused(xin, w_parts, w_out, frames):
    clips, spots, width = xin.shape
    parts, depth, heads_width = w_parts.shape
    groups = frames // clips
    per_group = heads_width // HS // groups
    lines = frames // 2
    any_spec = pl.BlockSpec(memory_space=pl.ANY)
    dma = pltpu.SemaphoreType.DMA
    return pl.pallas_call(
        fused_kernel,
        in_specs=[any_spec] * 3,
        out_specs=[any_spec] * 2,
        out_shape=[
            jax.ShapeDtypeStruct((2, clips * spots, heads_width), jnp.bfloat16),
            jax.ShapeDtypeStruct((w_out.shape[0], width), jnp.bfloat16),
        ],
        scratch_shapes=[
            pltpu.VMEM((2, frames, spots, width), jnp.bfloat16),
            pltpu.VMEM((per_group, parts, depth * frames, HS), jnp.bfloat16),
            pltpu.VMEM((frames, spots, parts * HS), jnp.float32),
            pltpu.VMEM((parts, frames, spots, HS), jnp.bfloat16),
            pltpu.VMEM((per_group, frames, spots, HS), jnp.bfloat16),
            dma((2, frames)), dma((16,)),
            dma((per_group, frames, 2)), dma((per_group, 15)),
            dma((4,)), dma((4,)),
            dma((per_group, frames)), dma((per_group, frames)),
            dma((per_group, frames)), dma((per_group, frames)),
            dma((per_group + 1,)),
        ],
        compiler_params=pltpu.CompilerParams(
            collective_id=2, has_side_effects=True, vmem_limit_bytes=60 << 20),
        name="fused",
    )(xin, w_parts, w_out)


def gather_mp(block, size):
    if size != 2:
        return lax.all_gather(block, "mp", axis=block.ndim - 1, tiled=True)
    other = lax.ppermute(block, "mp", [(0, 1), (1, 0)])
    first = lax.axis_index("mp") == 0
    return jnp.concatenate(
        [jnp.where(first, block, other), jnp.where(first, other, block)], axis=-1
    )


def fits_fused(mps, dps, frames, clips, spots, depth, heads_width):
    groups = frames // clips
    return (mps == dps == clips == 2 and frames == groups * clips and groups == 2 * clips
            and heads_width % (groups * HS) == 0 and heads_width // HS // groups > 1
            and spots % 32 == 0 and depth % HS == 0)


def body(mp_size, dp_size, tokens, token_mask, mask_embed, w_qkv, w_out, action_idx, codebook,
         act_proj, cotangent):
    clips, _, spots, width = tokens.shape
    heads_width = w_qkv.shape[2]
    depth = w_qkv.shape[0]
    xin = jnp.where(token_mask[..., None] == 1, mask_embed, tokens)
    frames = lax.axis_size("frame")
    if fits_fused(mp_size, dp_size, frames, clips, spots, depth, heads_width):
        my_mp = lax.axis_index("mp")
        heads, out_other = fused(xin.reshape(clips, spots, width), w_qkv.transpose(1, 0, 2), w_out, frames)
        out_mine = lax.dynamic_slice_in_dim(w_out, my_mp * width, width, axis=1)
        own = lax.dynamic_index_in_dim(heads, my_mp, 0, keepdims=False)
        other = lax.dynamic_index_in_dim(heads, 1 - my_mp, 0, keepdims=False)
        mixed_rows = jnp.dot(own, out_mine, preferred_element_type=jnp.float32) + jnp.dot(
            other, out_other, preferred_element_type=jnp.float32)
    else:
        share = depth // dp_size
        mine = lax.dynamic_slice_in_dim(
            w_qkv.reshape(depth, 3 * heads_width), lax.axis_index("dp") * share, share, axis=0
        )
        weights = lax.all_gather(mine, ("frame", "dp"), axis=0, tiled=True)
        if mp_size == 2:
            my_mp = lax.axis_index("mp")
            out_mine = lax.dynamic_slice_in_dim(w_out, my_mp * width, width, axis=1)
            out_other = lax.ppermute(
                lax.dynamic_slice_in_dim(w_out, (1 - my_mp) * width, width, axis=1),
                "mp", [(0, 1), (1, 0)])
        spread = lax.all_to_all(
            xin.reshape(clips, spots, width), "frame", split_axis=1, concat_axis=0, tiled=True
        )
        frames = spread.shape[0] // clips
        local = spread.shape[1]
        features = gather_mp(spread.reshape(frames * clips * local, width), mp_size)
        qkv = jnp.dot(features, weights, preferred_element_type=jnp.float32).astype(jnp.bfloat16)
        attn = attend(qkv.reshape(frames, clips * local, 3 * heads_width), frames, heads_width)
        back = lax.all_to_all(
            attn.reshape(frames * clips, local, heads_width), "frame", split_axis=0, concat_axis=1,
            tiled=True,
        )
        heads = back.reshape(clips * spots, heads_width)
        if mp_size == 2:
            other_heads = lax.ppermute(heads, "mp", [(0, 1), (1, 0)])
            mixed_rows = jnp.dot(heads, out_mine, preferred_element_type=jnp.float32) + jnp.dot(
                other_heads, out_other, preferred_element_type=jnp.float32)
        else:
            out_block = lax.all_to_all(w_out, "mp", split_axis=1, concat_axis=0, tiled=True)
            mixed_rows = jnp.dot(gather_mp(heads, mp_size), out_block,
                                 preferred_element_type=jnp.float32)
    mixed = mixed_rows.reshape(clips, 1, spots, width)
    onehot = (
        action_idx.reshape(clips)[:, None] == jnp.arange(codebook.shape[0])[None, :]
    ).astype(jnp.float32)
    codevec = jnp.dot(onehot, codebook, precision=lax.Precision.HIGHEST)
    gate = jnp.dot(codevec, act_proj, precision=lax.Precision.HIGHEST)
    next_state = (xin.astype(jnp.float32) + gate[:, None, None, :] * mixed).astype(jnp.bfloat16)
    dgate = jnp.sum(cotangent.astype(jnp.float32) * mixed, axis=2).reshape(clips, width)
    codes = codevec.shape[1]
    padded = jnp.pad(codevec, ((0, 0), (0, -codes % 128)))
    terms = spread_terms(jnp.concatenate([dgate, padded], axis=1), frames, dp_size)
    terms = terms.reshape(frames * dp_size * clips, -1)
    grad_proj = jnp.dot(
        terms[:, width : width + codes].T, terms[:, :width], precision=lax.Precision.HIGHEST)
    return (next_state, grad_proj)


def solution(mesh):
    in_specs = (
        P("dp", "frame", None, "mp"),
        P("dp", "frame", None),
        P("mp"),
        P("frame", None, "mp"),
        P("mp", None),
        P("dp", "frame"),
        P(),
        P(None, "mp"),
        P("dp", "frame", None, "mp"),
    )
    out_specs = (P("dp", "frame", None, "mp"), P(None, "mp"))
    return jax.shard_map(
        functools.partial(body, mesh.shape["mp"], mesh.shape["dp"]),
        mesh=mesh, in_specs=in_specs, out_specs=out_specs, check_vma=False,
    )
```

```python
import functools
import math

import jax
import jax.numpy as jnp
from jax import lax
from jax.experimental import pallas as pl
from jax.experimental.pallas import tpu as pltpu
from jax.sharding import PartitionSpec as P

HS = 128


def attend_kernel(frames, q_ref, k_ref, v_ref, o_ref):
    scale = 1.0 / math.sqrt(HS)
    for t in range(frames):
        q = q_ref[t].astype(jnp.float32) * scale
        scores = [
            jnp.sum(q * k_ref[u].astype(jnp.float32), axis=-1, keepdims=True) for u in range(t + 1)
        ]
        peak = functools.reduce(jnp.maximum, scores)
        weights = [jnp.exp(s - peak) for s in scores]
        total = functools.reduce(jnp.add, weights)
        accum = functools.reduce(
            jnp.add, [w * v_ref[u].astype(jnp.float32) for u, w in enumerate(weights)]
        )
        o_ref[t] = (accum / total).astype(o_ref.dtype)


def attend(qkv, frames, heads_width):
    rows = qkv.shape[1]
    heads = heads_width // HS
    spec = lambda part: pl.BlockSpec((frames, rows, HS), lambda h, part=part: (0, 0, part * heads + h))
    return pl.pallas_call(
        functools.partial(attend_kernel, frames),
        grid=(heads,),
        in_specs=[spec(0), spec(1), spec(2)],
        out_specs=spec(0),
        out_shape=jax.ShapeDtypeStruct((frames, rows, heads_width), jnp.bfloat16),
        cost_estimate=pl.CostEstimate(flops=4 * frames * frames * rows * heads_width,
                                      bytes_accessed=8 * frames * rows * heads_width,
                                      transcendentals=0),
        name="attend",
    )(qkv, qkv, qkv)


def spread_kernel(frames, dps, x_ref, o_ref, send_sem, recv_sem, own_sem):
    count = frames * dps
    me = lax.axis_index("frame") * dps + lax.axis_index("dp")
    barrier = pltpu.get_barrier_semaphore()

    def peer(shift):
        other = lax.rem(me + shift, count)
        return {"frame": other // dps, "dp": lax.rem(other, dps)}

    for shift in range(1, count):
        pl.semaphore_signal(barrier, inc=1, device_id=peer(shift),
                            device_id_type=pl.DeviceIdType.MESH)
    own = pltpu.make_async_copy(x_ref, o_ref.at[me], own_sem)
    own.start()
    pl.semaphore_wait(barrier, count - 1)
    copies = []
    for shift in range(1, count):
        copy = pltpu.make_async_remote_copy(
            src_ref=x_ref, dst_ref=o_ref.at[me], send_sem=send_sem.at[shift],
            recv_sem=recv_sem.at[shift], device_id=peer(shift),
            device_id_type=pl.DeviceIdType.MESH)
        copy.start()
        copies.append(copy)
    own.wait()
    for copy in copies:
        copy.wait()


def spread_terms(terms, frames, dps):
    count = frames * dps
    return pl.pallas_call(
        functools.partial(spread_kernel, frames, dps),
        in_specs=[pl.BlockSpec(memory_space=pltpu.VMEM)],
        out_specs=pl.BlockSpec(memory_space=pltpu.VMEM),
        out_shape=jax.ShapeDtypeStruct((count, *terms.shape), terms.dtype),
        scratch_shapes=[pltpu.SemaphoreType.DMA((count,)), pltpu.SemaphoreType.DMA((count,)),
                        pltpu.SemaphoreType.DMA],
        compiler_params=pltpu.CompilerParams(collective_id=1, has_side_effects=True),
        name="spread_terms",
    )(terms)


def fused_kernel(x_ref, w_ref, o_ref, attn_ref, wo_ref, xbuf, wbuf, acc, qkv, abuf, x_recv,
                 x_send, w_recv, w_send, o_recv, o_send, a_recv, a_send, e_recv, e_send, own_sem):
    mps, frames, spots, width = xbuf.shape
    per_group, _, _, _ = wbuf.shape
    depth = w_ref.shape[1]
    lines = frames // 2
    half = lines // 2
    part = depth // 2
    quarter = o_ref.shape[0] // 4
    f, m, d = lax.axis_index("frame"), lax.axis_index("mp"), lax.axis_index("dp")
    z, c = f // 2, f % 2
    hi, lo = z // 2, z % 2
    mine = hi * 2 + c
    inner = hi != lo
    pair, near, far = z + 1 - 2 * lo, half - hi, (lines - 1) * (1 - hi)
    other_core = 2 * z + 1 - c

    def remote(source, target, send_sem, recv_sem, frame=f, mp=m, dp=d):
        return pltpu.make_async_remote_copy(
            src_ref=source, dst_ref=target, send_sem=send_sem, recv_sem=recv_sem,
            device_id={"frame": frame, "mp": mp, "dp": dp},
            device_id_type=pl.DeviceIdType.MESH)

    def arrived(target, recv_sem):
        pltpu.make_async_copy(target, target, recv_sem).wait()

    def rows_of(owner, which):
        return pl.ds(pl.multiple_of(owner * depth + which * part, part), part)

    def whole_rows(owner):
        return pl.ds(pl.multiple_of(owner * depth, depth), depth)

    def columns(group, head):
        return pl.ds(pl.multiple_of((group * per_group + head) * HS, HS), HS)

    def line(j):
        return jnp.where(j == 0, pair, jnp.where(j == 1, near, far))

    def source_of(j):
        return 2 * line(j // 2) + j % 2

    def w_direct(h, k):
        target = jnp.where(k < 2, pair, near)
        group = jnp.where(k < 2, hi, 1 - hi) * 2 + k % 2
        return remote(w_ref.at[:, pl.ds(pl.multiple_of(d * part, part), part), columns(group, h)],
                      wbuf.at[h, :, rows_of(f, d), :], w_send.at[h, k], w_recv.at[h, f, d],
                      frame=2 * target + k % 2)

    def w_partner(h):
        return remote(w_ref.at[:, :, columns(hi * 2 + 1 - c, h)], wbuf.at[h, :, whole_rows(f), :],
                      w_send.at[h, 4], w_recv.at[h, f, 0], frame=other_core)

    def w_own(h):
        return pltpu.make_async_copy(w_ref.at[:, :, columns(mine, h)],
                                     wbuf.at[h, :, whole_rows(f), :], own_sem.at[h])

    def w_block(h, owner, which):
        return wbuf.at[h, :, rows_of(owner, which), :]

    def w_share(h, j):
        owner = source_of(j)
        block = w_block(h, owner, d)
        return remote(block, block, w_send.at[h, 5 + j], w_recv.at[h, owner, d], dp=1 - d)

    def w_relay(h, j):
        owner = source_of(j)
        block = w_block(h, owner, d)
        return remote(block, block, w_send.at[h, 9 + j], w_recv.at[h, owner, d],
                      frame=2 * pair + c)

    def forward_w(h, j):
        owner = source_of(j)
        arrived(w_block(h, owner, d), w_recv.at[h, owner, d])

        @pl.when(jnp.logical_and(inner, j >= 2))
        def _():
            w_relay(h, j).start()

        w_share(h, j).start()

    pieces = frames // mps

    def features(q):
        return pl.ds(pl.multiple_of(q * depth, depth), depth)

    def x_piece(which, owner, q):
        return xbuf.at[which, owner, :, features(q)]

    def x_direct(k, q):
        target = (z + k) % lines
        return remote(x_ref.at[target % 2, :, features(q)], x_piece(m, f, q), x_send.at[k, q],
                      x_recv.at[m, f, q], frame=2 * target + c)

    def x_across(owner, source, k, q):
        return remote(source, x_piece(m, owner, q), x_send.at[4 + k, q], x_recv.at[m, owner, q],
                      mp=1 - m)

    def x_core(owner, source, which, k, q):
        slot = jnp.where(which == m, 8, 12)
        return remote(source, x_piece(which, owner, q), x_send.at[slot + k, q],
                      x_recv.at[which, owner, q], frame=other_core)

    def x_own(q):
        return x_ref.at[lo, :, features(q)]

    def x_owner(k):
        return f if k == 0 else 2 * line(k - 1) + c

    def o_rows(which):
        return pl.ds(pl.multiple_of(which * quarter, quarter), quarter)

    def attn_block(which, owner, h):
        group = (owner // 4) * 2 + owner % 2
        clip = (owner // 2) % 2
        return attn_ref.at[which, pl.ds(pl.multiple_of(clip * spots, spots), spots),
                           columns(group, h)]

    def a_direct(h, k):
        target = (f + k) % frames
        return remote(abuf.at[h, target], attn_block(m, f, h), a_send.at[h, k], a_recv.at[h, f],
                      frame=target)

    def a_own(h):
        return pltpu.make_async_copy(abuf.at[h, f], attn_block(m, f, h), a_recv.at[h, f])

    def a_across(h, k):
        owner = (f + k) % frames
        block = attn_block(m, owner, h)
        return remote(block, block, e_send.at[h, k], e_recv.at[h, owner], mp=1 - m)

    def forward_attn(h):
        @pl.loop(0, frames)
        def _(k):
            owner = (f + k) % frames
            arrived(attn_block(m, owner, h), a_recv.at[h, owner])
            a_across(h, k).start()

    barrier = pltpu.get_barrier_semaphore()
    for k in range(1, frames):
        pl.semaphore_signal(barrier, inc=1, device_id={"frame": (f + k) % frames, "mp": m, "dp": d},
                            device_id_type=pl.DeviceIdType.MESH)
    pl.semaphore_signal(barrier, inc=1, device_id={"frame": f, "mp": 1 - m, "dp": d},
                        device_id_type=pl.DeviceIdType.MESH)
    pl.semaphore_signal(barrier, inc=1, device_id={"frame": f, "mp": m, "dp": 1 - d},
                        device_id_type=pl.DeviceIdType.MESH)
    own_x = pltpu.make_async_copy(x_ref.at[lo], xbuf.at[m, f], own_sem.at[per_group])
    own_x.start()
    for h in range(per_group):
        w_own(h).start()
    pl.semaphore_wait(barrier, frames + 1)

    last = per_group - 1
    outer = jnp.logical_not(inner)

    def send_tokens():
        @pl.loop(0, pieces)
        def _(q):
            for k in range(1, lines):
                x_direct(k, q).start()

    def send_weights(h, which):
        for k in which:
            w_direct(h, k).start()

    send_weights(0, range(4))
    for h in range(1, last):
        send_weights(h, range(2, 4))

    @pl.when(outer)
    def _():
        for h in range(1, last):
            send_weights(h, range(2))
        send_tokens()
        send_weights(last, range(4))

    q0, q1 = d * 2 + c, (1 - d) * 2 + c
    o_across = remote(o_ref.at[o_rows(q0), pl.ds(pl.multiple_of((1 - m) * width, width), width)],
                      wo_ref.at[o_rows(q0), :], o_send.at[0], o_recv.at[q0], mp=1 - m)

    @pl.loop(0, pieces)
    def _(q):
        x_across(f, x_own(q), 0, q).start()
        x_core(f, x_own(q), m, 0, q).start()

    o_across.start()
    for h in range(per_group):
        w_partner(h).start()

    for h in range(last):
        @pl.loop(0, 6)
        def _(j):
            forward_w(h, j)

        @pl.when(inner)
        def _():
            if h + 1 < last:
                send_weights(h + 1, range(2))
            else:
                send_tokens()
                send_weights(last, range(4))

    o_q0 = wo_ref.at[o_rows(q0), :]
    o_q1 = wo_ref.at[o_rows(q1), :]
    o_share = remote(o_q0, o_q0, o_send.at[1], o_recv.at[q0], dp=1 - d)
    o_core0 = remote(o_q0, o_q0, o_send.at[2], o_recv.at[q0], frame=other_core)
    o_core1 = remote(o_q1, o_q1, o_send.at[3], o_recv.at[q1], frame=other_core)
    arrived(o_q0, o_recv.at[q0])
    o_share.start()
    o_core0.start()

    def matmul(slot, h, owner, first):
        side = owner // (frames // mps)
        col = pl.multiple_of((owner % (frames // mps)) * depth, depth)
        w = jnp.concatenate([wbuf[h, p, whole_rows(owner), :] for p in range(3)], axis=1)
        step = frames // 2

        @pl.loop(0, 2)
        def _(i):
            x = xbuf[side, pl.ds(i * step, step), :, pl.ds(col, depth)].reshape(step * spots, depth)
            y = jnp.dot(x, w, preferred_element_type=jnp.float32).reshape(step, spots, 3 * HS)

            @pl.when(first)
            def _():
                acc[slot, pl.ds(i * step, step)] = y

            @pl.when(jnp.logical_not(first))
            def _():
                acc[slot, pl.ds(i * step, step)] += y

    def attention(slot, h):
        scale = 1.0 / math.sqrt(HS)

        @pl.loop(0, frames)
        def _(t):
            for p in range(3):
                qkv[p, t] = acc[slot, t, :, p * HS:(p + 1) * HS].astype(qkv.dtype)

        rows = math.gcd(spots, 32)

        @pl.loop(0, spots // rows)
        def _(i):
            at = pl.ds(pl.multiple_of(i * rows, rows), rows)
            for t in range(frames):
                q = qkv[0, t, at, :].astype(jnp.float32) * scale
                scores = [jnp.sum(q * qkv[1, u, at, :].astype(jnp.float32), axis=-1, keepdims=True)
                          for u in range(t + 1)]
                peak = functools.reduce(jnp.maximum, scores)
                weights = [jnp.exp(s - peak) for s in scores]
                total = functools.reduce(jnp.add, weights)
                accum = functools.reduce(
                    jnp.add,
                    [w * qkv[2, u, at, :].astype(jnp.float32) for u, w in enumerate(weights)])
                abuf[h, t, at, :] = (accum / total).astype(abuf.dtype)

        a_own(h).start()

        @pl.loop(1, frames)
        def _(k):
            a_direct(h, k).start()

    def ready_w(h, j):
        owner = source_of(j)
        arrived(w_block(h, owner, 1 - d), w_recv.at[h, owner, 1 - d])

    def ready_chip(h):
        w_own(h).wait()
        arrived(wbuf.at[h, :, whole_rows(other_core), :], w_recv.at[h, other_core, 0])

    @pl.loop(0, pieces + 2)
    def _(q):
        @pl.when(q < pieces)
        def _():
            for k in range(1, lines):
                owner = x_owner(k)
                block = x_piece(m, owner, q)
                arrived(block, x_recv.at[m, owner, q])
                x_across(owner, block, k, q).start()
                x_core(owner, block, m, k, q).start()

        @pl.when(jnp.logical_and(q >= 1, q < pieces + 1))
        def _():
            for k in range(lines):
                owner = x_owner(k)
                block = x_piece(1 - m, owner, q - 1)
                arrived(block, x_recv.at[1 - m, owner, q - 1])
                x_core(owner, block, 1 - m, k, q - 1).start()

        @pl.when(q == 2)
        def _():
            own_x.wait()

            @pl.loop(0, last)
            def _(h):
                ready_chip(h)
                for j in range(6):
                    ready_w(h, j)

        @pl.when(q >= pieces)
        def _():
            forward_w(last, q - pieces)

        @pl.when(q >= 2)
        def _():
            for k in range(lines):
                owner = x_owner(k) + 1 - 2 * c
                for which in range(mps):
                    arrived(x_piece(which, owner, q - 2), x_recv.at[which, owner, q - 2])

            @pl.loop(0, last * mps)
            def _(i):
                side = i % mps
                matmul(i // mps, i // mps, side * pieces + q - 2,
                       jnp.logical_and(side == 0, q == 2))

    arrived(o_q1, o_recv.at[q1])
    o_core1.start()

    @pl.loop(0, last)
    def _(h):
        forward_w(last, 2 + h)
        attention(h, h)

    ready_chip(last)
    matmul(0, last, f, True)
    matmul(0, last, other_core, False)

    @pl.loop(0, 6)
    def _(j):
        @pl.when(jnp.logical_and(j + 1 >= 2 + last, j < 5))
        def _():
            forward_w(last, j + 1)

        ready_w(last, j)
        matmul(0, last, source_of(j), False)

    for h in range(last - 1):
        forward_attn(h)
    attention(0, last)
    for h in range(last - 1, per_group):
        forward_attn(h)

    for which in (d * 2 + 1 - c, (1 - d) * 2 + 1 - c):
        arrived(wo_ref.at[o_rows(which), :], o_recv.at[which])
    for copy in (o_across, o_share, o_core0, o_core1):
        copy.wait_send()

    @pl.loop(0, pieces)
    def _(q):
        for k in range(1, lines):
            x_direct(k, q).wait_send()
        for k in range(lines):
            owner = x_owner(k)
            block = x_piece(m, owner, q)
            x_across(owner, block, k, q).wait_send()
            x_core(owner, block, m, k, q).wait_send()
            x_core(owner, x_piece(1 - m, owner, q), 1 - m, k, q).wait_send()

    @pl.loop(0, per_group)
    def _(h):
        for k in range(4):
            w_direct(h, k).wait_send()
        w_partner(h).wait_send()
        for j in range(6):
            w_share(h, j).wait_send()

        @pl.when(inner)
        def _():
            for j in range(2, 6):
                w_relay(h, j).wait_send()

        @pl.loop(1, frames)
        def _(k):
            a_direct(h, k).wait_send()

        @pl.loop(0, frames)
        def _(k):
            a_across(h, k).wait_send()
            owner = (f + k) % frames
            arrived(attn_block(1 - m, owner, h), e_recv.at[h, owner])


def fused(xin, w_parts, w_out, frames):
    clips, spots, width = xin.shape
    parts, depth, heads_width = w_parts.shape
    groups = frames // clips
    per_group = heads_width // HS // groups
    lines = frames // 2
    any_spec = pl.BlockSpec(memory_space=pl.ANY)
    dma = pltpu.SemaphoreType.DMA
    return pl.pallas_call(
        fused_kernel,
        in_specs=[any_spec] * 3,
        out_specs=[any_spec] * 2,
        out_shape=[
            jax.ShapeDtypeStruct((2, clips * spots, heads_width), jnp.bfloat16),
            jax.ShapeDtypeStruct((w_out.shape[0], width), jnp.bfloat16),
        ],
        scratch_shapes=[
            pltpu.VMEM((2, frames, spots, width), jnp.bfloat16),
            pltpu.VMEM((per_group, parts, depth * frames, HS), jnp.bfloat16),
            pltpu.VMEM((per_group - 1, frames, spots, parts * HS), jnp.float32),
            pltpu.VMEM((parts, frames, spots, HS), jnp.bfloat16),
            pltpu.VMEM((per_group, frames, spots, HS), jnp.bfloat16),
            dma((2, frames, frames // 2)), dma((16, frames // 2)),
            dma((per_group, frames, 2)), dma((per_group, 15)),
            dma((4,)), dma((4,)),
            dma((per_group, frames)), dma((per_group, frames)),
            dma((per_group, frames)), dma((per_group, frames)),
            dma((per_group + 1,)),
        ],
        compiler_params=pltpu.CompilerParams(
            collective_id=2, has_side_effects=True, vmem_limit_bytes=60 << 20),
        name="fused",
    )(xin, w_parts, w_out)


def gather_mp(block, size):
    if size != 2:
        return lax.all_gather(block, "mp", axis=block.ndim - 1, tiled=True)
    other = lax.ppermute(block, "mp", [(0, 1), (1, 0)])
    first = lax.axis_index("mp") == 0
    return jnp.concatenate(
        [jnp.where(first, block, other), jnp.where(first, other, block)], axis=-1
    )


def fits_fused(mps, dps, frames, clips, spots, width, depth, heads_width):
    groups = frames // clips
    return (mps == dps == clips == 2 and frames == groups * clips and groups == 2 * clips
            and heads_width % (groups * HS) == 0 and heads_width // HS // groups > 1
            and spots % 32 == 0 and depth % HS == 0
            and width * mps == depth * frames)


def body(mp_size, dp_size, tokens, token_mask, mask_embed, w_qkv, w_out, action_idx, codebook,
         act_proj, cotangent):
    clips, _, spots, width = tokens.shape
    heads_width = w_qkv.shape[2]
    depth = w_qkv.shape[0]
    xin = jnp.where(token_mask[..., None] == 1, mask_embed, tokens)
    frames = lax.axis_size("frame")
    if fits_fused(mp_size, dp_size, frames, clips, spots, width, depth, heads_width):
        my_mp = lax.axis_index("mp")
        heads, out_other = fused(xin.reshape(clips, spots, width), w_qkv.transpose(1, 0, 2), w_out, frames)
        out_mine = lax.dynamic_slice_in_dim(w_out, my_mp * width, width, axis=1)
        own = lax.dynamic_index_in_dim(heads, my_mp, 0, keepdims=False)
        other = lax.dynamic_index_in_dim(heads, 1 - my_mp, 0, keepdims=False)
        mixed_rows = jnp.dot(own, out_mine, preferred_element_type=jnp.float32) + jnp.dot(
            other, out_other, preferred_element_type=jnp.float32)
    else:
        share = depth // dp_size
        mine = lax.dynamic_slice_in_dim(
            w_qkv.reshape(depth, 3 * heads_width), lax.axis_index("dp") * share, share, axis=0
        )
        weights = lax.all_gather(mine, ("frame", "dp"), axis=0, tiled=True)
        if mp_size == 2:
            my_mp = lax.axis_index("mp")
            out_mine = lax.dynamic_slice_in_dim(w_out, my_mp * width, width, axis=1)
            out_other = lax.ppermute(
                lax.dynamic_slice_in_dim(w_out, (1 - my_mp) * width, width, axis=1),
                "mp", [(0, 1), (1, 0)])
        spread = lax.all_to_all(
            xin.reshape(clips, spots, width), "frame", split_axis=1, concat_axis=0, tiled=True
        )
        frames = spread.shape[0] // clips
        local = spread.shape[1]
        features = gather_mp(spread.reshape(frames * clips * local, width), mp_size)
        qkv = jnp.dot(features, weights, preferred_element_type=jnp.float32).astype(jnp.bfloat16)
        attn = attend(qkv.reshape(frames, clips * local, 3 * heads_width), frames, heads_width)
        back = lax.all_to_all(
            attn.reshape(frames * clips, local, heads_width), "frame", split_axis=0, concat_axis=1,
            tiled=True,
        )
        heads = back.reshape(clips * spots, heads_width)
        if mp_size == 2:
            other_heads = lax.ppermute(heads, "mp", [(0, 1), (1, 0)])
            mixed_rows = jnp.dot(heads, out_mine, preferred_element_type=jnp.float32) + jnp.dot(
                other_heads, out_other, preferred_element_type=jnp.float32)
        else:
            out_block = lax.all_to_all(w_out, "mp", split_axis=1, concat_axis=0, tiled=True)
            mixed_rows = jnp.dot(gather_mp(heads, mp_size), out_block,
                                 preferred_element_type=jnp.float32)
    mixed = mixed_rows.reshape(clips, 1, spots, width)
    onehot = (
        action_idx.reshape(clips)[:, None] == jnp.arange(codebook.shape[0])[None, :]
    ).astype(jnp.float32)
    codevec = jnp.dot(onehot, codebook, precision=lax.Precision.HIGHEST)
    gate = jnp.dot(codevec, act_proj, precision=lax.Precision.HIGHEST)
    next_state = (xin.astype(jnp.float32) + gate[:, None, None, :] * mixed).astype(jnp.bfloat16)
    dgate = jnp.sum(cotangent.astype(jnp.float32) * mixed, axis=2).reshape(clips, width)
    codes = codevec.shape[1]
    padded = jnp.pad(codevec, ((0, 0), (0, -codes % 128)))
    terms = spread_terms(jnp.concatenate([dgate, padded], axis=1), frames, dp_size)
    terms = terms.reshape(frames * dp_size * clips, -1)
    grad_proj = jnp.dot(
        terms[:, width : width + codes].T, terms[:, :width], precision=lax.Precision.HIGHEST)
    return (next_state, grad_proj)


def solution(mesh):
    in_specs = (
        P("dp", "frame", None, "mp"),
        P("dp", "frame", None),
        P("mp"),
        P("frame", None, "mp"),
        P("mp", None),
        P("dp", "frame"),
        P(),
        P(None, "mp"),
        P("dp", "frame", None, "mp"),
    )
    out_specs = (P("dp", "frame", None, "mp"), P(None, "mp"))
    return jax.shard_map(
        functools.partial(body, mesh.shape["mp"], mesh.shape["dp"]),
        mesh=mesh, in_specs=in_specs, out_specs=out_specs, check_vma=False,
    )
```

```python
import functools
import math

import jax
import jax.numpy as jnp
from jax import lax
from jax.experimental import pallas as pl
from jax.experimental.pallas import tpu as pltpu
from jax.sharding import PartitionSpec as P

HS = 128


def attend_kernel(frames, q_ref, k_ref, v_ref, o_ref):
    scale = 1.0 / math.sqrt(HS)
    for t in range(frames):
        q = q_ref[t].astype(jnp.float32) * scale
        scores = [
            jnp.sum(q * k_ref[u].astype(jnp.float32), axis=-1, keepdims=True) for u in range(t + 1)
        ]
        peak = functools.reduce(jnp.maximum, scores)
        weights = [jnp.exp(s - peak) for s in scores]
        total = functools.reduce(jnp.add, weights)
        accum = functools.reduce(
            jnp.add, [w * v_ref[u].astype(jnp.float32) for u, w in enumerate(weights)]
        )
        o_ref[t] = (accum / total).astype(o_ref.dtype)


def attend(qkv, frames, heads_width):
    rows = qkv.shape[1]
    heads = heads_width // HS
    spec = lambda part: pl.BlockSpec((frames, rows, HS), lambda h, part=part: (0, 0, part * heads + h))
    return pl.pallas_call(
        functools.partial(attend_kernel, frames),
        grid=(heads,),
        in_specs=[spec(0), spec(1), spec(2)],
        out_specs=spec(0),
        out_shape=jax.ShapeDtypeStruct((frames, rows, heads_width), jnp.bfloat16),
        cost_estimate=pl.CostEstimate(flops=4 * frames * frames * rows * heads_width,
                                      bytes_accessed=8 * frames * rows * heads_width,
                                      transcendentals=0),
        name="attend",
    )(qkv, qkv, qkv)


def spread_kernel(frames, dps, x_ref, o_ref, send_sem, recv_sem, own_sem):
    count = frames * dps
    me = lax.axis_index("frame") * dps + lax.axis_index("dp")
    barrier = pltpu.get_barrier_semaphore()

    def peer(shift):
        other = lax.rem(me + shift, count)
        return {"frame": other // dps, "dp": lax.rem(other, dps)}

    for shift in range(1, count):
        pl.semaphore_signal(barrier, inc=1, device_id=peer(shift),
                            device_id_type=pl.DeviceIdType.MESH)
    own = pltpu.make_async_copy(x_ref, o_ref.at[me], own_sem)
    own.start()
    pl.semaphore_wait(barrier, count - 1)
    copies = []
    for shift in range(1, count):
        copy = pltpu.make_async_remote_copy(
            src_ref=x_ref, dst_ref=o_ref.at[me], send_sem=send_sem.at[shift],
            recv_sem=recv_sem.at[shift], device_id=peer(shift),
            device_id_type=pl.DeviceIdType.MESH)
        copy.start()
        copies.append(copy)
    own.wait()
    for copy in copies:
        copy.wait()


def spread_terms(terms, frames, dps):
    count = frames * dps
    return pl.pallas_call(
        functools.partial(spread_kernel, frames, dps),
        in_specs=[pl.BlockSpec(memory_space=pltpu.VMEM)],
        out_specs=pl.BlockSpec(memory_space=pltpu.VMEM),
        out_shape=jax.ShapeDtypeStruct((count, *terms.shape), terms.dtype),
        scratch_shapes=[pltpu.SemaphoreType.DMA((count,)), pltpu.SemaphoreType.DMA((count,)),
                        pltpu.SemaphoreType.DMA],
        compiler_params=pltpu.CompilerParams(collective_id=1, has_side_effects=True),
        name="spread_terms",
    )(terms)


scope = jax.named_scope


def fused_kernel(x_ref, w_ref, o_ref, attn_ref, wo_ref, xbuf, wbuf, acc, qkv, abuf, x_recv,
                 x_send, w_recv, w_send, o_recv, o_send, a_recv, a_send, e_recv, e_send, own_sem):
    mps, frames, spots, width = xbuf.shape
    per_group, _, _, _ = wbuf.shape
    depth = w_ref.shape[1]
    lines = frames // 2
    half = lines // 2
    part = depth // 2
    quarter = o_ref.shape[0] // 4
    f, m, d = lax.axis_index("frame"), lax.axis_index("mp"), lax.axis_index("dp")
    z, c = f // 2, f % 2
    hi, lo = z // 2, z % 2
    mine = hi * 2 + c
    inner = hi != lo
    pair, near, far = z + 1 - 2 * lo, half - hi, (lines - 1) * (1 - hi)
    other_core = 2 * z + 1 - c
    q0, q1 = d * 2 + c, (1 - d) * 2 + c

    def remote(source, target, send_sem, recv_sem, frame=f, mp=m, dp=d):
        return pltpu.make_async_remote_copy(
            src_ref=source, dst_ref=target, send_sem=send_sem, recv_sem=recv_sem,
            device_id={"frame": frame, "mp": mp, "dp": dp},
            device_id_type=pl.DeviceIdType.MESH)

    def arrived(target, recv_sem):
        pltpu.make_async_copy(target, target, recv_sem).wait()

    def rows_of(owner, which):
        return pl.ds(pl.multiple_of(owner * depth + which * part, part), part)

    def whole_rows(owner):
        return pl.ds(pl.multiple_of(owner * depth, depth), depth)

    def columns(group, head):
        return pl.ds(pl.multiple_of((group * per_group + head) * HS, HS), HS)

    def line(j):
        return jnp.where(j == 0, pair, jnp.where(j == 1, near, far))

    def source_of(j):
        return 2 * line(j // 2) + j % 2

    def w_direct(h, k):
        target = jnp.where(k < 2, pair, near)
        group = jnp.where(k < 2, hi, 1 - hi) * 2 + k % 2
        return remote(w_ref.at[:, pl.ds(pl.multiple_of(d * part, part), part), columns(group, h)],
                      wbuf.at[h, :, rows_of(f, d), :], w_send.at[h, k], w_recv.at[h, f, d],
                      frame=2 * target + k % 2)

    def w_partner(h):
        return remote(w_ref.at[:, :, columns(hi * 2 + 1 - c, h)], wbuf.at[h, :, whole_rows(f), :],
                      w_send.at[h, 4], w_recv.at[h, f, 0], frame=other_core)

    def w_own(h):
        return pltpu.make_async_copy(w_ref.at[:, :, columns(mine, h)],
                                     wbuf.at[h, :, whole_rows(f), :], own_sem.at[h])

    def w_block(h, owner, which):
        return wbuf.at[h, :, rows_of(owner, which), :]

    def w_share(h, j):
        owner = source_of(j)
        block = w_block(h, owner, d)
        return remote(block, block, w_send.at[h, 5 + j], w_recv.at[h, owner, d], dp=1 - d)

    def w_relay(h, j):
        owner = source_of(j)
        block = w_block(h, owner, d)
        return remote(block, block, w_send.at[h, 9 + j], w_recv.at[h, owner, d],
                      frame=2 * pair + c)

    def forward_w(h, j):
        owner = source_of(j)
        with scope("fw"):
            arrived(w_block(h, owner, d), w_recv.at[h, owner, d])

        @pl.when(jnp.logical_and(inner, j >= 2))
        def _():
            w_relay(h, j).start()

        w_share(h, j).start()

    pieces = frames // mps

    def features(q):
        return pl.ds(pl.multiple_of(q * depth, depth), depth)

    def x_piece(which, owner, q):
        return xbuf.at[which, owner, :, features(q)]

    def x_direct(k, q):
        target = (z + k) % lines
        return remote(x_ref.at[target % 2, :, features(q)], x_piece(m, f, q), x_send.at[k, q],
                      x_recv.at[m, f, q], frame=2 * target + c)

    def x_across(owner, source, k, q):
        return remote(source, x_piece(m, owner, q), x_send.at[4 + k, q], x_recv.at[m, owner, q],
                      mp=1 - m)

    def x_core(owner, source, which, k, q):
        slot = jnp.where(which == m, 8, 12)
        return remote(source, x_piece(which, owner, q), x_send.at[slot + k, q],
                      x_recv.at[which, owner, q], frame=other_core)

    def x_own(q):
        return x_ref.at[lo, :, features(q)]

    def x_owner(k):
        return f if k == 0 else 2 * line(k - 1) + c

    slices = o_recv.shape[1]
    share = quarter // slices

    def o_rows(which, i):
        return pl.ds(pl.multiple_of(which * quarter + i * share, share), share)

    def o_piece(which, i):
        return wo_ref.at[o_rows(which, i), :]

    def o_across(i):
        return remote(
            o_ref.at[o_rows(q0, i), pl.ds(pl.multiple_of((1 - m) * width, width), width)],
            o_piece(q0, i), o_send.at[0, i], o_recv.at[q0, i], mp=1 - m)

    def o_share(i):
        return remote(o_piece(q0, i), o_piece(q0, i), o_send.at[1, i], o_recv.at[q0, i], dp=1 - d)

    def o_core(which, i, slot):
        return remote(o_piece(which, i), o_piece(which, i), o_send.at[slot, i],
                      o_recv.at[which, i], frame=other_core)

    def forward_o(i):
        with scope("o_0"):
            arrived(o_piece(q0, i), o_recv.at[q0, i])
        o_share(i).start()
        o_core(q0, i, 2).start()

    def attn_block(which, owner, h):
        group = (owner // 4) * 2 + owner % 2
        clip = (owner // 2) % 2
        return attn_ref.at[which, pl.ds(pl.multiple_of(clip * spots, spots), spots),
                           columns(group, h)]

    def a_direct(h, k):
        target = (f + k) % frames
        return remote(abuf.at[h, target], attn_block(m, f, h), a_send.at[h, k], a_recv.at[h, f],
                      frame=target)

    def a_own(h):
        return pltpu.make_async_copy(abuf.at[h, f], attn_block(m, f, h), a_recv.at[h, f])

    def a_across(h, k):
        owner = (f + k) % frames
        block = attn_block(m, owner, h)
        return remote(block, block, e_send.at[h, k], e_recv.at[h, owner], mp=1 - m)

    def forward_attn(h):
        @pl.loop(0, frames)
        def _(k):
            owner = (f + k) % frames
            arrived(attn_block(m, owner, h), a_recv.at[h, owner])
            a_across(h, k).start()

    barrier = pltpu.get_barrier_semaphore()
    for k in range(1, frames):
        pl.semaphore_signal(barrier, inc=1, device_id={"frame": (f + k) % frames, "mp": m, "dp": d},
                            device_id_type=pl.DeviceIdType.MESH)
    pl.semaphore_signal(barrier, inc=1, device_id={"frame": f, "mp": 1 - m, "dp": d},
                        device_id_type=pl.DeviceIdType.MESH)
    pl.semaphore_signal(barrier, inc=1, device_id={"frame": f, "mp": m, "dp": 1 - d},
                        device_id_type=pl.DeviceIdType.MESH)
    own_x = pltpu.make_async_copy(x_ref.at[lo], xbuf.at[m, f], own_sem.at[per_group])
    own_x.start()
    for h in range(per_group):
        w_own(h).start()
    pl.semaphore_wait(barrier, frames + 1)

    last = per_group - 1
    outer = jnp.logical_not(inner)

    def send_tokens(q):
        for k in range(1, lines):
            x_direct(k, q).start()

    def send_weights(h):
        for k in range(4):
            w_direct(h, k).start()

    send_weights(0)
    send_tokens(0)

    @pl.loop(0, slices)
    def _(i):
        o_across(i).start()

    for h in range(per_group):
        w_partner(h).start()

    @pl.loop(0, pieces)
    def _(q):
        x_core(f, x_own(q), m, 0, q).start()

    @pl.loop(0, 2)
    def _(j):
        forward_w(0, j)

    send_tokens(1)

    @pl.when(inner)
    def _():
        @pl.loop(2, 6)
        def _(j):
            forward_w(0, j)

    forward_o(0)
    forward_o(1)

    @pl.when(outer)
    def _():
        forward_w(0, 2)
        forward_w(0, 3)

    forward_o(2)

    def matmul(slot, h, owner, first):
        side = owner // (frames // mps)
        col = pl.multiple_of((owner % (frames // mps)) * depth, depth)
        w = jnp.concatenate([wbuf[h, p, whole_rows(owner), :] for p in range(3)], axis=1)
        step = frames // 2

        @pl.loop(0, 2)
        def _(i):
            x = xbuf[side, pl.ds(i * step, step), :, pl.ds(col, depth)].reshape(step * spots, depth)
            y = jnp.dot(x, w, preferred_element_type=jnp.float32).reshape(step, spots, 3 * HS)

            @pl.when(first)
            def _():
                acc[slot, pl.ds(i * step, step)] = y

            @pl.when(jnp.logical_not(first))
            def _():
                acc[slot, pl.ds(i * step, step)] += y

    def attend_rows(h, i, rows):
        scale = 1.0 / math.sqrt(HS)
        at = pl.ds(pl.multiple_of(i * rows, rows), rows)
        for t in range(frames):
            q = qkv[0, t, at, :].astype(jnp.float32) * scale
            scores = [jnp.sum(q * qkv[1, u, at, :].astype(jnp.float32), axis=-1, keepdims=True)
                      for u in range(t + 1)]
            peak = functools.reduce(jnp.maximum, scores)
            weights = [jnp.exp(s - peak) for s in scores]
            total = functools.reduce(jnp.add, weights)
            accum = functools.reduce(
                jnp.add,
                [w * qkv[2, u, at, :].astype(jnp.float32) for u, w in enumerate(weights)])
            abuf[h, t, at, :] = (accum / total).astype(abuf.dtype)

    def attention(slot, h):
        @pl.loop(0, frames)
        def _(t):
            for p in range(3):
                qkv[p, t] = acc[slot, t, :, p * HS:(p + 1) * HS].astype(qkv.dtype)

        rows = math.gcd(spots, 32)

        @pl.loop(0, spots // rows)
        def _(i):
            with scope("att"):
                attend_rows(h, i, rows)

        a_own(h).start()

        @pl.loop(1, frames)
        def _(k):
            a_direct(h, k).start()

    def ready_w(h, j):
        owner = source_of(j)
        arrived(w_block(h, owner, 1 - d), w_recv.at[h, owner, 1 - d])

    def ready_chip(h):
        w_own(h).wait()
        arrived(wbuf.at[h, :, whole_rows(other_core), :], w_recv.at[h, other_core, 0])

    def ready_w(h, j):
        owner = source_of(j)
        arrived(w_block(h, owner, 1 - d), w_recv.at[h, owner, 1 - d])

    def ready_chip(h):
        w_own(h).wait()
        arrived(wbuf.at[h, :, whole_rows(other_core), :], w_recv.at[h, other_core, 0])

    @pl.loop(0, pieces + 3)
    def _(q):
        @pl.when(q < pieces)
        def _():
            x_across(f, x_own(q), 0, q).start()
            for k in range(1, lines):
                owner = x_owner(k)
                block = x_piece(m, owner, q)
                with scope("x_own"):
                    arrived(block, x_recv.at[m, owner, q])
                x_across(owner, block, k, q).start()
                x_core(owner, block, m, k, q).start()

        @pl.when(q < pieces - 2)
        def _():
            send_tokens(q + 2)

        @pl.when(q == pieces - 2)
        def _():
            send_weights(1)

        @pl.when(q == 0)
        def _():
            forward_o(3)

            @pl.when(outer)
            def _():
                forward_w(0, 4)
                forward_w(0, 5)

        @pl.when(jnp.logical_and(q >= 2, q < pieces + 2))
        def _():
            for k in range(lines):
                owner = x_owner(k)
                block = x_piece(1 - m, owner, q - 2)
                with scope("x_other"):
                    arrived(block, x_recv.at[1 - m, owner, q - 2])
                x_core(owner, block, 1 - m, k, q - 2).start()

        @pl.when(q == 4)
        def _():
            for h in range(2, per_group):
                send_weights(h)

        @pl.when(jnp.logical_and(q >= 4, q < 6))
        def _():
            forward_w(1, 3 * (q - 4))
            forward_w(1, 3 * (q - 4) + 1)
            forward_w(1, 3 * (q - 4) + 2)

        @pl.when(q == 6)
        def _():
            forward_w(2, 0)
            forward_w(2, 1)

        @pl.when(q == 3)
        def _():
            with scope("w_0"):
                own_x.wait()
                ready_chip(0)
                for j in range(6):
                    ready_w(0, j)

        @pl.when(q >= 3)
        def _():
            with scope("x_core"):
                for k in range(lines):
                    owner = x_owner(k) + 1 - 2 * c
                    for which in range(mps):
                        arrived(x_piece(which, owner, q - 3), x_recv.at[which, owner, q - 3])

            @pl.loop(0, mps)
            def _(side):
                with scope("mm0"):
                    matmul(0, 0, side * pieces + q - 3, jnp.logical_and(side == 0, q == 3))

    @pl.loop(0, slices)
    def _(i):
        with scope("o_1"):
            arrived(o_piece(q1, i), o_recv.at[q1, i])
        o_core(q1, i, 3).start()

    attention(0, 0)

    @pl.loop(0, last * frames)
    def _(i):
        h, jj = 1 + i // frames, i % frames

        @pl.when(jnp.logical_and(inner, jnp.logical_and(h < last, jj >= 4)))
        def _():
            forward_w(h + 1, jj - 2)

        @pl.when(jnp.logical_and(outer, jnp.logical_and(h < last, jj >= 6)))
        def _():
            forward_w(h + 1, jj - 4)

        @pl.when(jnp.logical_and(outer, jnp.logical_and(h > 1, jnp.logical_and(jj >= 4, jj < 6))))
        def _():
            forward_w(h, jj)

        @pl.when(jj == 0)
        def _():
            ready_chip(h)

        @pl.when(jj >= 2)
        def _():
            with scope("w_y"):
                ready_w(h, jnp.maximum(jj - 2, 0))

        owner = jnp.where(jj == 0, f, jnp.where(jj == 1, other_core, source_of(jnp.maximum(jj - 2, 0))))
        with scope("mm"):
            matmul(0, h, owner, jj == 0)

        @pl.when(jj == frames - 1)
        def _():
            @pl.when(h == last)
            def _():
                with scope("fa"):
                    forward_attn(last - 1)

            attention(0, h)

        @pl.when(jnp.logical_and(h == last, jj == 3))
        def _():
            for before in range(last - 1):
                with scope("fa"):
                    forward_attn(before)

    with scope("fa"):
        forward_attn(last)
    @pl.loop(0, slices)
    def _(i):
        for which in (d * 2 + 1 - c, (1 - d) * 2 + 1 - c):
            arrived(o_piece(which, i), o_recv.at[which, i])
        for copy in (o_across(i), o_share(i), o_core(q0, i, 2), o_core(q1, i, 3)):
            copy.wait_send()

    @pl.loop(0, pieces)
    def _(q):
        for k in range(1, lines):
            x_direct(k, q).wait_send()
        for k in range(lines):
            owner = x_owner(k)
            block = x_piece(m, owner, q)
            x_across(owner, block, k, q).wait_send()
            x_core(owner, block, m, k, q).wait_send()
            x_core(owner, x_piece(1 - m, owner, q), 1 - m, k, q).wait_send()

    @pl.loop(0, per_group)
    def _(h):
        for k in range(4):
            w_direct(h, k).wait_send()
        w_partner(h).wait_send()
        for j in range(6):
            w_share(h, j).wait_send()

        @pl.when(inner)
        def _():
            for j in range(2, 6):
                w_relay(h, j).wait_send()

        @pl.loop(1, frames)
        def _(k):
            a_direct(h, k).wait_send()

        @pl.loop(0, frames)
        def _(k):
            a_across(h, k).wait_send()
            owner = (f + k) % frames
            arrived(attn_block(1 - m, owner, h), e_recv.at[h, owner])


def fused(xin, w_parts, w_out, frames):
    clips, spots, width = xin.shape
    parts, depth, heads_width = w_parts.shape
    groups = frames // clips
    per_group = heads_width // HS // groups
    lines = frames // 2
    any_spec = pl.BlockSpec(memory_space=pl.ANY)
    dma = pltpu.SemaphoreType.DMA
    return pl.pallas_call(
        fused_kernel,
        in_specs=[any_spec] * 3,
        out_specs=[any_spec] * 2,
        out_shape=[
            jax.ShapeDtypeStruct((2, clips * spots, heads_width), jnp.bfloat16),
            jax.ShapeDtypeStruct((w_out.shape[0], width), jnp.bfloat16),
        ],
        scratch_shapes=[
            pltpu.VMEM((2, frames, spots, width), jnp.bfloat16),
            pltpu.VMEM((per_group, parts, depth * frames, HS), jnp.bfloat16),
            pltpu.VMEM((1, frames, spots, parts * HS), jnp.float32),
            pltpu.VMEM((parts, frames, spots, HS), jnp.bfloat16),
            pltpu.VMEM((per_group, frames, spots, HS), jnp.bfloat16),
            dma((2, frames, frames // 2)), dma((16, frames // 2)),
            dma((per_group, frames, 2)), dma((per_group, 15)),
            dma((4, 4)), dma((4, 4)),
            dma((per_group, frames)), dma((per_group, frames)),
            dma((per_group, frames)), dma((per_group, frames)),
            dma((per_group + 1,)),
        ],
        compiler_params=pltpu.CompilerParams(
            collective_id=2, has_side_effects=True, vmem_limit_bytes=60 << 20),
        name="fused",
    )(xin, w_parts, w_out)


def gather_mp(block, size):
    if size != 2:
        return lax.all_gather(block, "mp", axis=block.ndim - 1, tiled=True)
    other = lax.ppermute(block, "mp", [(0, 1), (1, 0)])
    first = lax.axis_index("mp") == 0
    return jnp.concatenate(
        [jnp.where(first, block, other), jnp.where(first, other, block)], axis=-1
    )


def fits_fused(mps, dps, frames, clips, spots, width, depth, heads_width):
    groups = frames // clips
    return (mps == dps == clips == 2 and frames == groups * clips and groups == 2 * clips
            and heads_width % (groups * HS) == 0 and heads_width // HS // groups > 1
            and spots % 32 == 0 and depth % HS == 0
            and width * mps == depth * frames and heads_width % (16 * 16) == 0)


def body(mp_size, dp_size, tokens, token_mask, mask_embed, w_qkv, w_out, action_idx, codebook,
         act_proj, cotangent):
    clips, _, spots, width = tokens.shape
    heads_width = w_qkv.shape[2]
    depth = w_qkv.shape[0]
    xin = jnp.where(token_mask[..., None] == 1, mask_embed, tokens)
    frames = lax.axis_size("frame")
    if fits_fused(mp_size, dp_size, frames, clips, spots, width, depth, heads_width):
        my_mp = lax.axis_index("mp")
        heads, out_other = fused(xin.reshape(clips, spots, width), w_qkv.transpose(1, 0, 2), w_out, frames)
        out_mine = lax.dynamic_slice_in_dim(w_out, my_mp * width, width, axis=1)
        own = lax.dynamic_index_in_dim(heads, my_mp, 0, keepdims=False)
        other = lax.dynamic_index_in_dim(heads, 1 - my_mp, 0, keepdims=False)
        mixed_rows = jnp.dot(own, out_mine, preferred_element_type=jnp.float32) + jnp.dot(
            other, out_other, preferred_element_type=jnp.float32)
    else:
        share = depth // dp_size
        mine = lax.dynamic_slice_in_dim(
            w_qkv.reshape(depth, 3 * heads_width), lax.axis_index("dp") * share, share, axis=0
        )
        weights = lax.all_gather(mine, ("frame", "dp"), axis=0, tiled=True)
        if mp_size == 2:
            my_mp = lax.axis_index("mp")
            out_mine = lax.dynamic_slice_in_dim(w_out, my_mp * width, width, axis=1)
            out_other = lax.ppermute(
                lax.dynamic_slice_in_dim(w_out, (1 - my_mp) * width, width, axis=1),
                "mp", [(0, 1), (1, 0)])
        spread = lax.all_to_all(
            xin.reshape(clips, spots, width), "frame", split_axis=1, concat_axis=0, tiled=True
        )
        frames = spread.shape[0] // clips
        local = spread.shape[1]
        features = gather_mp(spread.reshape(frames * clips * local, width), mp_size)
        qkv = jnp.dot(features, weights, preferred_element_type=jnp.float32).astype(jnp.bfloat16)
        attn = attend(qkv.reshape(frames, clips * local, 3 * heads_width), frames, heads_width)
        back = lax.all_to_all(
            attn.reshape(frames * clips, local, heads_width), "frame", split_axis=0, concat_axis=1,
            tiled=True,
        )
        heads = back.reshape(clips * spots, heads_width)
        if mp_size == 2:
            other_heads = lax.ppermute(heads, "mp", [(0, 1), (1, 0)])
            mixed_rows = jnp.dot(heads, out_mine, preferred_element_type=jnp.float32) + jnp.dot(
                other_heads, out_other, preferred_element_type=jnp.float32)
        else:
            out_block = lax.all_to_all(w_out, "mp", split_axis=1, concat_axis=0, tiled=True)
            mixed_rows = jnp.dot(gather_mp(heads, mp_size), out_block,
                                 preferred_element_type=jnp.float32)
    mixed = mixed_rows.reshape(clips, 1, spots, width)
    onehot = (
        action_idx.reshape(clips)[:, None] == jnp.arange(codebook.shape[0])[None, :]
    ).astype(jnp.float32)
    codevec = jnp.dot(onehot, codebook, precision=lax.Precision.HIGHEST)
    gate = jnp.dot(codevec, act_proj, precision=lax.Precision.HIGHEST)
    next_state = (xin.astype(jnp.float32) + gate[:, None, None, :] * mixed).astype(jnp.bfloat16)
    dgate = jnp.sum(cotangent.astype(jnp.float32) * mixed, axis=2).reshape(clips, width)
    codes = codevec.shape[1]
    padded = jnp.pad(codevec, ((0, 0), (0, -codes % 128)))
    terms = spread_terms(jnp.concatenate([dgate, padded], axis=1), frames, dp_size)
    terms = terms.reshape(frames * dp_size * clips, -1)
    grad_proj = jnp.dot(
        terms[:, width : width + codes].T, terms[:, :width], precision=lax.Precision.HIGHEST)
    return (next_state, grad_proj)


def solution(mesh):
    in_specs = (
        P("dp", "frame", None, "mp"),
        P("dp", "frame", None),
        P("mp"),
        P("frame", None, "mp"),
        P("mp", None),
        P("dp", "frame"),
        P(),
        P(None, "mp"),
        P("dp", "frame", None, "mp"),
    )
    out_specs = (P("dp", "frame", None, "mp"), P(None, "mp"))
    return jax.shard_map(
        functools.partial(body, mesh.shape["mp"], mesh.shape["dp"]),
        mesh=mesh, in_specs=in_specs, out_specs=out_specs, check_vma=False,
    )
```

```python
import functools
import math

import jax
import jax.numpy as jnp
from jax import lax
from jax.experimental import pallas as pl
from jax.experimental.pallas import tpu as pltpu
from jax.sharding import PartitionSpec as P

HS = 128


def attend_kernel(frames, q_ref, k_ref, v_ref, o_ref):
    scale = 1.0 / math.sqrt(HS)
    for t in range(frames):
        q = q_ref[t].astype(jnp.float32) * scale
        scores = [
            jnp.sum(q * k_ref[u].astype(jnp.float32), axis=-1, keepdims=True) for u in range(t + 1)
        ]
        peak = functools.reduce(jnp.maximum, scores)
        weights = [jnp.exp(s - peak) for s in scores]
        total = functools.reduce(jnp.add, weights)
        accum = functools.reduce(
            jnp.add, [w * v_ref[u].astype(jnp.float32) for u, w in enumerate(weights)]
        )
        o_ref[t] = (accum / total).astype(o_ref.dtype)


def attend(qkv, frames, heads_width):
    rows = qkv.shape[1]
    heads = heads_width // HS
    spec = lambda part: pl.BlockSpec((frames, rows, HS), lambda h, part=part: (0, 0, part * heads + h))
    return pl.pallas_call(
        functools.partial(attend_kernel, frames),
        grid=(heads,),
        in_specs=[spec(0), spec(1), spec(2)],
        out_specs=spec(0),
        out_shape=jax.ShapeDtypeStruct((frames, rows, heads_width), jnp.bfloat16),
        cost_estimate=pl.CostEstimate(flops=4 * frames * frames * rows * heads_width,
                                      bytes_accessed=8 * frames * rows * heads_width,
                                      transcendentals=0),
        name="attend",
    )(qkv, qkv, qkv)


def spread_kernel(frames, dps, x_ref, o_ref, send_sem, recv_sem, own_sem):
    count = frames * dps
    me = lax.axis_index("frame") * dps + lax.axis_index("dp")
    barrier = pltpu.get_barrier_semaphore()

    def peer(shift):
        other = lax.rem(me + shift, count)
        return {"frame": other // dps, "dp": lax.rem(other, dps)}

    for shift in range(1, count):
        pl.semaphore_signal(barrier, inc=1, device_id=peer(shift),
                            device_id_type=pl.DeviceIdType.MESH)
    own = pltpu.make_async_copy(x_ref, o_ref.at[me], own_sem)
    own.start()
    pl.semaphore_wait(barrier, count - 1)
    copies = []
    for shift in range(1, count):
        copy = pltpu.make_async_remote_copy(
            src_ref=x_ref, dst_ref=o_ref.at[me], send_sem=send_sem.at[shift],
            recv_sem=recv_sem.at[shift], device_id=peer(shift),
            device_id_type=pl.DeviceIdType.MESH)
        copy.start()
        copies.append(copy)
    own.wait()
    for copy in copies:
        copy.wait()


def spread_terms(terms, frames, dps):
    count = frames * dps
    return pl.pallas_call(
        functools.partial(spread_kernel, frames, dps),
        in_specs=[pl.BlockSpec(memory_space=pltpu.VMEM)],
        out_specs=pl.BlockSpec(memory_space=pltpu.VMEM),
        out_shape=jax.ShapeDtypeStruct((count, *terms.shape), terms.dtype),
        scratch_shapes=[pltpu.SemaphoreType.DMA((count,)), pltpu.SemaphoreType.DMA((count,)),
                        pltpu.SemaphoreType.DMA],
        compiler_params=pltpu.CompilerParams(collective_id=1, has_side_effects=True),
        name="spread_terms",
    )(terms)


scope = jax.named_scope


def fused_kernel(dps, x_ref, w_ref, o_ref, cot_ref, act_ref, book_ref, idx_ref, next_ref, grad_ref,
                 xbuf, wbuf, acc, qkv, abuf, heads, wo, total, xin, cot, act, gate, terms, table,
                 x_recv, x_send, w_recv, w_send, o_recv, o_send, a_recv, a_send, e_recv, e_send,
                 own_sem, t_recv, t_send, out_sem):
    mps, frames, spots, width = xbuf.shape
    per_group, _, _, _ = wbuf.shape
    depth = w_ref.shape[1]
    lines = frames // 2
    half = lines // 2
    part = depth // 2
    quarter = o_ref.shape[0] // 4
    f, m, d = lax.axis_index("frame"), lax.axis_index("mp"), lax.axis_index("dp")
    z, c = f // 2, f % 2
    hi, lo = z // 2, z % 2
    mine = hi * 2 + c
    inner = hi != lo
    pair, near, far = z + 1 - 2 * lo, half - hi, (lines - 1) * (1 - hi)
    other_core = 2 * z + 1 - c
    q0, q1 = d * 2 + c, (1 - d) * 2 + c

    def remote(source, target, send_sem, recv_sem, frame=f, mp=m, dp=d):
        return pltpu.make_async_remote_copy(
            src_ref=source, dst_ref=target, send_sem=send_sem, recv_sem=recv_sem,
            device_id={"frame": frame, "mp": mp, "dp": dp},
            device_id_type=pl.DeviceIdType.MESH)

    def arrived(target, recv_sem):
        pltpu.make_async_copy(target, target, recv_sem).wait()

    def rows_of(owner, which):
        return pl.ds(pl.multiple_of(owner * depth + which * part, part), part)

    def whole_rows(owner):
        return pl.ds(pl.multiple_of(owner * depth, depth), depth)

    def columns(group, head):
        return pl.ds(pl.multiple_of((group * per_group + head) * HS, HS), HS)

    def line(j):
        return jnp.where(j == 0, pair, jnp.where(j == 1, near, far))

    def source_of(j):
        return 2 * line(j // 2) + j % 2

    def w_direct(h, k):
        target = jnp.where(k < 2, pair, near)
        group = jnp.where(k < 2, hi, 1 - hi) * 2 + k % 2
        return remote(w_ref.at[:, pl.ds(pl.multiple_of(d * part, part), part), columns(group, h)],
                      wbuf.at[h, :, rows_of(f, d), :], w_send.at[h, k], w_recv.at[h, f, d],
                      frame=2 * target + k % 2)

    def w_partner(h):
        return remote(w_ref.at[:, :, columns(hi * 2 + 1 - c, h)], wbuf.at[h, :, whole_rows(f), :],
                      w_send.at[h, 4], w_recv.at[h, f, 0], frame=other_core)

    def w_own(h):
        return pltpu.make_async_copy(w_ref.at[:, :, columns(mine, h)],
                                     wbuf.at[h, :, whole_rows(f), :], own_sem.at[h])

    def w_block(h, owner, which):
        return wbuf.at[h, :, rows_of(owner, which), :]

    def w_share(h, j):
        owner = source_of(j)
        block = w_block(h, owner, d)
        return remote(block, block, w_send.at[h, 5 + j], w_recv.at[h, owner, d], dp=1 - d)

    def w_relay(h, j):
        owner = source_of(j)
        block = w_block(h, owner, d)
        return remote(block, block, w_send.at[h, 9 + j], w_recv.at[h, owner, d],
                      frame=2 * pair + c)

    def forward_w(h, j):
        owner = source_of(j)
        with scope("fw"):
            arrived(w_block(h, owner, d), w_recv.at[h, owner, d])

        @pl.when(jnp.logical_and(inner, j >= 2))
        def _():
            w_relay(h, j).start()

        w_share(h, j).start()

    pieces = frames // mps

    def features(q):
        return pl.ds(pl.multiple_of(q * depth, depth), depth)

    def x_piece(which, owner, q):
        return xbuf.at[which, owner, :, features(q)]

    def x_direct(k, q):
        target = (z + k) % lines
        return remote(x_ref.at[target % 2, :, features(q)], x_piece(m, f, q), x_send.at[k, q],
                      x_recv.at[m, f, q], frame=2 * target + c)

    def x_across(owner, source, k, q):
        return remote(source, x_piece(m, owner, q), x_send.at[4 + k, q], x_recv.at[m, owner, q],
                      mp=1 - m)

    def x_core(owner, source, which, k, q):
        slot = jnp.where(which == m, 8, 12)
        return remote(source, x_piece(which, owner, q), x_send.at[slot + k, q],
                      x_recv.at[which, owner, q], frame=other_core)

    def x_own(q):
        return x_ref.at[lo, :, features(q)]

    def x_owner(k):
        return f if k == 0 else 2 * line(k - 1) + c

    slices = o_recv.shape[1]
    share = quarter // slices

    def o_rows(which, i):
        return pl.ds(pl.multiple_of(which * quarter + i * share, share), share)

    def o_piece(which, i):
        return wo.at[1 - m, o_rows(which, i), :]

    def o_across(i):
        return remote(
            o_ref.at[o_rows(q0, i), pl.ds(pl.multiple_of((1 - m) * width, width), width)],
            wo.at[m, o_rows(q0, i), :], o_send.at[0, i], o_recv.at[q0, i], mp=1 - m)

    def o_share(i):
        return remote(o_piece(q0, i), o_piece(q0, i), o_send.at[1, i], o_recv.at[q0, i], dp=1 - d)

    def o_core(which, i, slot):
        return remote(o_piece(which, i), o_piece(which, i), o_send.at[slot, i],
                      o_recv.at[which, i], frame=other_core)

    def forward_o(i):
        with scope("o_0"):
            arrived(o_piece(q0, i), o_recv.at[q0, i])
        o_share(i).start()
        o_core(q0, i, 2).start()

    def attn_block(which, owner, h):
        group = (owner // 4) * 2 + owner % 2
        clip = (owner // 2) % 2
        return heads.at[which, h, pl.ds(pl.multiple_of(clip * spots, spots), spots),
                        pl.ds(pl.multiple_of(group * HS, HS), HS)]

    def a_direct(h, k):
        target = (f + k) % frames
        return remote(abuf.at[h, target], attn_block(m, f, h), a_send.at[h, k], a_recv.at[h, f],
                      frame=target)

    def a_own(h):
        return pltpu.make_async_copy(abuf.at[h, f], attn_block(m, f, h), a_recv.at[h, f])

    def a_across(h, k):
        owner = (f + k) % frames
        block = attn_block(m, owner, h)
        return remote(block, block, e_send.at[h, k], e_recv.at[h, owner], mp=1 - m)

    def forward_attn(h):
        @pl.loop(0, frames)
        def _(k):
            owner = (f + k) % frames
            arrived(attn_block(m, owner, h), a_recv.at[h, owner])
            a_across(h, k).start()

    barrier = pltpu.get_barrier_semaphore()
    count = frames * dps
    me = f * dps + d

    def peer(shift):
        other = (me + shift) % count
        return other // dps, other % dps

    for shift in range(1, count):
        frame, dp = peer(shift)
        pl.semaphore_signal(barrier, inc=1, device_id={"frame": frame, "mp": m, "dp": dp},
                            device_id_type=pl.DeviceIdType.MESH)
    pl.semaphore_signal(barrier, inc=1, device_id={"frame": f, "mp": 1 - m, "dp": d},
                        device_id_type=pl.DeviceIdType.MESH)
    loads = [pltpu.make_async_copy(source, target, out_sem.at[i]) for i, (source, target) in enumerate((
        (x_ref, xin), (cot_ref, cot), (act_ref, act),
        (o_ref.at[:, pl.ds(pl.multiple_of(m * width, width), width)], wo.at[m])))]
    own_x = pltpu.make_async_copy(x_ref.at[lo], xbuf.at[m, f], own_sem.at[per_group])
    own_x.start()
    for h in range(per_group):
        w_own(h).start()
    for copy in loads:
        copy.start()
    pl.semaphore_wait(barrier, count)

    last = per_group - 1
    outer = jnp.logical_not(inner)

    def send_tokens(q):
        for k in range(1, lines):
            x_direct(k, q).start()

    def send_weights(h):
        for k in range(4):
            w_direct(h, k).start()

    send_weights(0)
    send_tokens(0)

    @pl.loop(0, slices)
    def _(i):
        o_across(i).start()

    for h in range(per_group):
        w_partner(h).start()

    @pl.loop(0, pieces)
    def _(q):
        x_core(f, x_own(q), m, 0, q).start()

    @pl.loop(0, 2)
    def _(j):
        forward_w(0, j)

    send_tokens(1)

    @pl.when(inner)
    def _():
        @pl.loop(2, 6)
        def _(j):
            forward_w(0, j)

    forward_o(0)
    forward_o(1)

    @pl.when(outer)
    def _():
        forward_w(0, 2)
        forward_w(0, 3)

    forward_o(2)

    def matmul(slot, h, owner, first):
        side = owner // (frames // mps)
        col = pl.multiple_of((owner % (frames // mps)) * depth, depth)
        w = jnp.concatenate([wbuf[h, p, whole_rows(owner), :] for p in range(3)], axis=1)
        step = frames // 2

        @pl.loop(0, 2)
        def _(i):
            x = xbuf[side, pl.ds(i * step, step), :, pl.ds(col, depth)].reshape(step * spots, depth)
            y = jnp.dot(x, w, preferred_element_type=jnp.float32).reshape(step, spots, 3 * HS)

            @pl.when(first)
            def _():
                acc[slot, pl.ds(i * step, step)] = y

            @pl.when(jnp.logical_not(first))
            def _():
                acc[slot, pl.ds(i * step, step)] += y

    def attend_rows(h, i, rows):
        scale = 1.0 / math.sqrt(HS)
        at = pl.ds(pl.multiple_of(i * rows, rows), rows)
        for t in range(frames):
            q = qkv[0, t, at, :].astype(jnp.float32) * scale
            scores = [jnp.sum(q * qkv[1, u, at, :].astype(jnp.float32), axis=-1, keepdims=True)
                      for u in range(t + 1)]
            peak = functools.reduce(jnp.maximum, scores)
            weights = [jnp.exp(s - peak) for s in scores]
            total = functools.reduce(jnp.add, weights)
            accum = functools.reduce(
                jnp.add,
                [w * qkv[2, u, at, :].astype(jnp.float32) for u, w in enumerate(weights)])
            abuf[h, t, at, :] = (accum / total).astype(abuf.dtype)

    def attention(slot, h):
        @pl.loop(0, frames)
        def _(t):
            for p in range(3):
                qkv[p, t] = acc[slot, t, :, p * HS:(p + 1) * HS].astype(qkv.dtype)

        rows = math.gcd(spots, 32)

        @pl.loop(0, spots // rows)
        def _(i):
            with scope("att"):
                attend_rows(h, i, rows)

        a_own(h).start()

        @pl.loop(1, frames)
        def _(k):
            a_direct(h, k).start()

    def ready_w(h, j):
        owner = source_of(j)
        arrived(w_block(h, owner, 1 - d), w_recv.at[h, owner, 1 - d])

    def ready_chip(h):
        w_own(h).wait()
        arrived(wbuf.at[h, :, whole_rows(other_core), :], w_recv.at[h, other_core, 0])

    def ready_w(h, j):
        owner = source_of(j)
        arrived(w_block(h, owner, 1 - d), w_recv.at[h, owner, 1 - d])

    def ready_chip(h):
        w_own(h).wait()
        arrived(wbuf.at[h, :, whole_rows(other_core), :], w_recv.at[h, other_core, 0])

    @pl.loop(0, pieces + 3)
    def _(q):
        @pl.when(q < pieces)
        def _():
            x_across(f, x_own(q), 0, q).start()
            for k in range(1, lines):
                owner = x_owner(k)
                block = x_piece(m, owner, q)
                with scope("x_own"):
                    arrived(block, x_recv.at[m, owner, q])
                x_across(owner, block, k, q).start()
                x_core(owner, block, m, k, q).start()

        @pl.when(q < pieces - 2)
        def _():
            send_tokens(q + 2)

        @pl.when(q == pieces - 2)
        def _():
            send_weights(1)

        @pl.when(q == 0)
        def _():
            forward_o(3)

            @pl.when(outer)
            def _():
                forward_w(0, 4)
                forward_w(0, 5)

        @pl.when(jnp.logical_and(q >= 2, q < pieces + 2))
        def _():
            for k in range(lines):
                owner = x_owner(k)
                block = x_piece(1 - m, owner, q - 2)
                with scope("x_other"):
                    arrived(block, x_recv.at[1 - m, owner, q - 2])
                x_core(owner, block, 1 - m, k, q - 2).start()

        @pl.when(q == 4)
        def _():
            for h in range(2, per_group):
                send_weights(h)

        @pl.when(jnp.logical_and(q >= 4, q < 6))
        def _():
            forward_w(1, 3 * (q - 4))
            forward_w(1, 3 * (q - 4) + 1)
            forward_w(1, 3 * (q - 4) + 2)

        @pl.when(q == 6)
        def _():
            forward_w(2, 0)
            forward_w(2, 1)

        @pl.when(q == 3)
        def _():
            with scope("w_0"):
                own_x.wait()
                ready_chip(0)
                for j in range(6):
                    ready_w(0, j)

        @pl.when(q >= 3)
        def _():
            with scope("x_core"):
                for k in range(lines):
                    owner = x_owner(k) + 1 - 2 * c
                    for which in range(mps):
                        arrived(x_piece(which, owner, q - 3), x_recv.at[which, owner, q - 3])

            @pl.loop(0, mps)
            def _(side):
                with scope("mm0"):
                    matmul(0, 0, side * pieces + q - 3, jnp.logical_and(side == 0, q == 3))

    @pl.loop(0, slices)
    def _(i):
        with scope("o_1"):
            arrived(o_piece(q1, i), o_recv.at[q1, i])
        o_core(q1, i, 3).start()

    attention(0, 0)

    @pl.loop(0, last * frames)
    def _(i):
        h, jj = 1 + i // frames, i % frames

        @pl.when(jnp.logical_and(inner, jnp.logical_and(h < last, jj >= 4)))
        def _():
            forward_w(h + 1, jj - 2)

        @pl.when(jnp.logical_and(outer, jnp.logical_and(h < last, jj >= 6)))
        def _():
            forward_w(h + 1, jj - 4)

        @pl.when(jnp.logical_and(outer, jnp.logical_and(h > 1, jnp.logical_and(jj >= 4, jj < 6))))
        def _():
            forward_w(h, jj)

        @pl.when(jj == 0)
        def _():
            ready_chip(h)

        @pl.when(jj >= 2)
        def _():
            with scope("w_y"):
                ready_w(h, jnp.maximum(jj - 2, 0))

        owner = jnp.where(jj == 0, f, jnp.where(jj == 1, other_core, source_of(jnp.maximum(jj - 2, 0))))
        with scope("mm"):
            matmul(0, h, owner, jj == 0)

        @pl.when(jj == frames - 1)
        def _():
            @pl.when(h == last)
            def _():
                with scope("fa"):
                    forward_attn(last - 1)

            attention(0, h)

        @pl.when(jnp.logical_and(h == last, jj == 3))
        def _():
            for before in range(last - 1):
                with scope("fa"):
                    forward_attn(before)

    @pl.loop(0, slices)
    def _(i):
        for which in (d * 2 + 1 - c, (1 - d) * 2 + 1 - c):
            arrived(o_piece(which, i), o_recv.at[which, i])

    for copy in loads:
        copy.wait()
    clips = x_ref.shape[0]
    groups = heads.shape[3] // HS
    tile = math.gcd(width, 512)
    codes = act.shape[0]
    kinds = book_ref.shape[0]
    index = jnp.concatenate([jnp.full((1, kinds), idx_ref[r], jnp.int32) for r in range(clips)], axis=0)
    onehot = (index == lax.broadcasted_iota(jnp.int32, (clips, kinds), 1)).astype(jnp.float32)
    codevec = jnp.dot(onehot, book_ref[...], precision=lax.Precision.HIGHEST,
                      preferred_element_type=jnp.float32)
    gate[...] = jnp.dot(codevec, act[...], precision=lax.Precision.HIGHEST,
                        preferred_element_type=jnp.float32)
    terms[me, :, width:] = jnp.concatenate(
        [codevec, jnp.zeros((clips, HS - codes), jnp.float32)], axis=1)

    def partial(h, side, cols):
        w = jnp.concatenate(
            [wo[side, pl.ds(pl.multiple_of((g * per_group + h) * HS, HS), HS), cols]
             for g in range(groups)], axis=0)
        return jnp.dot(heads[side, h], w, preferred_element_type=jnp.float32)

    def tile_of(n):
        return pl.ds(pl.multiple_of(n * tile, tile), tile)

    def exchanged(h):
        @pl.loop(0, frames)
        def _(k):
            owner = (f + k) % frames
            arrived(attn_block(1 - m, owner, h), e_recv.at[h, owner])

    @pl.loop(0, last)
    def _(h):
        with scope("exchanged"):
            exchanged(h)

        @pl.loop(0, width // tile)
        def _(n):
            cols = tile_of(n)
            y = partial(h, 0, cols) + partial(h, 1, cols)

            @pl.when(h == 0)
            def _():
                total[:, cols] = y

            @pl.when(h > 0)
            def _():
                total[:, cols] += y

    with scope("fa"):
        forward_attn(last)

    @pl.loop(0, width // tile)
    def _(n):
        cols = tile_of(n)
        total[:, cols] += partial(last, m, cols)

    with scope("exchanged"):
        exchanged(last)

    @pl.loop(0, width // tile)
    def _(n):
        cols = tile_of(n)
        y = total[:, cols] + partial(last, 1 - m, cols)
        for r in range(clips):
            mixed = y[r * spots:(r + 1) * spots]
            factor = gate[r:r + 1, cols]
            xin[r, :, cols] = (xin[r, :, cols].astype(jnp.float32) + factor * mixed).astype(xin.dtype)
            terms[me, r:r + 1, cols] = jnp.sum(
                cot[r, :, cols].astype(jnp.float32) * mixed, axis=0, keepdims=True)

    def t_copy(shift):
        frame, dp = peer(shift)
        return remote(terms.at[me], terms.at[me], t_send.at[shift], t_recv.at[me],
                      frame=frame, dp=dp)

    for shift in range(1, count):
        t_copy(shift).start()
    result = pltpu.make_async_copy(xin, next_ref, out_sem.at[0])
    result.start()

    @pl.loop(0, slices)
    def _(i):
        for copy in (o_across(i), o_share(i), o_core(q0, i, 2), o_core(q1, i, 3)):
            copy.wait_send()

    @pl.loop(0, pieces)
    def _(q):
        for k in range(1, lines):
            x_direct(k, q).wait_send()
        for k in range(lines):
            owner = x_owner(k)
            block = x_piece(m, owner, q)
            x_across(owner, block, k, q).wait_send()
            x_core(owner, block, m, k, q).wait_send()
            x_core(owner, x_piece(1 - m, owner, q), 1 - m, k, q).wait_send()

    @pl.loop(0, per_group)
    def _(h):
        for k in range(4):
            w_direct(h, k).wait_send()
        w_partner(h).wait_send()
        for j in range(6):
            w_share(h, j).wait_send()

        @pl.when(inner)
        def _():
            for j in range(2, 6):
                w_relay(h, j).wait_send()

        @pl.loop(1, frames)
        def _(k):
            a_direct(h, k).wait_send()

        @pl.loop(0, frames)
        def _(k):
            a_across(h, k).wait_send()

    with scope("terms"):
        for shift in range(1, count):
            t_copy(shift).wait_send()
            frame, dp = peer(shift)
            other = frame * dps + dp
            arrived(terms.at[other], t_recv.at[other])
    for i in range(count):
        table[clips * i:clips * (i + 1), :] = terms[i]
    code_columns = table[:, width:].T[:codes]

    @pl.loop(0, width // tile)
    def _(n):
        cols = tile_of(n)
        act[:, cols] = jnp.dot(code_columns, table[:, cols], precision=lax.Precision.HIGHEST,
                               preferred_element_type=jnp.float32)

    gradient = pltpu.make_async_copy(act, grad_ref, out_sem.at[1])
    gradient.start()
    gradient.wait()
    result.wait()


def fused(dps, xin, w_parts, w_out, cotangent, act_proj, codebook, action_idx, frames):
    clips, spots, width = xin.shape
    parts, depth, heads_width = w_parts.shape
    groups = frames // clips
    per_group = heads_width // HS // groups
    count = frames * dps
    any_spec = pl.BlockSpec(memory_space=pl.ANY)
    dma = pltpu.SemaphoreType.DMA
    return pl.pallas_call(
        functools.partial(fused_kernel, dps),
        in_specs=[any_spec] * 5 + [pl.BlockSpec(memory_space=pltpu.VMEM),
                                   pl.BlockSpec(memory_space=pltpu.SMEM)],
        out_specs=[any_spec] * 2,
        out_shape=[
            jax.ShapeDtypeStruct(xin.shape, xin.dtype),
            jax.ShapeDtypeStruct(act_proj.shape, jnp.float32),
        ],
        scratch_shapes=[
            pltpu.VMEM((2, frames, spots, width), jnp.bfloat16),
            pltpu.VMEM((per_group, parts, depth * frames, HS), jnp.bfloat16),
            pltpu.VMEM((1, frames, spots, parts * HS), jnp.float32),
            pltpu.VMEM((parts, frames, spots, HS), jnp.bfloat16),
            pltpu.VMEM((per_group, frames, spots, HS), jnp.bfloat16),
            pltpu.VMEM((2, per_group, clips * spots, groups * HS), jnp.bfloat16),
            pltpu.VMEM((2, heads_width, width), jnp.bfloat16),
            pltpu.VMEM((clips * spots, width), jnp.float32),
            pltpu.VMEM(xin.shape, jnp.bfloat16),
            pltpu.VMEM(xin.shape, jnp.bfloat16),
            pltpu.VMEM(act_proj.shape, jnp.float32),
            pltpu.VMEM((clips, width), jnp.float32),
            pltpu.VMEM((count, clips, width + HS), jnp.float32),
            pltpu.VMEM((count * clips, width + HS), jnp.float32),
            dma((2, frames, frames // 2)), dma((16, frames // 2)),
            dma((per_group, frames, 2)), dma((per_group, 15)),
            dma((4, 4)), dma((4, 4)),
            dma((per_group, frames)), dma((per_group, frames)),
            dma((per_group, frames)), dma((per_group, frames)),
            dma((per_group + 1,)), dma((count,)), dma((count,)), dma((4,)),
        ],
        compiler_params=pltpu.CompilerParams(
            collective_id=2, has_side_effects=True, vmem_limit_bytes=63 << 20),
        name="fused",
    )(xin, w_parts, w_out, cotangent, act_proj, codebook, action_idx)


def gather_mp(block, size):
    if size != 2:
        return lax.all_gather(block, "mp", axis=block.ndim - 1, tiled=True)
    other = lax.ppermute(block, "mp", [(0, 1), (1, 0)])
    first = lax.axis_index("mp") == 0
    return jnp.concatenate(
        [jnp.where(first, block, other), jnp.where(first, other, block)], axis=-1
    )


def fits_fused(mps, dps, frames, clips, spots, width, depth, heads_width):
    groups = frames // clips
    return (mps == dps == clips == 2 and frames == groups * clips and groups == 2 * clips
            and heads_width == 3 * groups * HS
            and spots % 32 == 0 and depth % HS == 0
            and width * mps == depth * frames and heads_width % (16 * 16) == 0)


def body(mp_size, dp_size, tokens, token_mask, mask_embed, w_qkv, w_out, action_idx, codebook,
         act_proj, cotangent):
    clips, _, spots, width = tokens.shape
    heads_width = w_qkv.shape[2]
    depth = w_qkv.shape[0]
    xin = jnp.where(token_mask[..., None] == 1, mask_embed, tokens)
    frames = lax.axis_size("frame")
    if fits_fused(mp_size, dp_size, frames, clips, spots, width, depth, heads_width):
        next_state, grad_proj = fused(
            dp_size, xin.reshape(clips, spots, width), w_qkv.transpose(1, 0, 2), w_out,
            cotangent.reshape(clips, spots, width), act_proj, codebook,
            action_idx.reshape(clips), frames)
        return (next_state.reshape(clips, 1, spots, width), grad_proj)
    else:
        share = depth // dp_size
        mine = lax.dynamic_slice_in_dim(
            w_qkv.reshape(depth, 3 * heads_width), lax.axis_index("dp") * share, share, axis=0
        )
        weights = lax.all_gather(mine, ("frame", "dp"), axis=0, tiled=True)
        if mp_size == 2:
            my_mp = lax.axis_index("mp")
            out_mine = lax.dynamic_slice_in_dim(w_out, my_mp * width, width, axis=1)
            out_other = lax.ppermute(
                lax.dynamic_slice_in_dim(w_out, (1 - my_mp) * width, width, axis=1),
                "mp", [(0, 1), (1, 0)])
        spread = lax.all_to_all(
            xin.reshape(clips, spots, width), "frame", split_axis=1, concat_axis=0, tiled=True
        )
        frames = spread.shape[0] // clips
        local = spread.shape[1]
        features = gather_mp(spread.reshape(frames * clips * local, width), mp_size)
        qkv = jnp.dot(features, weights, preferred_element_type=jnp.float32).astype(jnp.bfloat16)
        attn = attend(qkv.reshape(frames, clips * local, 3 * heads_width), frames, heads_width)
        back = lax.all_to_all(
            attn.reshape(frames * clips, local, heads_width), "frame", split_axis=0, concat_axis=1,
            tiled=True,
        )
        heads = back.reshape(clips * spots, heads_width)
        if mp_size == 2:
            other_heads = lax.ppermute(heads, "mp", [(0, 1), (1, 0)])
            mixed_rows = jnp.dot(heads, out_mine, preferred_element_type=jnp.float32) + jnp.dot(
                other_heads, out_other, preferred_element_type=jnp.float32)
        else:
            out_block = lax.all_to_all(w_out, "mp", split_axis=1, concat_axis=0, tiled=True)
            mixed_rows = jnp.dot(gather_mp(heads, mp_size), out_block,
                                 preferred_element_type=jnp.float32)
    mixed = mixed_rows.reshape(clips, 1, spots, width)
    onehot = (
        action_idx.reshape(clips)[:, None] == jnp.arange(codebook.shape[0])[None, :]
    ).astype(jnp.float32)
    codevec = jnp.dot(onehot, codebook, precision=lax.Precision.HIGHEST)
    gate = jnp.dot(codevec, act_proj, precision=lax.Precision.HIGHEST)
    next_state = (xin.astype(jnp.float32) + gate[:, None, None, :] * mixed).astype(jnp.bfloat16)
    dgate = jnp.sum(cotangent.astype(jnp.float32) * mixed, axis=2).reshape(clips, width)
    codes = codevec.shape[1]
    padded = jnp.pad(codevec, ((0, 0), (0, -codes % 128)))
    terms = spread_terms(jnp.concatenate([dgate, padded], axis=1), frames, dp_size)
    terms = terms.reshape(frames * dp_size * clips, -1)
    grad_proj = jnp.dot(
        terms[:, width : width + codes].T, terms[:, :width], precision=lax.Precision.HIGHEST)
    return (next_state, grad_proj)


def solution(mesh):
    in_specs = (
        P("dp", "frame", None, "mp"),
        P("dp", "frame", None),
        P("mp"),
        P("frame", None, "mp"),
        P("mp", None),
        P("dp", "frame"),
        P(),
        P(None, "mp"),
        P("dp", "frame", None, "mp"),
    )
    out_specs = (P("dp", "frame", None, "mp"), P(None, "mp"))
    return jax.shard_map(
        functools.partial(body, mesh.shape["mp"], mesh.shape["dp"]),
        mesh=mesh, in_specs=in_specs, out_specs=out_specs, check_vma=False,
    )
```

```python
import functools
import math

import jax
import jax.numpy as jnp
from jax import lax
from jax.experimental import pallas as pl
from jax.experimental.pallas import tpu as pltpu
from jax.sharding import PartitionSpec as P

HS = 128


def attend_kernel(frames, q_ref, k_ref, v_ref, o_ref):
    scale = 1.0 / math.sqrt(HS)
    for t in range(frames):
        q = q_ref[t].astype(jnp.float32) * scale
        scores = [
            jnp.sum(q * k_ref[u].astype(jnp.float32), axis=-1, keepdims=True) for u in range(t + 1)
        ]
        peak = functools.reduce(jnp.maximum, scores)
        weights = [jnp.exp(s - peak) for s in scores]
        total = functools.reduce(jnp.add, weights)
        accum = functools.reduce(
            jnp.add, [w * v_ref[u].astype(jnp.float32) for u, w in enumerate(weights)]
        )
        o_ref[t] = (accum / total).astype(o_ref.dtype)


def attend(qkv, frames, heads_width):
    rows = qkv.shape[1]
    heads = heads_width // HS
    spec = lambda part: pl.BlockSpec((frames, rows, HS), lambda h, part=part: (0, 0, part * heads + h))
    return pl.pallas_call(
        functools.partial(attend_kernel, frames),
        grid=(heads,),
        in_specs=[spec(0), spec(1), spec(2)],
        out_specs=spec(0),
        out_shape=jax.ShapeDtypeStruct((frames, rows, heads_width), jnp.bfloat16),
        cost_estimate=pl.CostEstimate(flops=4 * frames * frames * rows * heads_width,
                                      bytes_accessed=8 * frames * rows * heads_width,
                                      transcendentals=0),
        name="attend",
    )(qkv, qkv, qkv)


def spread_kernel(frames, dps, x_ref, o_ref, send_sem, recv_sem, own_sem):
    count = frames * dps
    me = lax.axis_index("frame") * dps + lax.axis_index("dp")
    barrier = pltpu.get_barrier_semaphore()

    def peer(shift):
        other = lax.rem(me + shift, count)
        return {"frame": other // dps, "dp": lax.rem(other, dps)}

    for shift in range(1, count):
        pl.semaphore_signal(barrier, inc=1, device_id=peer(shift),
                            device_id_type=pl.DeviceIdType.MESH)
    own = pltpu.make_async_copy(x_ref, o_ref.at[me], own_sem)
    own.start()
    pl.semaphore_wait(barrier, count - 1)
    copies = []
    for shift in range(1, count):
        copy = pltpu.make_async_remote_copy(
            src_ref=x_ref, dst_ref=o_ref.at[me], send_sem=send_sem.at[shift],
            recv_sem=recv_sem.at[shift], device_id=peer(shift),
            device_id_type=pl.DeviceIdType.MESH)
        copy.start()
        copies.append(copy)
    own.wait()
    for copy in copies:
        copy.wait()


def spread_terms(terms, frames, dps):
    count = frames * dps
    return pl.pallas_call(
        functools.partial(spread_kernel, frames, dps),
        in_specs=[pl.BlockSpec(memory_space=pltpu.VMEM)],
        out_specs=pl.BlockSpec(memory_space=pltpu.VMEM),
        out_shape=jax.ShapeDtypeStruct((count, *terms.shape), terms.dtype),
        scratch_shapes=[pltpu.SemaphoreType.DMA((count,)), pltpu.SemaphoreType.DMA((count,)),
                        pltpu.SemaphoreType.DMA],
        compiler_params=pltpu.CompilerParams(collective_id=1, has_side_effects=True),
        name="spread_terms",
    )(terms)


scope = jax.named_scope


def fused_kernel(dps, tokens_ref, mask_ref, embed_ref, w_ref, o_ref, cot_ref, act_ref, book_ref, idx_ref, next_ref, grad_ref,
                 xbuf, wbuf, acc, qkv, abuf, heads, wo, total, xin, cot, act, gate, terms, table, after,
                 x_recv, x_send, w_recv, w_send, o_recv, o_send, a_recv, a_send, e_recv, e_send,
                 own_sem, t_recv, t_send, out_sem):
    mps, frames, spots, width = xbuf.shape
    per_group, _, _, _ = wbuf.shape
    depth = w_ref.shape[1]
    lines = frames // 2
    half = lines // 2
    part = depth // 2
    quarter = o_ref.shape[0] // 4
    f, m, d = lax.axis_index("frame"), lax.axis_index("mp"), lax.axis_index("dp")
    z, c = f // 2, f % 2
    hi, lo = z // 2, z % 2
    mine = hi * 2 + c
    inner = hi != lo
    pair, near, far = z + 1 - 2 * lo, half - hi, (lines - 1) * (1 - hi)
    other_core = 2 * z + 1 - c
    q0, q1 = d * 2 + c, (1 - d) * 2 + c

    def remote(source, target, send_sem, recv_sem, frame=f, mp=m, dp=d):
        return pltpu.make_async_remote_copy(
            src_ref=source, dst_ref=target, send_sem=send_sem, recv_sem=recv_sem,
            device_id={"frame": frame, "mp": mp, "dp": dp},
            device_id_type=pl.DeviceIdType.MESH)

    def arrived(target, recv_sem):
        pltpu.make_async_copy(target, target, recv_sem).wait()

    def rows_of(owner, which):
        return pl.ds(pl.multiple_of(owner * depth + which * part, part), part)

    def whole_rows(owner):
        return pl.ds(pl.multiple_of(owner * depth, depth), depth)

    def columns(group, head):
        return pl.ds(pl.multiple_of((group * per_group + head) * HS, HS), HS)

    def line(j):
        return jnp.where(j == 0, pair, jnp.where(j == 1, near, far))

    def source_of(j):
        return 2 * line(j // 2) + j % 2

    def w_direct(h, k):
        target = jnp.where(k < 2, pair, near)
        group = jnp.where(k < 2, hi, 1 - hi) * 2 + k % 2
        return remote(w_ref.at[:, pl.ds(pl.multiple_of(d * part, part), part), columns(group, h)],
                      wbuf.at[h, :, rows_of(f, d), :], w_send.at[h, k], w_recv.at[h, f, d],
                      frame=2 * target + k % 2)

    def w_partner(h):
        return remote(w_ref.at[:, :, columns(hi * 2 + 1 - c, h)], wbuf.at[h, :, whole_rows(f), :],
                      w_send.at[h, 4], w_recv.at[h, f, 0], frame=other_core)

    def w_own(h):
        return pltpu.make_async_copy(w_ref.at[:, :, columns(mine, h)],
                                     wbuf.at[h, :, whole_rows(f), :], own_sem.at[h])

    def w_block(h, owner, which):
        return wbuf.at[h, :, rows_of(owner, which), :]

    def w_share(h, j):
        owner = source_of(j)
        block = w_block(h, owner, d)
        return remote(block, block, w_send.at[h, 5 + j], w_recv.at[h, owner, d], dp=1 - d)

    def w_relay(h, j):
        owner = source_of(j)
        block = w_block(h, owner, d)
        return remote(block, block, w_send.at[h, 9 + j], w_recv.at[h, owner, d],
                      frame=2 * pair + c)

    def forward_w(h, j):
        owner = source_of(j)
        with scope("fw"):
            arrived(w_block(h, owner, d), w_recv.at[h, owner, d])

        @pl.when(jnp.logical_and(inner, j >= 2))
        def _():
            w_relay(h, j).start()

        w_share(h, j).start()

    pieces = frames // mps

    def features(q):
        return pl.ds(pl.multiple_of(q * depth, depth), depth)

    def x_piece(which, owner, q):
        return xbuf.at[which, owner, :, features(q)]

    def x_direct(k, q):
        target = (z + k) % lines
        return remote(xin.at[target % 2, :, features(q)], x_piece(m, f, q), x_send.at[k, q],
                      x_recv.at[m, f, q], frame=2 * target + c)

    def x_across(owner, source, k, q):
        return remote(source, x_piece(m, owner, q), x_send.at[4 + k, q], x_recv.at[m, owner, q],
                      mp=1 - m)

    def x_core(owner, source, which, k, q):
        slot = jnp.where(which == m, 8, 12)
        return remote(source, x_piece(which, owner, q), x_send.at[slot + k, q],
                      x_recv.at[which, owner, q], frame=other_core)

    def x_own(q):
        return xin.at[lo, :, features(q)]

    def x_owner(k):
        return f if k == 0 else 2 * line(k - 1) + c

    slices = o_recv.shape[1]
    share = quarter // slices

    def o_rows(which, i):
        return pl.ds(pl.multiple_of(which * quarter + i * share, share), share)

    def o_piece(which, i):
        return wo.at[1 - m, o_rows(which, i), :]

    def o_across(i):
        return remote(
            o_ref.at[o_rows(q0, i), pl.ds(pl.multiple_of((1 - m) * width, width), width)],
            wo.at[m, o_rows(q0, i), :], o_send.at[0, i], o_recv.at[q0, i], mp=1 - m)

    def o_share(i):
        return remote(o_piece(q0, i), o_piece(q0, i), o_send.at[1, i], o_recv.at[q0, i], dp=1 - d)

    def o_core(which, i, slot):
        return remote(o_piece(which, i), o_piece(which, i), o_send.at[slot, i],
                      o_recv.at[which, i], frame=other_core)

    def forward_o(i):
        with scope("o_0"):
            arrived(o_piece(q0, i), o_recv.at[q0, i])
        o_share(i).start()
        o_core(q0, i, 2).start()

    def attn_block(which, owner, h):
        group = (owner // 4) * 2 + owner % 2
        clip = (owner // 2) % 2
        return heads.at[which, h, pl.ds(pl.multiple_of(clip * spots, spots), spots),
                        pl.ds(pl.multiple_of(group * HS, HS), HS)]

    def a_direct(h, k):
        target = (f + k) % frames
        return remote(abuf.at[h, target], attn_block(m, f, h), a_send.at[h, k], a_recv.at[h, f],
                      frame=target)

    def a_own(h):
        return pltpu.make_async_copy(abuf.at[h, f], attn_block(m, f, h), a_recv.at[h, f])

    def a_across(h, k):
        owner = (f + frames - k) % frames
        block = attn_block(m, owner, h)
        return remote(block, block, e_send.at[h, k], e_recv.at[h, owner], mp=1 - m)

    def forward_attn(h):
        @pl.loop(0, frames)
        def _(k):
            owner = (f + frames - k) % frames
            arrived(attn_block(m, owner, h), a_recv.at[h, owner])
            a_across(h, k).start()

    barrier = pltpu.get_barrier_semaphore()
    clips = xin.shape[0]
    tile = math.gcd(width, 512)

    def tile_of(n):
        return pl.ds(pl.multiple_of(n * tile, tile), tile)

    count = frames * dps
    me = f * dps + d

    def peer(shift):
        other = (me + shift) % count
        return other // dps, other % dps

    for shift in range(1, count):
        frame, dp = peer(shift)
        pl.semaphore_signal(barrier, inc=1, device_id={"frame": frame, "mp": m, "dp": dp},
                            device_id_type=pl.DeviceIdType.MESH)
    pl.semaphore_signal(barrier, inc=1, device_id={"frame": f, "mp": 1 - m, "dp": d},
                        device_id_type=pl.DeviceIdType.MESH)
    loads = [pltpu.make_async_copy(source, target, out_sem.at[i]) for i, (source, target) in enumerate((
        (tokens_ref, xin), (cot_ref, cot), (act_ref, act),
        (o_ref.at[:, pl.ds(pl.multiple_of(m * width, width), width)], wo.at[m])))]
    own_x = pltpu.make_async_copy(xin.at[lo], xbuf.at[m, f], own_sem.at[per_group])
    for h in range(per_group):
        w_own(h).start()
    for copy in loads:
        copy.start()
    loads[0].wait()
    same = (lax.broadcasted_iota(jnp.int32, (spots, spots), 0)
            == lax.broadcasted_iota(jnp.int32, (spots, spots), 1))
    for r in range(clips):
        row = jnp.broadcast_to(mask_ref[r].astype(jnp.float32), (spots, spots))
        masked = jnp.sum(jnp.where(same, row, 0.0), axis=1, keepdims=True) == 1.0

        @pl.loop(0, width // tile)
        def _(n):
            cols = tile_of(n)
            xin[r, :, cols] = jnp.where(masked, embed_ref[:, cols].astype(jnp.float32),
                                        xin[r, :, cols].astype(jnp.float32)).astype(xin.dtype)

    own_x.start()
    pl.semaphore_wait(barrier, count)

    last = per_group - 1
    outer = jnp.logical_not(inner)

    def send_tokens(q):
        for k in range(1, lines):
            x_direct(k, q).start()

    def send_weights(h):
        for k in range(4):
            w_direct(h, k).start()

    send_weights(0)
    send_tokens(0)

    @pl.loop(0, slices)
    def _(i):
        o_across(i).start()

    for h in range(per_group):
        w_partner(h).start()

    @pl.loop(0, pieces)
    def _(q):
        x_core(f, x_own(q), m, 0, q).start()

    @pl.loop(0, 2)
    def _(j):
        forward_w(0, j)

    send_tokens(1)

    @pl.when(inner)
    def _():
        @pl.loop(2, 6)
        def _(j):
            forward_w(0, j)

    forward_o(0)
    forward_o(1)

    @pl.when(outer)
    def _():
        forward_w(0, 2)
        forward_w(0, 3)

    forward_o(2)

    def matmul(slot, h, owner, first):
        side = owner // (frames // mps)
        col = pl.multiple_of((owner % (frames // mps)) * depth, depth)
        w = jnp.concatenate([wbuf[h, p, whole_rows(owner), :] for p in range(3)], axis=1)
        step = frames // 2

        @pl.loop(0, 2)
        def _(i):
            x = xbuf[side, pl.ds(i * step, step), :, pl.ds(col, depth)].reshape(step * spots, depth)
            y = jnp.dot(x, w, preferred_element_type=jnp.float32).reshape(step, spots, 3 * HS)

            @pl.when(first)
            def _():
                acc[slot, pl.ds(i * step, step)] = y

            @pl.when(jnp.logical_not(first))
            def _():
                acc[slot, pl.ds(i * step, step)] += y

    def attend_rows(h, i, rows):
        scale = 1.0 / math.sqrt(HS)
        at = pl.ds(pl.multiple_of(i * rows, rows), rows)
        for t in range(frames):
            q = qkv[0, t, at, :].astype(jnp.float32) * scale
            scores = [jnp.sum(q * qkv[1, u, at, :].astype(jnp.float32), axis=-1, keepdims=True)
                      for u in range(t + 1)]
            peak = functools.reduce(jnp.maximum, scores)
            weights = [jnp.exp(s - peak) for s in scores]
            total = functools.reduce(jnp.add, weights)
            accum = functools.reduce(
                jnp.add,
                [w * qkv[2, u, at, :].astype(jnp.float32) for u, w in enumerate(weights)])
            abuf[h, t, at, :] = (accum / total).astype(abuf.dtype)

    def attention(slot, h):
        @pl.loop(0, frames)
        def _(t):
            for p in range(3):
                qkv[p, t] = acc[slot, t, :, p * HS:(p + 1) * HS].astype(qkv.dtype)

        rows = math.gcd(spots, 32)

        @pl.loop(0, spots // rows)
        def _(i):
            with scope("att"):
                attend_rows(h, i, rows)

        a_own(h).start()

        @pl.loop(1, frames)
        def _(k):
            a_direct(h, k).start()

    def ready_w(h, j):
        owner = source_of(j)
        arrived(w_block(h, owner, 1 - d), w_recv.at[h, owner, 1 - d])

    def ready_chip(h):
        w_own(h).wait()
        arrived(wbuf.at[h, :, whole_rows(other_core), :], w_recv.at[h, other_core, 0])

    def ready_w(h, j):
        owner = source_of(j)
        arrived(w_block(h, owner, 1 - d), w_recv.at[h, owner, 1 - d])

    def ready_chip(h):
        w_own(h).wait()
        arrived(wbuf.at[h, :, whole_rows(other_core), :], w_recv.at[h, other_core, 0])

    @pl.loop(0, pieces + 3)
    def _(q):
        @pl.when(q < pieces)
        def _():
            x_across(f, x_own(q), 0, q).start()
            for k in range(1, lines):
                owner = x_owner(k)
                block = x_piece(m, owner, q)
                with scope("x_own"):
                    arrived(block, x_recv.at[m, owner, q])
                x_across(owner, block, k, q).start()
                x_core(owner, block, m, k, q).start()

        @pl.when(q < pieces - 2)
        def _():
            send_tokens(q + 2)

        @pl.when(q == pieces - 2 - jnp.where(outer, 1, 0))
        def _():
            send_weights(1)

        @pl.when(q == 0)
        def _():
            forward_o(3)

            @pl.when(outer)
            def _():
                forward_w(0, 4)
                forward_w(0, 5)

        @pl.when(jnp.logical_and(q >= 2, q < pieces + 2))
        def _():
            for k in range(lines):
                owner = x_owner(k)
                block = x_piece(1 - m, owner, q - 2)
                with scope("x_other"):
                    arrived(block, x_recv.at[1 - m, owner, q - 2])
                x_core(owner, block, 1 - m, k, q - 2).start()

        @pl.when(q == 4)
        def _():
            for h in range(2, per_group):
                send_weights(h)

        @pl.when(jnp.logical_and(q >= 4, q < 6))
        def _():
            forward_w(1, 3 * (q - 4))
            forward_w(1, 3 * (q - 4) + 1)
            forward_w(1, 3 * (q - 4) + 2)

        @pl.when(q == 6)
        def _():
            forward_w(2, 0)
            forward_w(2, 1)

        @pl.when(q == 3)
        def _():
            with scope("w_0"):
                own_x.wait()
                ready_chip(0)
                for j in range(6):
                    ready_w(0, j)

        @pl.when(q >= 3)
        def _():
            with scope("x_core"):
                for k in range(lines):
                    owner = x_owner(k) + 1 - 2 * c
                    for which in range(mps):
                        arrived(x_piece(which, owner, q - 3), x_recv.at[which, owner, q - 3])

            @pl.loop(0, mps)
            def _(side):
                with scope("mm0"):
                    matmul(0, 0, side * pieces + q - 3, jnp.logical_and(side == 0, q == 3))

    @pl.loop(0, slices)
    def _(i):
        with scope("o_1"):
            arrived(o_piece(q1, i), o_recv.at[q1, i])
        o_core(q1, i, 3).start()

    attention(0, 0)

    @pl.loop(0, last * frames)
    def _(i):
        h, jj = 1 + i // frames, i % frames

        @pl.when(jnp.logical_and(inner, jnp.logical_and(h < last, jj >= 4)))
        def _():
            forward_w(h + 1, jj - 2)

        @pl.when(jnp.logical_and(outer, jnp.logical_and(h < last, jj >= 6)))
        def _():
            forward_w(h + 1, jj - 4)

        @pl.when(jnp.logical_and(outer, jnp.logical_and(h > 1, jnp.logical_and(jj >= 4, jj < 6))))
        def _():
            forward_w(h, jj)

        @pl.when(jj == 0)
        def _():
            ready_chip(h)

        @pl.when(jj >= 2)
        def _():
            with scope("w_y"):
                ready_w(h, jnp.maximum(jj - 2, 0))

        owner = jnp.where(jj == 0, f, jnp.where(jj == 1, other_core, source_of(jnp.maximum(jj - 2, 0))))
        with scope("mm"):
            matmul(0, h, owner, jj == 0)

        @pl.when(jj == frames - 1)
        def _():
            attention(0, h)

        @pl.when(jnp.logical_and(h == last, jj == 5))
        def _():
            with scope("fa"):
                forward_attn(last - 1)

        @pl.when(jnp.logical_and(h == last, jj == 3))
        def _():
            for before in range(last - 1):
                with scope("fa"):
                    forward_attn(before)

    @pl.loop(0, slices)
    def _(i):
        for which in (d * 2 + 1 - c, (1 - d) * 2 + 1 - c):
            arrived(o_piece(which, i), o_recv.at[which, i])

    for copy in loads[1:]:
        copy.wait()
    groups = heads.shape[3] // HS
    codes = act.shape[0]
    kinds = book_ref.shape[0]
    index = jnp.concatenate([jnp.full((1, kinds), idx_ref[r], jnp.int32) for r in range(clips)], axis=0)
    onehot = (index == lax.broadcasted_iota(jnp.int32, (clips, kinds), 1)).astype(jnp.float32)
    codevec = jnp.dot(onehot, book_ref[...], precision=lax.Precision.HIGHEST,
                      preferred_element_type=jnp.float32)
    gate[...] = jnp.dot(codevec, act[...], precision=lax.Precision.HIGHEST,
                        preferred_element_type=jnp.float32)
    terms[me, :, width:] = jnp.concatenate(
        [codevec, jnp.zeros((clips, HS - codes), jnp.float32)], axis=1)

    def partial(h, side, cols):
        w = jnp.concatenate(
            [wo[side, pl.ds(pl.multiple_of((g * per_group + h) * HS, HS), HS), cols]
             for g in range(groups)], axis=0)
        return jnp.dot(heads[side, h], w, preferred_element_type=jnp.float32)

    def exchanged(h):
        @pl.loop(0, frames)
        def _(k):
            owner = (f + k) % frames
            arrived(attn_block(1 - m, owner, h), e_recv.at[h, owner])

    @pl.loop(0, last)
    def _(h):
        @pl.when(h == last - 1)
        def _():
            with scope("fa"):
                forward_attn(last)

        with scope("exchanged"):
            exchanged(h)

        @pl.loop(0, width // tile)
        def _(n):
            cols = tile_of(n)
            y = partial(h, 0, cols) + partial(h, 1, cols)

            @pl.when(h == 0)
            def _():
                total[:, cols] = y

            @pl.when(h > 0)
            def _():
                total[:, cols] += y

    @pl.loop(0, width // tile)
    def _(n):
        cols = tile_of(n)
        total[:, cols] += partial(last, m, cols)

    with scope("exchanged"):
        exchanged(last)

    @pl.loop(0, width // tile)
    def _(n):
        cols = tile_of(n)
        y = total[:, cols] + partial(last, 1 - m, cols)
        for r in range(clips):
            mixed = y[r * spots:(r + 1) * spots]
            factor = gate[r:r + 1, cols]
            after[r, :, cols] = (
                xin[r, :, cols].astype(jnp.float32) + factor * mixed).astype(xin.dtype)
            terms[me, r:r + 1, cols] = jnp.sum(
                cot[r, :, cols].astype(jnp.float32) * mixed, axis=0, keepdims=True)

    def t_copy(shift):
        frame, dp = peer(shift)
        return remote(terms.at[me], terms.at[me], t_send.at[shift], t_recv.at[me],
                      frame=frame, dp=dp)

    for shift in range(1, count):
        t_copy(shift).start()
    result = pltpu.make_async_copy(after, next_ref, out_sem.at[0])
    result.start()

    @pl.loop(0, slices)
    def _(i):
        for copy in (o_across(i), o_share(i), o_core(q0, i, 2), o_core(q1, i, 3)):
            copy.wait_send()

    @pl.loop(0, pieces)
    def _(q):
        for k in range(1, lines):
            x_direct(k, q).wait_send()
        for k in range(lines):
            owner = x_owner(k)
            block = x_piece(m, owner, q)
            x_across(owner, block, k, q).wait_send()
            x_core(owner, block, m, k, q).wait_send()
            x_core(owner, x_piece(1 - m, owner, q), 1 - m, k, q).wait_send()

    @pl.loop(0, per_group)
    def _(h):
        for k in range(4):
            w_direct(h, k).wait_send()
        w_partner(h).wait_send()
        for j in range(6):
            w_share(h, j).wait_send()

        @pl.when(inner)
        def _():
            for j in range(2, 6):
                w_relay(h, j).wait_send()

        @pl.loop(1, frames)
        def _(k):
            a_direct(h, k).wait_send()

        @pl.loop(0, frames)
        def _(k):
            a_across(h, k).wait_send()

    with scope("terms"):
        for shift in range(1, count):
            t_copy(shift).wait_send()
            frame, dp = peer(shift)
            other = frame * dps + dp
            arrived(terms.at[other], t_recv.at[other])
    for i in range(count):
        table[clips * i:clips * (i + 1), :] = terms[i]
    code_columns = table[:, width:].T[:codes]

    act[...] = jnp.dot(code_columns, table[:, :width], precision=lax.Precision.HIGHEST,
                       preferred_element_type=jnp.float32)

    gradient = pltpu.make_async_copy(act, grad_ref, out_sem.at[1])
    gradient.start()
    gradient.wait()
    result.wait()


def fused(dps, tokens, mask, embed, w_parts, w_out, cotangent, act_proj, codebook, action_idx, frames):
    clips, spots, width = tokens.shape
    parts, depth, heads_width = w_parts.shape
    groups = frames // clips
    per_group = heads_width // HS // groups
    count = frames * dps
    any_spec = pl.BlockSpec(memory_space=pl.ANY)
    vmem = pl.BlockSpec(memory_space=pltpu.VMEM)
    dma = pltpu.SemaphoreType.DMA
    return pl.pallas_call(
        functools.partial(fused_kernel, dps),
        in_specs=[any_spec, vmem, vmem] + [any_spec] * 4 + [vmem, pl.BlockSpec(memory_space=pltpu.SMEM)],
        out_specs=[any_spec] * 2,
        out_shape=[
            jax.ShapeDtypeStruct(tokens.shape, tokens.dtype),
            jax.ShapeDtypeStruct(act_proj.shape, jnp.float32),
        ],
        scratch_shapes=[
            pltpu.VMEM((2, frames, spots, width), jnp.bfloat16),
            pltpu.VMEM((per_group, parts, depth * frames, HS), jnp.bfloat16),
            pltpu.VMEM((1, frames, spots, parts * HS), jnp.float32),
            pltpu.VMEM((parts, frames, spots, HS), jnp.bfloat16),
            pltpu.VMEM((per_group, frames, spots, HS), jnp.bfloat16),
            pltpu.VMEM((2, per_group, clips * spots, groups * HS), jnp.bfloat16),
            pltpu.VMEM((2, heads_width, width), jnp.bfloat16),
            pltpu.VMEM((clips * spots, width), jnp.float32),
            pltpu.VMEM(tokens.shape, jnp.bfloat16),
            pltpu.VMEM(tokens.shape, jnp.bfloat16),
            pltpu.VMEM(act_proj.shape, jnp.float32),
            pltpu.VMEM((clips, width), jnp.float32),
            pltpu.VMEM((count, clips, width + HS), jnp.float32),
            pltpu.VMEM((count * clips, width + HS), jnp.float32),
            pltpu.VMEM(tokens.shape, jnp.bfloat16),
            dma((2, frames, frames // 2)), dma((16, frames // 2)),
            dma((per_group, frames, 2)), dma((per_group, 15)),
            dma((4, 4)), dma((4, 4)),
            dma((per_group, frames)), dma((per_group, frames)),
            dma((per_group, frames)), dma((per_group, frames)),
            dma((per_group + 1,)), dma((count,)), dma((count,)), dma((4,)),
        ],
        compiler_params=pltpu.CompilerParams(
            collective_id=2, has_side_effects=True, vmem_limit_bytes=60 << 20),
        name="fused",
    )(tokens, mask, embed, w_parts, w_out, cotangent, act_proj, codebook, action_idx)


def finish_kernel(next_ref, grad_ref, next_out, grad_out, rows, grads, load, store):
    copies = []
    for i, (source, middle, target) in enumerate(
            [(next_ref.at[r], rows.at[r], next_out.at[r]) for r in range(rows.shape[0])]
            + [(grad_ref, grads, grad_out)]):
        copies.append((pltpu.make_async_copy(source, middle, load.at[i]),
                       pltpu.make_async_copy(middle, target, store.at[i])))
    for first, _ in copies:
        first.start()
    for first, second in copies:
        first.wait()
        second.start()
    for _, second in copies:
        second.wait()


def finish(next_state, grad_proj):
    any_spec = pl.BlockSpec(memory_space=pl.ANY)
    count = next_state.shape[0] + 1
    return pl.pallas_call(
        finish_kernel,
        in_specs=[any_spec] * 2,
        out_specs=[any_spec] * 2,
        out_shape=[jax.ShapeDtypeStruct(a.shape, a.dtype) for a in (next_state, grad_proj)],
        scratch_shapes=[pltpu.VMEM(next_state.shape, next_state.dtype),
                        pltpu.VMEM(grad_proj.shape, grad_proj.dtype),
                        pltpu.SemaphoreType.DMA((count,)), pltpu.SemaphoreType.DMA((count,))],
        name="finish",
    )(next_state, grad_proj)


def gather_mp(block, size):
    if size != 2:
        return lax.all_gather(block, "mp", axis=block.ndim - 1, tiled=True)
    other = lax.ppermute(block, "mp", [(0, 1), (1, 0)])
    first = lax.axis_index("mp") == 0
    return jnp.concatenate(
        [jnp.where(first, block, other), jnp.where(first, other, block)], axis=-1
    )


def fits_fused(mps, dps, frames, clips, spots, width, depth, heads_width):
    groups = frames // clips
    return (mps == dps == clips == 2 and frames == groups * clips and groups == 2 * clips
            and heads_width == 3 * groups * HS
            and spots % 32 == 0 and depth % HS == 0
            and width * mps == depth * frames and heads_width % (16 * 16) == 0)


def body(mp_size, dp_size, tokens, token_mask, mask_embed, w_qkv, w_out, action_idx, codebook,
         act_proj, cotangent):
    clips, _, spots, width = tokens.shape
    heads_width = w_qkv.shape[2]
    depth = w_qkv.shape[0]
    xin = jnp.where(token_mask[..., None] == 1, mask_embed, tokens)
    frames = lax.axis_size("frame")
    if fits_fused(mp_size, dp_size, frames, clips, spots, width, depth, heads_width):
        next_state, grad_proj = fused(
            dp_size, tokens.reshape(clips, spots, width), token_mask, mask_embed.reshape(1, width), w_qkv.transpose(1, 0, 2), w_out,
            cotangent.reshape(clips, spots, width), act_proj, codebook,
            action_idx.reshape(clips), frames)
        next_state, grad_proj = finish(next_state.reshape(2 * clips, spots // 2, width), grad_proj)
        return (next_state.reshape(clips, 1, spots, width), grad_proj)
    else:
        share = depth // dp_size
        mine = lax.dynamic_slice_in_dim(
            w_qkv.reshape(depth, 3 * heads_width), lax.axis_index("dp") * share, share, axis=0
        )
        weights = lax.all_gather(mine, ("frame", "dp"), axis=0, tiled=True)
        if mp_size == 2:
            my_mp = lax.axis_index("mp")
            out_mine = lax.dynamic_slice_in_dim(w_out, my_mp * width, width, axis=1)
            out_other = lax.ppermute(
                lax.dynamic_slice_in_dim(w_out, (1 - my_mp) * width, width, axis=1),
                "mp", [(0, 1), (1, 0)])
        spread = lax.all_to_all(
            xin.reshape(clips, spots, width), "frame", split_axis=1, concat_axis=0, tiled=True
        )
        frames = spread.shape[0] // clips
        local = spread.shape[1]
        features = gather_mp(spread.reshape(frames * clips * local, width), mp_size)
        qkv = jnp.dot(features, weights, preferred_element_type=jnp.float32).astype(jnp.bfloat16)
        attn = attend(qkv.reshape(frames, clips * local, 3 * heads_width), frames, heads_width)
        back = lax.all_to_all(
            attn.reshape(frames * clips, local, heads_width), "frame", split_axis=0, concat_axis=1,
            tiled=True,
        )
        heads = back.reshape(clips * spots, heads_width)
        if mp_size == 2:
            other_heads = lax.ppermute(heads, "mp", [(0, 1), (1, 0)])
            mixed_rows = jnp.dot(heads, out_mine, preferred_element_type=jnp.float32) + jnp.dot(
                other_heads, out_other, preferred_element_type=jnp.float32)
        else:
            out_block = lax.all_to_all(w_out, "mp", split_axis=1, concat_axis=0, tiled=True)
            mixed_rows = jnp.dot(gather_mp(heads, mp_size), out_block,
                                 preferred_element_type=jnp.float32)
    mixed = mixed_rows.reshape(clips, 1, spots, width)
    onehot = (
        action_idx.reshape(clips)[:, None] == jnp.arange(codebook.shape[0])[None, :]
    ).astype(jnp.float32)
    codevec = jnp.dot(onehot, codebook, precision=lax.Precision.HIGHEST)
    gate = jnp.dot(codevec, act_proj, precision=lax.Precision.HIGHEST)
    next_state = (xin.astype(jnp.float32) + gate[:, None, None, :] * mixed).astype(jnp.bfloat16)
    dgate = jnp.sum(cotangent.astype(jnp.float32) * mixed, axis=2).reshape(clips, width)
    codes = codevec.shape[1]
    padded = jnp.pad(codevec, ((0, 0), (0, -codes % 128)))
    terms = spread_terms(jnp.concatenate([dgate, padded], axis=1), frames, dp_size)
    terms = terms.reshape(frames * dp_size * clips, -1)
    grad_proj = jnp.dot(
        terms[:, width : width + codes].T, terms[:, :width], precision=lax.Precision.HIGHEST)
    return (next_state, grad_proj)


def solution(mesh):
    in_specs = (
        P("dp", "frame", None, "mp"),
        P("dp", "frame", None),
        P("mp"),
        P("frame", None, "mp"),
        P("mp", None),
        P("dp", "frame"),
        P(),
        P(None, "mp"),
        P("dp", "frame", None, "mp"),
    )
    out_specs = (P("dp", "frame", None, "mp"), P(None, "mp"))
    return jax.shard_map(
        functools.partial(body, mesh.shape["mp"], mesh.shape["dp"]),
        mesh=mesh, in_specs=in_specs, out_specs=out_specs, check_vma=False,
    )
```

```python
import functools
import math

import jax
import jax.numpy as jnp
from jax import lax
from jax.experimental import pallas as pl
from jax.experimental.pallas import tpu as pltpu
from jax.sharding import PartitionSpec as P

HS = 128


def attend_kernel(frames, q_ref, k_ref, v_ref, o_ref):
    scale = 1.0 / math.sqrt(HS)
    for t in range(frames):
        q = q_ref[t].astype(jnp.float32) * scale
        scores = [
            jnp.sum(q * k_ref[u].astype(jnp.float32), axis=-1, keepdims=True) for u in range(t + 1)
        ]
        peak = functools.reduce(jnp.maximum, scores)
        weights = [jnp.exp(s - peak) for s in scores]
        total = functools.reduce(jnp.add, weights)
        accum = functools.reduce(
            jnp.add, [w * v_ref[u].astype(jnp.float32) for u, w in enumerate(weights)]
        )
        o_ref[t] = (accum / total).astype(o_ref.dtype)


def attend(qkv, frames, heads_width):
    rows = qkv.shape[1]
    heads = heads_width // HS
    spec = lambda part: pl.BlockSpec((frames, rows, HS), lambda h, part=part: (0, 0, part * heads + h))
    return pl.pallas_call(
        functools.partial(attend_kernel, frames),
        grid=(heads,),
        in_specs=[spec(0), spec(1), spec(2)],
        out_specs=spec(0),
        out_shape=jax.ShapeDtypeStruct((frames, rows, heads_width), jnp.bfloat16),
        cost_estimate=pl.CostEstimate(flops=4 * frames * frames * rows * heads_width,
                                      bytes_accessed=8 * frames * rows * heads_width,
                                      transcendentals=0),
        name="attend",
    )(qkv, qkv, qkv)


def spread_kernel(frames, dps, x_ref, o_ref, send_sem, recv_sem, own_sem):
    count = frames * dps
    me = lax.axis_index("frame") * dps + lax.axis_index("dp")
    barrier = pltpu.get_barrier_semaphore()

    def peer(shift):
        other = lax.rem(me + shift, count)
        return {"frame": other // dps, "dp": lax.rem(other, dps)}

    for shift in range(1, count):
        pl.semaphore_signal(barrier, inc=1, device_id=peer(shift),
                            device_id_type=pl.DeviceIdType.MESH)
    own = pltpu.make_async_copy(x_ref, o_ref.at[me], own_sem)
    own.start()
    pl.semaphore_wait(barrier, count - 1)
    copies = []
    for shift in range(1, count):
        copy = pltpu.make_async_remote_copy(
            src_ref=x_ref, dst_ref=o_ref.at[me], send_sem=send_sem.at[shift],
            recv_sem=recv_sem.at[shift], device_id=peer(shift),
            device_id_type=pl.DeviceIdType.MESH)
        copy.start()
        copies.append(copy)
    own.wait()
    for copy in copies:
        copy.wait()


def spread_terms(terms, frames, dps):
    count = frames * dps
    return pl.pallas_call(
        functools.partial(spread_kernel, frames, dps),
        in_specs=[pl.BlockSpec(memory_space=pltpu.VMEM)],
        out_specs=pl.BlockSpec(memory_space=pltpu.VMEM),
        out_shape=jax.ShapeDtypeStruct((count, *terms.shape), terms.dtype),
        scratch_shapes=[pltpu.SemaphoreType.DMA((count,)), pltpu.SemaphoreType.DMA((count,)),
                        pltpu.SemaphoreType.DMA],
        compiler_params=pltpu.CompilerParams(collective_id=1, has_side_effects=True),
        name="spread_terms",
    )(terms)


scope = jax.named_scope


def fused_kernel(dps, tokens_ref, mask_ref, embed_ref, w_ref, o_ref, cot_ref, act_ref, book_ref, idx_ref, next_ref, grad_ref,
                 xbuf, wbuf, acc, qkv, abuf, heads, wo, total, xin, cot, act, gate, mine_terms, terms, sums, after,
                 x_recv, x_send, w_recv, w_send, o_recv, o_send, a_recv, a_send, e_recv, e_send,
                 own_sem, t_recv, t_send, out_sem, halves, g_send, g_recv):
    mps, frames, spots, width = xbuf.shape
    per_group, _, _, _ = wbuf.shape
    depth = w_ref.shape[1]
    lines = frames // 2
    half = lines // 2
    part = depth // 2
    quarter = o_ref.shape[0] // 4
    f, m, d = lax.axis_index("frame"), lax.axis_index("mp"), lax.axis_index("dp")
    z, c = f // 2, f % 2
    hi, lo = z // 2, z % 2
    mine = hi * 2 + c
    inner = hi != lo
    pair, near, far = z + 1 - 2 * lo, half - hi, (lines - 1) * (1 - hi)
    other_core = 2 * z + 1 - c
    q0, q1 = d * 2 + c, (1 - d) * 2 + c

    def remote(source, target, send_sem, recv_sem, frame=f, mp=m, dp=d):
        return pltpu.make_async_remote_copy(
            src_ref=source, dst_ref=target, send_sem=send_sem, recv_sem=recv_sem,
            device_id={"frame": frame, "mp": mp, "dp": dp},
            device_id_type=pl.DeviceIdType.MESH)

    def arrived(target, recv_sem):
        pltpu.make_async_copy(target, target, recv_sem).wait()

    def rows_of(owner, which):
        return pl.ds(pl.multiple_of(owner * depth + which * part, part), part)

    def whole_rows(owner):
        return pl.ds(pl.multiple_of(owner * depth, depth), depth)

    def columns(group, head):
        return pl.ds(pl.multiple_of((group * per_group + head) * HS, HS), HS)

    def line(j):
        return jnp.where(j == 0, pair, jnp.where(j == 1, near, far))

    def source_of(j):
        return 2 * line(j // 2) + j % 2

    def w_direct(h, k):
        target = jnp.where(k < 2, pair, near)
        group = jnp.where(k < 2, hi, 1 - hi) * 2 + k % 2
        return remote(w_ref.at[:, pl.ds(pl.multiple_of(d * part, part), part), columns(group, h)],
                      wbuf.at[h, :, rows_of(f, d), :], w_send.at[0], w_recv.at[h, f, d],
                      frame=2 * target + k % 2)

    def w_partner(h):
        return remote(w_ref.at[:, :, columns(hi * 2 + 1 - c, h)], wbuf.at[h, :, whole_rows(f), :],
                      w_send.at[1], w_recv.at[h, f, 0], frame=other_core)

    def w_own(h):
        return pltpu.make_async_copy(w_ref.at[:, :, columns(mine, h)],
                                     wbuf.at[h, :, whole_rows(f), :], own_sem.at[h])

    def w_block(h, owner, which):
        return wbuf.at[h, :, rows_of(owner, which), :]

    def w_share(h, j):
        owner = source_of(j)
        block = w_block(h, owner, d)
        return remote(block, block, w_send.at[2], w_recv.at[h, owner, d], dp=1 - d)

    def w_relay(h, j):
        owner = source_of(j)
        block = w_block(h, owner, d)
        return remote(block, block, w_send.at[3], w_recv.at[h, owner, d],
                      frame=2 * pair + c)

    def forward_w(h, j):
        owner = source_of(j)
        with scope("fw"):
            arrived(w_block(h, owner, d), w_recv.at[h, owner, d])

        @pl.when(jnp.logical_and(inner, j >= 2))
        def _():
            w_relay(h, j).start()

        w_share(h, j).start()

    pieces = frames // mps

    def features(q):
        return pl.ds(pl.multiple_of(q * depth, depth), depth)

    def x_piece(which, owner, q):
        return xbuf.at[which, owner, :, features(q)]

    def x_direct(k, q):
        target = (z + k) % lines
        return remote(xin.at[target % 2, :, features(q)], x_piece(m, f, q), x_send.at[0],
                      x_recv.at[m, f, q], frame=2 * target + c)

    def x_across(owner, source, k, q):
        return remote(source, x_piece(m, owner, q), x_send.at[1], x_recv.at[m, owner, q],
                      mp=1 - m)

    def x_core(owner, source, which, k, q):
        return remote(source, x_piece(which, owner, q), x_send.at[2],
                      x_recv.at[which, owner, q], frame=other_core)

    def x_own(q):
        return xin.at[lo, :, features(q)]

    def x_owner(k):
        return f if k == 0 else 2 * line(k - 1) + c

    slices = o_recv.shape[1]
    share = quarter // slices

    def o_rows(which, i):
        return pl.ds(pl.multiple_of(which * quarter + i * share, share), share)

    def o_piece(which, i):
        return wo.at[1 - m, o_rows(which, i), :]

    def o_across(i):
        return remote(
            o_ref.at[o_rows(q0, i), pl.ds(pl.multiple_of((1 - m) * width, width), width)],
            wo.at[m, o_rows(q0, i), :], o_send, o_recv.at[q0, i], mp=1 - m)

    def o_share(i):
        return remote(o_piece(q0, i), o_piece(q0, i), o_send, o_recv.at[q0, i], dp=1 - d)

    def o_core(which, i, slot):
        return remote(o_piece(which, i), o_piece(which, i), o_send,
                      o_recv.at[which, i], frame=other_core)

    def forward_o(i):
        with scope("o_0"):
            arrived(o_piece(q0, i), o_recv.at[q0, i])
        o_share(i).start()
        o_core(q0, i, 2).start()

    def attn_block(which, owner, h):
        group = (owner // 4) * 2 + owner % 2
        clip = (owner // 2) % 2
        return heads.at[which, h, pl.ds(pl.multiple_of(clip * spots, spots), spots),
                        pl.ds(pl.multiple_of(group * HS, HS), HS)]

    def a_direct(h, k):
        target = (f + k) % frames
        return remote(abuf.at[h, target], attn_block(m, f, h), a_send, a_recv.at[h, f],
                      frame=target)

    def a_own(h):
        return pltpu.make_async_copy(abuf.at[h, f], attn_block(m, f, h), a_recv.at[h, f])

    def a_across(h, k):
        owner = (f + frames - k) % frames
        block = attn_block(m, owner, h)
        return remote(block, block, e_send, e_recv.at[h], mp=1 - m)

    def forward_attn(h):
        @pl.loop(0, frames)
        def _(k):
            owner = (f + frames - k) % frames
            arrived(attn_block(m, owner, h), a_recv.at[h, owner])
            a_across(h, k).start()

    barrier = pltpu.get_barrier_semaphore()
    clips = xin.shape[0]
    tile = math.gcd(width, 512)

    def tile_of(n):
        return pl.ds(pl.multiple_of(n * tile, tile), tile)

    count = frames * dps
    me = f * dps + d

    def peer(shift):
        other = (me + shift) % count
        return other // dps, other % dps

    for shift in range(1, count):
        frame, dp = peer(shift)
        pl.semaphore_signal(barrier, inc=1, device_id={"frame": frame, "mp": m, "dp": dp},
                            device_id_type=pl.DeviceIdType.MESH)
    pl.semaphore_signal(barrier, inc=1, device_id={"frame": f, "mp": 1 - m, "dp": d},
                        device_id_type=pl.DeviceIdType.MESH)
    loads = [pltpu.make_async_copy(source, target, out_sem.at[i]) for i, (source, target) in enumerate((
        (tokens_ref, xin), (cot_ref, cot), (act_ref, act),
        (o_ref.at[:, pl.ds(pl.multiple_of(m * width, width), width)], wo.at[m])))]
    own_x = pltpu.make_async_copy(xin.at[lo], xbuf.at[m, f], own_sem.at[per_group])
    for h in range(per_group):
        w_own(h).start()
    for copy in loads:
        copy.start()
    loads[0].wait()
    gate[0:1, :] = embed_ref[...].astype(jnp.float32)[None, :]
    same = (lax.broadcasted_iota(jnp.int32, (spots, spots), 0)
            == lax.broadcasted_iota(jnp.int32, (spots, spots), 1))
    for r in range(clips):
        row = jnp.broadcast_to(mask_ref[r].astype(jnp.float32), (spots, spots))
        masked = jnp.sum(jnp.where(same, row, 0.0), axis=1, keepdims=True) == 1.0

        @pl.loop(0, width // tile)
        def _(n):
            cols = tile_of(n)
            xin[r, :, cols] = jnp.where(masked, gate[0:1, cols],
                                        xin[r, :, cols].astype(jnp.float32)).astype(xin.dtype)

    own_x.start()
    pl.semaphore_wait(barrier, count)

    last = per_group - 1
    outer = jnp.logical_not(inner)

    def send_tokens(q):
        for k in range(1, lines):
            x_direct(k, q).start()

    def send_weights(h):
        for k in range(4):
            w_direct(h, k).start()

    send_weights(0)
    send_tokens(0)

    @pl.loop(0, slices)
    def _(i):
        o_across(i).start()

    for h in range(per_group):
        w_partner(h).start()

    @pl.loop(0, pieces)
    def _(q):
        x_core(f, x_own(q), m, 0, q).start()

    @pl.loop(0, 2)
    def _(j):
        forward_w(0, j)

    send_tokens(1)

    @pl.when(inner)
    def _():
        @pl.loop(2, 6)
        def _(j):
            forward_w(0, j)

    forward_o(0)
    forward_o(1)

    @pl.when(outer)
    def _():
        forward_w(0, 2)
        forward_w(0, 3)

    forward_o(2)

    def matmul(slot, h, owner, first):
        side = owner // (frames // mps)
        col = pl.multiple_of((owner % (frames // mps)) * depth, depth)
        w = jnp.concatenate([wbuf[h, p, whole_rows(owner), :] for p in range(3)], axis=1)
        step = frames // 2

        @pl.loop(0, 2)
        def _(i):
            x = xbuf[side, pl.ds(i * step, step), :, pl.ds(col, depth)].reshape(step * spots, depth)
            y = jnp.dot(x, w, preferred_element_type=jnp.float32).reshape(step, spots, 3 * HS)

            @pl.when(first)
            def _():
                acc[slot, pl.ds(i * step, step)] = y

            @pl.when(jnp.logical_not(first))
            def _():
                acc[slot, pl.ds(i * step, step)] += y

    def attend_rows(h, i, rows):
        scale = 1.0 / math.sqrt(HS)
        at = pl.ds(pl.multiple_of(i * rows, rows), rows)
        for t in range(frames):
            q = qkv[0, t, at, :].astype(jnp.float32) * scale
            scores = [jnp.sum(q * qkv[1, u, at, :].astype(jnp.float32), axis=-1, keepdims=True)
                      for u in range(t + 1)]
            peak = functools.reduce(jnp.maximum, scores)
            weights = [jnp.exp(s - peak) for s in scores]
            total = functools.reduce(jnp.add, weights)
            accum = functools.reduce(
                jnp.add,
                [w * qkv[2, u, at, :].astype(jnp.float32) for u, w in enumerate(weights)])
            abuf[h, t, at, :] = (accum / total).astype(abuf.dtype)

    def attention(slot, h):
        @pl.loop(0, frames)
        def _(t):
            for p in range(3):
                qkv[p, t] = acc[slot, t, :, p * HS:(p + 1) * HS].astype(qkv.dtype)

        rows = math.gcd(spots, 32)

        @pl.loop(0, spots // rows)
        def _(i):
            with scope("att"):
                attend_rows(h, i, rows)

        a_own(h).start()

        @pl.loop(1, frames)
        def _(k):
            a_direct(h, k).start()

    def ready_w(h, j):
        owner = source_of(j)
        arrived(w_block(h, owner, 1 - d), w_recv.at[h, owner, 1 - d])

    def ready_chip(h):
        w_own(h).wait()
        arrived(wbuf.at[h, :, whole_rows(other_core), :], w_recv.at[h, other_core, 0])

    def ready_w(h, j):
        owner = source_of(j)
        arrived(w_block(h, owner, 1 - d), w_recv.at[h, owner, 1 - d])

    def ready_chip(h):
        w_own(h).wait()
        arrived(wbuf.at[h, :, whole_rows(other_core), :], w_recv.at[h, other_core, 0])

    @pl.loop(0, pieces + 3)
    def _(q):
        @pl.when(q < pieces)
        def _():
            x_across(f, x_own(q), 0, q).start()
            for k in range(1, lines):
                owner = x_owner(k)
                block = x_piece(m, owner, q)
                with scope("x_own"):
                    arrived(block, x_recv.at[m, owner, q])
                x_across(owner, block, k, q).start()
                x_core(owner, block, m, k, q).start()

        @pl.when(q < pieces - 2)
        def _():
            send_tokens(q + 2)

        @pl.when(q == pieces - 2 - jnp.where(outer, 1, 0))
        def _():
            send_weights(1)

        @pl.when(q == 0)
        def _():
            forward_o(3)

            @pl.when(outer)
            def _():
                forward_w(0, 4)
                forward_w(0, 5)

        @pl.when(jnp.logical_and(q >= 2, q < pieces + 2))
        def _():
            for k in range(lines):
                owner = x_owner(k)
                block = x_piece(1 - m, owner, q - 2)
                with scope("x_other"):
                    arrived(block, x_recv.at[1 - m, owner, q - 2])
                x_core(owner, block, 1 - m, k, q - 2).start()

        @pl.when(q == 4)
        def _():
            for h in range(2, per_group):
                send_weights(h)

        @pl.when(jnp.logical_and(q >= 4, q < 6))
        def _():
            forward_w(1, 3 * (q - 4))
            forward_w(1, 3 * (q - 4) + 1)
            forward_w(1, 3 * (q - 4) + 2)

        @pl.when(q == 6)
        def _():
            forward_w(2, 0)
            forward_w(2, 1)

        @pl.when(q == 3)
        def _():
            with scope("w_0"):
                own_x.wait()
                ready_chip(0)
                for j in range(6):
                    ready_w(0, j)

        @pl.when(q >= 3)
        def _():
            with scope("x_core"):
                for k in range(lines):
                    owner = x_owner(k) + 1 - 2 * c
                    for which in range(mps):
                        arrived(x_piece(which, owner, q - 3), x_recv.at[which, owner, q - 3])

            @pl.loop(0, mps)
            def _(side):
                with scope("mm0"):
                    matmul(0, 0, side * pieces + q - 3, jnp.logical_and(side == 0, q == 3))

    @pl.loop(0, slices)
    def _(i):
        with scope("o_1"):
            arrived(o_piece(q1, i), o_recv.at[q1, i])
        o_core(q1, i, 3).start()

    attention(0, 0)

    @pl.loop(0, last * frames)
    def _(i):
        h, jj = 1 + i // frames, i % frames

        @pl.when(jnp.logical_and(inner, jnp.logical_and(h < last, jj >= 4)))
        def _():
            forward_w(h + 1, jj - 2)

        @pl.when(jnp.logical_and(outer, jnp.logical_and(h < last, jj >= 6)))
        def _():
            forward_w(h + 1, jj - 4)

        @pl.when(jnp.logical_and(outer, jnp.logical_and(h > 1, jnp.logical_and(jj >= 4, jj < 6))))
        def _():
            forward_w(h, jj)

        @pl.when(jj == 0)
        def _():
            ready_chip(h)

        @pl.when(jj >= 2)
        def _():
            with scope("w_y"):
                ready_w(h, jnp.maximum(jj - 2, 0))

        owner = jnp.where(jj == 0, f, jnp.where(jj == 1, other_core, source_of(jnp.maximum(jj - 2, 0))))
        with scope("mm"):
            matmul(0, h, owner, jj == 0)

        @pl.when(jj == frames - 1)
        def _():
            attention(0, h)

        @pl.when(jnp.logical_and(h == last, jj == 5))
        def _():
            with scope("fa"):
                forward_attn(last - 1)

        @pl.when(jnp.logical_and(h == last, jj == 3))
        def _():
            for before in range(last - 1):
                with scope("fa"):
                    forward_attn(before)

    @pl.loop(0, slices)
    def _(i):
        for which in (d * 2 + 1 - c, (1 - d) * 2 + 1 - c):
            arrived(o_piece(which, i), o_recv.at[which, i])

    for copy in loads[1:]:
        copy.wait()
    groups = heads.shape[3] // HS
    codes = act.shape[0]
    kinds = book_ref.shape[0]
    index = jnp.concatenate([jnp.full((1, kinds), idx_ref[r], jnp.int32) for r in range(clips)], axis=0)
    onehot = (index == lax.broadcasted_iota(jnp.int32, (clips, kinds), 1)).astype(jnp.float32)
    codevec = jnp.dot(onehot, book_ref[...], precision=lax.Precision.HIGHEST,
                      preferred_element_type=jnp.float32)
    gate[...] = jnp.dot(codevec, act[...], precision=lax.Precision.HIGHEST,
                        preferred_element_type=jnp.float32)
    marks = jnp.concatenate(
        [jnp.full((1, HS), idx_ref[r], jnp.int32).astype(jnp.float32) for r in range(clips)], axis=0)
    side = width // 2
    for half_of in range(2):
        mine_terms[half_of, :, side:] = marks

    def partial(h, side, cols):
        w = jnp.concatenate(
            [wo[side, pl.ds(pl.multiple_of((g * per_group + h) * HS, HS), HS), cols]
             for g in range(groups)], axis=0)
        return jnp.dot(heads[side, h], w, preferred_element_type=jnp.float32)

    def exchanged(h):
        arrived(heads.at[1 - m, h], e_recv.at[h])

    @pl.loop(0, last)
    def _(h):
        @pl.when(h == last - 1)
        def _():
            with scope("fa"):
                forward_attn(last)

        with scope("exchanged"):
            exchanged(h)

        @pl.loop(0, width // tile)
        def _(n):
            cols = tile_of(n)
            y = partial(h, 0, cols) + partial(h, 1, cols)

            @pl.when(h == 0)
            def _():
                total[:, cols] = y

            @pl.when(h > 0)
            def _():
                total[:, cols] += y

    @pl.loop(0, width // tile)
    def _(n):
        cols = tile_of(n)
        total[:, cols] += partial(last, m, cols)

    with scope("exchanged"):
        exchanged(last)

    @pl.loop(0, width // tile)
    def _(n):
        cols = tile_of(n)
        y = total[:, cols] + partial(last, 1 - m, cols)
        for r in range(clips):
            mixed = y[r * spots:(r + 1) * spots]
            factor = gate[r:r + 1, cols]
            after[r, :, cols] = (
                xin[r, :, cols].astype(jnp.float32) + factor * mixed).astype(xin.dtype)
            weighed = jnp.sum(cot[r, :, cols].astype(jnp.float32) * mixed, axis=0, keepdims=True)
            piece = math.gcd(tile, side)
            for i in range(tile // piece):
                at = n * (tile // piece) + i
                mine_terms[at // (side // piece), r:r + 1,
                           pl.ds(pl.multiple_of(at % (side // piece) * piece, piece), piece)] = (
                    weighed[:, i * piece:(i + 1) * piece])

    def t_copy(shift):
        frame, dp = peer(shift)
        return remote(mine_terms.at[frame % 2], terms.at[me], t_send.at[0], t_recv.at[me],
                      frame=frame, dp=dp)

    for shift in range(1, count):
        t_copy(shift).start()
    own_terms = pltpu.make_async_copy(mine_terms.at[c], terms.at[me], t_send.at[1])
    own_terms.start()
    result = pltpu.make_async_copy(after, next_ref, out_sem.at[0])
    result.start()

    arrived(wo.at[0], o_send)
    arrived(xbuf.at[0, pl.ds(0, lines - 1)], x_send.at[0])
    arrived(xbuf.at[0, pl.ds(0, lines)], x_send.at[1])
    arrived(xbuf.at[0], x_send.at[2])
    arrived(wbuf.at[:, :, pl.ds(0, 4 * part), :], w_send.at[0])
    arrived(wbuf.at[:, :, pl.ds(0, depth), :], w_send.at[1])
    arrived(wbuf.at[:, :, pl.ds(0, 6 * part), :], w_send.at[2])

    @pl.when(inner)
    def _():
        arrived(wbuf.at[:, :, pl.ds(0, 4 * part), :], w_send.at[3])

    arrived(abuf.at[:, pl.ds(0, frames - 1)], a_send)
    arrived(abuf, e_send)
    kind = lax.broadcasted_iota(jnp.int32, (kinds, HS), 0).astype(jnp.float32)

    def gathered(other):
        total = sums[c]
        for r in range(clips):
            mask = jnp.tile(terms[other, r:r + 1, side:] == kind, (1, side // HS))
            total += jnp.where(mask, terms[other, r:r + 1, :side], 0.0)
        sums[c] = total

    sums[c] = jnp.zeros((kinds, side), jnp.float32)
    own_terms.wait()
    gathered(me)
    with scope("terms"):
        @pl.loop(1, count)
        def _(shift):
            frame, dp = peer(count - shift)
            other = frame * dps + dp
            arrived(terms.at[other], t_recv.at[other])
            gathered(other)

    arrived(terms.at[pl.ds(0, count - 1)], t_send.at[0])
    swap = remote(sums.at[c], sums.at[c], g_send, g_recv, frame=other_core)
    swap.start()
    book_columns = book_ref[...].T

    def gradient(i):
        halves[i] = jnp.dot(book_columns, sums[i], precision=lax.Precision.HIGHEST,
                            preferred_element_type=jnp.float32)
        copy = pltpu.make_async_copy(
            halves.at[i], grad_ref.at[:, pl.ds(pl.multiple_of(i * side, HS), side)],
            out_sem.at[1 + i])
        copy.start()
        return copy

    first = gradient(c)
    arrived(sums.at[1 - c], g_recv)
    second = gradient(1 - c)
    swap.wait_send()
    first.wait()
    second.wait()
    result.wait()


def fused(dps, tokens, mask, embed, w_parts, w_out, cotangent, act_proj, codebook, action_idx, frames):
    clips, spots, width = tokens.shape
    parts, depth, heads_width = w_parts.shape
    groups = frames // clips
    per_group = heads_width // HS // groups
    count = frames * dps
    any_spec = pl.BlockSpec(memory_space=pl.ANY)
    vmem = pl.BlockSpec(memory_space=pltpu.VMEM)
    dma = pltpu.SemaphoreType.DMA
    return pl.pallas_call(
        functools.partial(fused_kernel, dps),
        in_specs=[any_spec, vmem, vmem] + [any_spec] * 4 + [vmem, pl.BlockSpec(memory_space=pltpu.SMEM)],
        out_specs=[any_spec] * 2,
        out_shape=[
            jax.ShapeDtypeStruct(tokens.shape, tokens.dtype),
            jax.ShapeDtypeStruct(act_proj.shape, jnp.float32),
        ],
        scratch_shapes=[
            pltpu.VMEM((2, frames, spots, width), jnp.bfloat16),
            pltpu.VMEM((per_group, parts, depth * frames, HS), jnp.bfloat16),
            pltpu.VMEM((1, frames, spots, parts * HS), jnp.float32),
            pltpu.VMEM((parts, frames, spots, HS), jnp.bfloat16),
            pltpu.VMEM((per_group, frames, spots, HS), jnp.bfloat16),
            pltpu.VMEM((2, per_group, clips * spots, groups * HS), jnp.bfloat16),
            pltpu.VMEM((2, heads_width, width), jnp.bfloat16),
            pltpu.VMEM((clips * spots, width), jnp.float32),
            pltpu.VMEM(tokens.shape, jnp.bfloat16),
            pltpu.VMEM(tokens.shape, jnp.bfloat16),
            pltpu.VMEM(act_proj.shape, jnp.float32),
            pltpu.VMEM((clips, width), jnp.float32),
            pltpu.VMEM((2, clips, width // 2 + HS), jnp.float32),
            pltpu.VMEM((count, clips, width // 2 + HS), jnp.float32),
            pltpu.VMEM((2, codebook.shape[0], width // 2), jnp.float32),
            pltpu.VMEM(tokens.shape, jnp.bfloat16),
            dma((2, frames, frames // 2)), dma((3,)),
            dma((per_group, frames, 2)), dma((4,)),
            dma((4, 4)), dma,
            dma((per_group, frames)), dma,
            dma((per_group,)), dma,
            dma((per_group + 1,)), dma((count,)), dma((2,)), dma((4,)),
            pltpu.VMEM((2, act_proj.shape[0], width // 2), jnp.float32), dma, dma,
        ],
        compiler_params=pltpu.CompilerParams(
            collective_id=2, has_side_effects=True, vmem_limit_bytes=60 << 20),
        name="fused",
    )(tokens, mask, embed, w_parts, w_out, cotangent, act_proj, codebook, action_idx)


def finish_kernel(next_ref, grad_ref, next_out, grad_out, rows, grads, load, store):
    copies = []
    for i, (source, middle, target) in enumerate(
            [(next_ref.at[r], rows.at[r], next_out.at[r]) for r in range(rows.shape[0])]
            + [(grad_ref, grads, grad_out)]):
        copies.append((pltpu.make_async_copy(source, middle, load.at[i]),
                       pltpu.make_async_copy(middle, target, store.at[i])))
    for first, _ in copies:
        first.start()
    for first, second in copies:
        first.wait()
        second.start()
    for _, second in copies:
        second.wait()


def finish(next_state, grad_proj):
    any_spec = pl.BlockSpec(memory_space=pl.ANY)
    count = next_state.shape[0] + 1
    return pl.pallas_call(
        finish_kernel,
        in_specs=[any_spec] * 2,
        out_specs=[any_spec] * 2,
        out_shape=[jax.ShapeDtypeStruct(a.shape, a.dtype) for a in (next_state, grad_proj)],
        scratch_shapes=[pltpu.VMEM(next_state.shape, next_state.dtype),
                        pltpu.VMEM(grad_proj.shape, grad_proj.dtype),
                        pltpu.SemaphoreType.DMA((count,)), pltpu.SemaphoreType.DMA((count,))],
        name="finish",
    )(next_state, grad_proj)


def gather_mp(block, size):
    if size != 2:
        return lax.all_gather(block, "mp", axis=block.ndim - 1, tiled=True)
    other = lax.ppermute(block, "mp", [(0, 1), (1, 0)])
    first = lax.axis_index("mp") == 0
    return jnp.concatenate(
        [jnp.where(first, block, other), jnp.where(first, other, block)], axis=-1
    )


def fits_fused(mps, dps, frames, clips, spots, width, depth, heads_width):
    groups = frames // clips
    return (mps == dps == clips == 2 and frames == groups * clips and groups == 2 * clips
            and heads_width == 3 * groups * HS
            and spots % 32 == 0 and depth % HS == 0
            and width * mps == depth * frames and heads_width % (16 * 16) == 0)


def body(mp_size, dp_size, tokens, token_mask, mask_embed, w_qkv, w_out, action_idx, codebook,
         act_proj, cotangent):
    clips, _, spots, width = tokens.shape
    heads_width = w_qkv.shape[2]
    depth = w_qkv.shape[0]
    xin = jnp.where(token_mask[..., None] == 1, mask_embed, tokens)
    frames = lax.axis_size("frame")
    if fits_fused(mp_size, dp_size, frames, clips, spots, width, depth, heads_width):
        next_state, grad_proj = fused(
            dp_size, tokens.reshape(clips, spots, width), token_mask, mask_embed, w_qkv.transpose(1, 0, 2), w_out,
            cotangent.reshape(clips, spots, width), act_proj, codebook,
            action_idx.reshape(clips), frames)
        next_state, grad_proj = finish(next_state.reshape(2 * clips, spots // 2, width), grad_proj)
        return (next_state.reshape(clips, 1, spots, width), grad_proj)
    else:
        share = depth // dp_size
        mine = lax.dynamic_slice_in_dim(
            w_qkv.reshape(depth, 3 * heads_width), lax.axis_index("dp") * share, share, axis=0
        )
        weights = lax.all_gather(mine, ("frame", "dp"), axis=0, tiled=True)
        if mp_size == 2:
            my_mp = lax.axis_index("mp")
            out_mine = lax.dynamic_slice_in_dim(w_out, my_mp * width, width, axis=1)
            out_other = lax.ppermute(
                lax.dynamic_slice_in_dim(w_out, (1 - my_mp) * width, width, axis=1),
                "mp", [(0, 1), (1, 0)])
        spread = lax.all_to_all(
            xin.reshape(clips, spots, width), "frame", split_axis=1, concat_axis=0, tiled=True
        )
        frames = spread.shape[0] // clips
        local = spread.shape[1]
        features = gather_mp(spread.reshape(frames * clips * local, width), mp_size)
        qkv = jnp.dot(features, weights, preferred_element_type=jnp.float32).astype(jnp.bfloat16)
        attn = attend(qkv.reshape(frames, clips * local, 3 * heads_width), frames, heads_width)
        back = lax.all_to_all(
            attn.reshape(frames * clips, local, heads_width), "frame", split_axis=0, concat_axis=1,
            tiled=True,
        )
        heads = back.reshape(clips * spots, heads_width)
        if mp_size == 2:
            other_heads = lax.ppermute(heads, "mp", [(0, 1), (1, 0)])
            mixed_rows = jnp.dot(heads, out_mine, preferred_element_type=jnp.float32) + jnp.dot(
                other_heads, out_other, preferred_element_type=jnp.float32)
        else:
            out_block = lax.all_to_all(w_out, "mp", split_axis=1, concat_axis=0, tiled=True)
            mixed_rows = jnp.dot(gather_mp(heads, mp_size), out_block,
                                 preferred_element_type=jnp.float32)
    mixed = mixed_rows.reshape(clips, 1, spots, width)
    onehot = (
        action_idx.reshape(clips)[:, None] == jnp.arange(codebook.shape[0])[None, :]
    ).astype(jnp.float32)
    codevec = jnp.dot(onehot, codebook, precision=lax.Precision.HIGHEST)
    gate = jnp.dot(codevec, act_proj, precision=lax.Precision.HIGHEST)
    next_state = (xin.astype(jnp.float32) + gate[:, None, None, :] * mixed).astype(jnp.bfloat16)
    dgate = jnp.sum(cotangent.astype(jnp.float32) * mixed, axis=2).reshape(clips, width)
    codes = codevec.shape[1]
    padded = jnp.pad(codevec, ((0, 0), (0, -codes % 128)))
    terms = spread_terms(jnp.concatenate([dgate, padded], axis=1), frames, dp_size)
    terms = terms.reshape(frames * dp_size * clips, -1)
    grad_proj = jnp.dot(
        terms[:, width : width + codes].T, terms[:, :width], precision=lax.Precision.HIGHEST)
    return (next_state, grad_proj)


def solution(mesh):
    in_specs = (
        P("dp", "frame", None, "mp"),
        P("dp", "frame", None),
        P("mp"),
        P("frame", None, "mp"),
        P("mp", None),
        P("dp", "frame"),
        P(),
        P(None, "mp"),
        P("dp", "frame", None, "mp"),
    )
    out_specs = (P("dp", "frame", None, "mp"), P(None, "mp"))
    return jax.shard_map(
        functools.partial(body, mesh.shape["mp"], mesh.shape["dp"]),
        mesh=mesh, in_specs=in_specs, out_specs=out_specs, check_vma=False,
    )
```

```python
import functools
import math

import jax
import jax.numpy as jnp
from jax import lax
from jax.experimental import pallas as pl
from jax.experimental.pallas import tpu as pltpu
from jax.sharding import PartitionSpec as P

HS = 128


def attend_kernel(frames, q_ref, k_ref, v_ref, o_ref):
    scale = 1.0 / math.sqrt(HS)
    for t in range(frames):
        q = q_ref[t].astype(jnp.float32) * scale
        scores = [
            jnp.sum(q * k_ref[u].astype(jnp.float32), axis=-1, keepdims=True) for u in range(t + 1)
        ]
        peak = functools.reduce(jnp.maximum, scores)
        weights = [jnp.exp(s - peak) for s in scores]
        total = functools.reduce(jnp.add, weights)
        accum = functools.reduce(
            jnp.add, [w * v_ref[u].astype(jnp.float32) for u, w in enumerate(weights)]
        )
        o_ref[t] = (accum / total).astype(o_ref.dtype)


def attend(qkv, frames, heads_width):
    rows = qkv.shape[1]
    heads = heads_width // HS
    spec = lambda part: pl.BlockSpec((frames, rows, HS), lambda h, part=part: (0, 0, part * heads + h))
    return pl.pallas_call(
        functools.partial(attend_kernel, frames),
        grid=(heads,),
        in_specs=[spec(0), spec(1), spec(2)],
        out_specs=spec(0),
        out_shape=jax.ShapeDtypeStruct((frames, rows, heads_width), jnp.bfloat16),
        cost_estimate=pl.CostEstimate(flops=4 * frames * frames * rows * heads_width,
                                      bytes_accessed=8 * frames * rows * heads_width,
                                      transcendentals=0),
        name="attend",
    )(qkv, qkv, qkv)


def spread_kernel(frames, dps, x_ref, o_ref, send_sem, recv_sem, own_sem):
    count = frames * dps
    me = lax.axis_index("frame") * dps + lax.axis_index("dp")
    barrier = pltpu.get_barrier_semaphore()

    def peer(shift):
        other = lax.rem(me + shift, count)
        return {"frame": other // dps, "dp": lax.rem(other, dps)}

    for shift in range(1, count):
        pl.semaphore_signal(barrier, inc=1, device_id=peer(shift),
                            device_id_type=pl.DeviceIdType.MESH)
    own = pltpu.make_async_copy(x_ref, o_ref.at[me], own_sem)
    own.start()
    pl.semaphore_wait(barrier, count - 1)
    copies = []
    for shift in range(1, count):
        copy = pltpu.make_async_remote_copy(
            src_ref=x_ref, dst_ref=o_ref.at[me], send_sem=send_sem.at[shift],
            recv_sem=recv_sem.at[shift], device_id=peer(shift),
            device_id_type=pl.DeviceIdType.MESH)
        copy.start()
        copies.append(copy)
    own.wait()
    for copy in copies:
        copy.wait()


def spread_terms(terms, frames, dps):
    count = frames * dps
    return pl.pallas_call(
        functools.partial(spread_kernel, frames, dps),
        in_specs=[pl.BlockSpec(memory_space=pltpu.VMEM)],
        out_specs=pl.BlockSpec(memory_space=pltpu.VMEM),
        out_shape=jax.ShapeDtypeStruct((count, *terms.shape), terms.dtype),
        scratch_shapes=[pltpu.SemaphoreType.DMA((count,)), pltpu.SemaphoreType.DMA((count,)),
                        pltpu.SemaphoreType.DMA],
        compiler_params=pltpu.CompilerParams(collective_id=1, has_side_effects=True),
        name="spread_terms",
    )(terms)


scope = jax.named_scope


def fused_kernel(dps, tokens_ref, mask_ref, embed_ref, w_ref, o_ref, cot_ref, act_ref, book_ref, idx_ref, next_ref, grad_ref,
                 xbuf, wbuf, acc, qkv, abuf, heads, wo, total, xin, cot, act, gate, mine_terms, terms, sums, after,
                 x_recv, x_send, w_recv, w_send, o_recv, o_send, a_recv, a_send, e_recv, e_send,
                 own_sem, t_recv, t_send, out_sem, halves, g_send, g_recv):
    mps, frames, spots, width = xbuf.shape
    per_group, _, _, _ = wbuf.shape
    depth = w_ref.shape[1]
    lines = frames // 2
    half = lines // 2
    part = depth // 2
    quarter = o_ref.shape[0] // 4
    f, m, d = lax.axis_index("frame"), lax.axis_index("mp"), lax.axis_index("dp")
    z, c = f // 2, f % 2
    hi, lo = z // 2, z % 2
    mine = hi * 2 + c
    inner = hi != lo
    pair, near, far = z + 1 - 2 * lo, half - hi, (lines - 1) * (1 - hi)
    other_core = 2 * z + 1 - c
    q0, q1 = d * 2 + c, (1 - d) * 2 + c

    def remote(source, target, send_sem, recv_sem, frame=f, mp=m, dp=d):
        return pltpu.make_async_remote_copy(
            src_ref=source, dst_ref=target, send_sem=send_sem, recv_sem=recv_sem,
            device_id={"frame": frame, "mp": mp, "dp": dp},
            device_id_type=pl.DeviceIdType.MESH)

    def arrived(target, recv_sem):
        pltpu.make_async_copy(target, target, recv_sem).wait()

    def rows_of(owner, which):
        return pl.ds(pl.multiple_of(owner * depth + which * part, part), part)

    def whole_rows(owner):
        return pl.ds(pl.multiple_of(owner * depth, depth), depth)

    def columns(group, head):
        return pl.ds(pl.multiple_of((group * per_group + head) * HS, HS), HS)

    def line(j):
        return jnp.where(j == 0, pair, jnp.where(j == 1, near, far))

    def source_of(j):
        return 2 * line(j // 2) + j % 2

    def w_direct(h, k):
        target = jnp.where(k < 2, pair, near)
        group = jnp.where(k < 2, hi, 1 - hi) * 2 + k % 2
        return remote(w_ref.at[:, pl.ds(pl.multiple_of(d * part, part), part), columns(group, h)],
                      wbuf.at[h, :, rows_of(f, d), :], w_send.at[0], w_recv.at[h, f, d],
                      frame=2 * target + k % 2)

    def w_partner(h):
        return remote(w_ref.at[:, :, columns(hi * 2 + 1 - c, h)], wbuf.at[h, :, whole_rows(f), :],
                      w_send.at[1], w_recv.at[h, f, 0], frame=other_core)

    def w_own(h):
        return pltpu.make_async_copy(w_ref.at[:, :, columns(mine, h)],
                                     wbuf.at[h, :, whole_rows(f), :], own_sem.at[h])

    def w_block(h, owner, which):
        return wbuf.at[h, :, rows_of(owner, which), :]

    def w_share(h, j):
        owner = source_of(j)
        block = w_block(h, owner, d)
        return remote(block, block, w_send.at[2], w_recv.at[h, owner, d], dp=1 - d)

    def w_relay(h, j):
        owner = source_of(j)
        block = w_block(h, owner, d)
        return remote(block, block, w_send.at[3], w_recv.at[h, owner, d],
                      frame=2 * pair + c)

    def forward_w(h, j):
        owner = source_of(j)
        with scope("fw"):
            arrived(w_block(h, owner, d), w_recv.at[h, owner, d])

        @pl.when(jnp.logical_and(inner, j >= 2))
        def _():
            w_relay(h, j).start()

        w_share(h, j).start()

    pieces = frames // mps

    def features(q):
        return pl.ds(pl.multiple_of(q * depth, depth), depth)

    def x_piece(which, owner, q):
        return xbuf.at[which, owner, :, features(q)]

    def x_direct(k, q):
        target = (z + k) % lines
        return remote(xin.at[target % 2, :, features(q)], x_piece(m, f, q), x_send.at[0],
                      x_recv.at[m, f, q], frame=2 * target + c)

    def x_across(owner, source, k, q):
        return remote(source, x_piece(m, owner, q), x_send.at[1], x_recv.at[m, owner, q],
                      mp=1 - m)

    def x_core(owner, source, which, k, q):
        return remote(source, x_piece(which, owner, q), x_send.at[2],
                      x_recv.at[which, owner, q], frame=other_core)

    def x_own(q):
        return xin.at[lo, :, features(q)]

    def x_owner(k):
        return f if k == 0 else 2 * line(k - 1) + c

    slices = o_recv.shape[1]
    share = quarter // slices

    def o_rows(which, i):
        return pl.ds(pl.multiple_of(which * quarter + i * share, share), share)

    def o_piece(which, i):
        return wo.at[1 - m, o_rows(which, i), :]

    def o_across(i):
        return remote(
            o_ref.at[o_rows(q0, i), pl.ds(pl.multiple_of((1 - m) * width, width), width)],
            wo.at[m, o_rows(q0, i), :], o_send, o_recv.at[q0, i], mp=1 - m)

    def o_share(i):
        return remote(o_piece(q0, i), o_piece(q0, i), o_send, o_recv.at[q0, i], dp=1 - d)

    def o_core(which, i, slot):
        return remote(o_piece(which, i), o_piece(which, i), o_send,
                      o_recv.at[which, i], frame=other_core)

    def forward_o(i):
        with scope("o_0"):
            arrived(o_piece(q0, i), o_recv.at[q0, i])
        o_share(i).start()
        o_core(q0, i, 2).start()

    def attn_block(which, owner, h):
        group = (owner // 4) * 2 + owner % 2
        clip = (owner // 2) % 2
        return heads.at[which, h, pl.ds(pl.multiple_of(clip * spots, spots), spots),
                        pl.ds(pl.multiple_of(group * HS, HS), HS)]

    def a_direct(h, k):
        target = (f + k) % frames
        return remote(abuf.at[h, target], attn_block(m, f, h), a_send, a_recv.at[h, f],
                      frame=target)

    def a_own(h):
        return pltpu.make_async_copy(abuf.at[h, f], attn_block(m, f, h), a_recv.at[h, f])

    def a_across(h, k):
        owner = (f + frames - k) % frames
        block = attn_block(m, owner, h)
        return remote(block, block, e_send, e_recv.at[h], mp=1 - m)

    def forward_attn(h):
        @pl.loop(0, frames)
        def _(k):
            owner = (f + frames - k) % frames
            arrived(attn_block(m, owner, h), a_recv.at[h, owner])
            a_across(h, k).start()

    barrier = pltpu.get_barrier_semaphore()
    clips = xin.shape[0]
    tile = math.gcd(width, 512)

    def tile_of(n):
        return pl.ds(pl.multiple_of(n * tile, tile), tile)

    count = frames * dps
    me = f * dps + d

    def peer(shift):
        other = (me + shift) % count
        return other // dps, other % dps

    for shift in range(1, count):
        frame, dp = peer(shift)
        pl.semaphore_signal(barrier, inc=1, device_id={"frame": frame, "mp": m, "dp": dp},
                            device_id_type=pl.DeviceIdType.MESH)
    pl.semaphore_signal(barrier, inc=1, device_id={"frame": f, "mp": 1 - m, "dp": d},
                        device_id_type=pl.DeviceIdType.MESH)
    loads = [pltpu.make_async_copy(source, target, out_sem.at[i]) for i, (source, target) in enumerate((
        (tokens_ref, xin), (cot_ref, cot), (act_ref, act),
        (o_ref.at[:, pl.ds(pl.multiple_of(m * width, width), width)], wo.at[m])))]
    own_x = pltpu.make_async_copy(xin.at[lo], xbuf.at[m, f], own_sem.at[per_group])
    for h in range(per_group):
        w_own(h).start()
    loads[0].start()
    pl.semaphore_wait(barrier, count)

    last = per_group - 1
    outer = jnp.logical_not(inner)

    def send_tokens(q):
        for k in range(1, lines):
            x_direct(k, q).start()

    def send_weights(h):
        for k in range(4):
            w_direct(h, k).start()

    send_weights(0)

    @pl.loop(0, slices)
    def _(i):
        o_across(i).start()

    loads[0].wait()
    gate[0:1, :] = embed_ref[...].astype(jnp.float32)[None, :]
    same = (lax.broadcasted_iota(jnp.int32, (spots, spots), 0)
            == lax.broadcasted_iota(jnp.int32, (spots, spots), 1))
    for r in range(clips):
        row = jnp.broadcast_to(mask_ref[r].astype(jnp.float32), (spots, spots))
        masked = jnp.sum(jnp.where(same, row, 0.0), axis=1, keepdims=True) == 1.0

        @pl.loop(0, width // tile)
        def _(n):
            cols = tile_of(n)
            xin[r, :, cols] = jnp.where(masked, gate[0:1, cols],
                                        xin[r, :, cols].astype(jnp.float32)).astype(xin.dtype)

    own_x.start()
    send_tokens(0)

    w_partner(0).start()

    @pl.loop(0, pieces)
    def _(q):
        x_core(f, x_own(q), m, 0, q).start()

    @pl.loop(0, 2)
    def _(j):
        forward_w(0, j)

    for copy in loads[1:]:
        copy.start()

    send_tokens(1)

    @pl.when(inner)
    def _():
        @pl.loop(2, 6)
        def _(j):
            forward_w(0, j)

    forward_o(0)
    forward_o(1)

    @pl.when(outer)
    def _():
        forward_w(0, 2)
        forward_w(0, 3)

    forward_o(2)

    def matmul(slot, h, owner, first):
        side = owner // (frames // mps)
        col = pl.multiple_of((owner % (frames // mps)) * depth, depth)
        w = jnp.concatenate([wbuf[h, p, whole_rows(owner), :] for p in range(3)], axis=1)
        step = frames // 2

        @pl.loop(0, 2)
        def _(i):
            x = xbuf[side, pl.ds(i * step, step), :, pl.ds(col, depth)].reshape(step * spots, depth)
            y = jnp.dot(x, w, preferred_element_type=jnp.float32).reshape(step, spots, 3 * HS)

            @pl.when(first)
            def _():
                acc[slot, pl.ds(i * step, step)] = y

            @pl.when(jnp.logical_not(first))
            def _():
                acc[slot, pl.ds(i * step, step)] += y

    def attend_rows(h, i, rows):
        scale = 1.0 / math.sqrt(HS)
        at = pl.ds(pl.multiple_of(i * rows, rows), rows)
        for t in range(frames):
            q = qkv[0, t, at, :].astype(jnp.float32) * scale
            scores = [jnp.sum(q * qkv[1, u, at, :].astype(jnp.float32), axis=-1, keepdims=True)
                      for u in range(t + 1)]
            peak = functools.reduce(jnp.maximum, scores)
            weights = [jnp.exp(s - peak) for s in scores]
            total = functools.reduce(jnp.add, weights)
            accum = functools.reduce(
                jnp.add,
                [w * qkv[2, u, at, :].astype(jnp.float32) for u, w in enumerate(weights)])
            abuf[h, t, at, :] = (accum / total).astype(abuf.dtype)

    def attention(slot, h):
        @pl.loop(0, frames)
        def _(t):
            for p in range(3):
                qkv[p, t] = acc[slot, t, :, p * HS:(p + 1) * HS].astype(qkv.dtype)

        rows = math.gcd(spots, 32)

        @pl.loop(0, spots // rows)
        def _(i):
            with scope("att"):
                attend_rows(h, i, rows)

        a_own(h).start()

        @pl.loop(1, frames)
        def _(k):
            a_direct(h, k).start()

    def ready_w(h, j):
        owner = source_of(j)
        arrived(w_block(h, owner, 1 - d), w_recv.at[h, owner, 1 - d])

    def ready_chip(h):
        w_own(h).wait()
        arrived(wbuf.at[h, :, whole_rows(other_core), :], w_recv.at[h, other_core, 0])

    def ready_w(h, j):
        owner = source_of(j)
        arrived(w_block(h, owner, 1 - d), w_recv.at[h, owner, 1 - d])

    def ready_chip(h):
        w_own(h).wait()
        arrived(wbuf.at[h, :, whole_rows(other_core), :], w_recv.at[h, other_core, 0])

    for h in range(1, per_group):
        w_partner(h).start()

    @pl.loop(0, pieces + 3)
    def _(q):
        @pl.when(q < pieces)
        def _():
            x_across(f, x_own(q), 0, q).start()
            for k in range(1, lines):
                owner = x_owner(k)
                block = x_piece(m, owner, q)
                with scope("x_own"):
                    arrived(block, x_recv.at[m, owner, q])
                x_across(owner, block, k, q).start()
                x_core(owner, block, m, k, q).start()

        @pl.when(q < pieces - 2)
        def _():
            send_tokens(q + 2)

        @pl.when(q == pieces - 2 - jnp.where(outer, 1, 0))
        def _():
            send_weights(1)

        @pl.when(q == 0)
        def _():
            forward_o(3)

            @pl.when(outer)
            def _():
                forward_w(0, 4)
                forward_w(0, 5)

        @pl.when(jnp.logical_and(q >= 2, q < pieces + 2))
        def _():
            for k in range(lines):
                owner = x_owner(k)
                block = x_piece(1 - m, owner, q - 2)
                with scope("x_other"):
                    arrived(block, x_recv.at[1 - m, owner, q - 2])
                x_core(owner, block, 1 - m, k, q - 2).start()

        @pl.when(q == 4)
        def _():
            for h in range(2, per_group):
                send_weights(h)

        @pl.when(jnp.logical_and(q >= 4, q < 6))
        def _():
            forward_w(1, 3 * (q - 4))
            forward_w(1, 3 * (q - 4) + 1)
            forward_w(1, 3 * (q - 4) + 2)

        @pl.when(q == 6)
        def _():
            forward_w(2, 0)
            forward_w(2, 1)

        @pl.when(q == 3)
        def _():
            with scope("w_0"):
                own_x.wait()
                ready_chip(0)
                for j in range(6):
                    ready_w(0, j)

        @pl.when(q >= 3)
        def _():
            with scope("x_core"):
                for k in range(lines):
                    owner = x_owner(k) + 1 - 2 * c
                    for which in range(mps):
                        arrived(x_piece(which, owner, q - 3), x_recv.at[which, owner, q - 3])

            @pl.loop(0, mps)
            def _(side):
                with scope("mm0"):
                    matmul(0, 0, side * pieces + q - 3, jnp.logical_and(side == 0, q == 3))

    @pl.loop(0, slices)
    def _(i):
        with scope("o_1"):
            arrived(o_piece(q1, i), o_recv.at[q1, i])
        o_core(q1, i, 3).start()

    attention(0, 0)

    @pl.loop(0, last * frames)
    def _(i):
        h, jj = 1 + i // frames, i % frames

        @pl.when(jnp.logical_and(inner, jnp.logical_and(h < last, jj >= 4)))
        def _():
            forward_w(h + 1, jj - 2)

        @pl.when(jnp.logical_and(outer, jnp.logical_and(h < last, jj >= 6)))
        def _():
            forward_w(h + 1, jj - 4)

        @pl.when(jnp.logical_and(outer, jnp.logical_and(h > 1, jnp.logical_and(jj >= 4, jj < 6))))
        def _():
            forward_w(h, jj)

        @pl.when(jj == 0)
        def _():
            ready_chip(h)

        @pl.when(jj >= 2)
        def _():
            with scope("w_y"):
                ready_w(h, jnp.maximum(jj - 2, 0))

        owner = jnp.where(jj == 0, f, jnp.where(jj == 1, other_core, source_of(jnp.maximum(jj - 2, 0))))
        with scope("mm"):
            matmul(0, h, owner, jj == 0)

        @pl.when(jj == frames - 1)
        def _():
            attention(0, h)

        @pl.when(jnp.logical_and(h == last, jj == 5))
        def _():
            with scope("fa"):
                forward_attn(last - 1)

        @pl.when(jnp.logical_and(h == last, jj == 3))
        def _():
            for before in range(last - 1):
                with scope("fa"):
                    forward_attn(before)

    @pl.loop(0, slices)
    def _(i):
        for which in (d * 2 + 1 - c, (1 - d) * 2 + 1 - c):
            arrived(o_piece(which, i), o_recv.at[which, i])

    for copy in loads[1:]:
        copy.wait()
    groups = heads.shape[3] // HS
    codes = act.shape[0]
    kinds = book_ref.shape[0]
    index = jnp.concatenate([jnp.full((1, kinds), idx_ref[r], jnp.int32) for r in range(clips)], axis=0)
    onehot = (index == lax.broadcasted_iota(jnp.int32, (clips, kinds), 1)).astype(jnp.float32)
    codevec = jnp.dot(onehot, book_ref[...], precision=lax.Precision.HIGHEST,
                      preferred_element_type=jnp.float32)
    gate[...] = jnp.dot(codevec, act[...], precision=lax.Precision.HIGHEST,
                        preferred_element_type=jnp.float32)
    marks = jnp.concatenate(
        [jnp.full((1, HS), idx_ref[r], jnp.int32).astype(jnp.float32) for r in range(clips)], axis=0)
    side = width // 2
    for half_of in range(2):
        mine_terms[half_of, :, side:] = marks

    def partial(h, side, cols):
        w = jnp.concatenate(
            [wo[side, pl.ds(pl.multiple_of((g * per_group + h) * HS, HS), HS), cols]
             for g in range(groups)], axis=0)
        return jnp.dot(heads[side, h], w, preferred_element_type=jnp.float32)

    def exchanged(h):
        arrived(heads.at[1 - m, h], e_recv.at[h])

    @pl.loop(0, last)
    def _(h):
        @pl.when(h == last - 1)
        def _():
            with scope("fa"):
                forward_attn(last)

        with scope("exchanged"):
            exchanged(h)

        @pl.loop(0, width // tile)
        def _(n):
            cols = tile_of(n)
            y = partial(h, 0, cols) + partial(h, 1, cols)

            @pl.when(h == 0)
            def _():
                total[:, cols] = y

            @pl.when(h > 0)
            def _():
                total[:, cols] += y

    @pl.loop(0, width // tile)
    def _(n):
        cols = tile_of(n)
        total[:, cols] += partial(last, m, cols)

    with scope("exchanged"):
        exchanged(last)

    @pl.loop(0, width // tile)
    def _(n):
        cols = tile_of(n)
        y = total[:, cols] + partial(last, 1 - m, cols)
        for r in range(clips):
            mixed = y[r * spots:(r + 1) * spots]
            factor = gate[r:r + 1, cols]
            after[r, :, cols] = (
                xin[r, :, cols].astype(jnp.float32) + factor * mixed).astype(xin.dtype)
            weighed = jnp.sum(cot[r, :, cols].astype(jnp.float32) * mixed, axis=0, keepdims=True)
            piece = math.gcd(tile, side)
            for i in range(tile // piece):
                at = n * (tile // piece) + i
                mine_terms[at // (side // piece), r:r + 1,
                           pl.ds(pl.multiple_of(at % (side // piece) * piece, piece), piece)] = (
                    weighed[:, i * piece:(i + 1) * piece])

    def t_copy(shift):
        frame, dp = peer(shift)
        return remote(mine_terms.at[frame % 2], terms.at[me], t_send.at[0], t_recv.at[me],
                      frame=frame, dp=dp)

    for shift in range(1, count):
        t_copy(shift).start()
    own_terms = pltpu.make_async_copy(mine_terms.at[c], terms.at[me], t_send.at[1])
    own_terms.start()
    result = pltpu.make_async_copy(after, next_ref, out_sem.at[0])
    result.start()

    arrived(wo.at[0], o_send)
    arrived(xbuf.at[0, pl.ds(0, lines - 1)], x_send.at[0])
    arrived(xbuf.at[0, pl.ds(0, lines)], x_send.at[1])
    arrived(xbuf.at[0], x_send.at[2])
    arrived(wbuf.at[:, :, pl.ds(0, 4 * part), :], w_send.at[0])
    arrived(wbuf.at[:, :, pl.ds(0, depth), :], w_send.at[1])
    arrived(wbuf.at[:, :, pl.ds(0, 6 * part), :], w_send.at[2])

    @pl.when(inner)
    def _():
        arrived(wbuf.at[:, :, pl.ds(0, 4 * part), :], w_send.at[3])

    arrived(abuf.at[:, pl.ds(0, frames - 1)], a_send)
    arrived(abuf, e_send)
    kind = lax.broadcasted_iota(jnp.int32, (kinds, HS), 0).astype(jnp.float32)

    def gathered(other):
        total = sums[c]
        for r in range(clips):
            mask = jnp.tile(terms[other, r:r + 1, side:] == kind, (1, side // HS))
            total += jnp.where(mask, terms[other, r:r + 1, :side], 0.0)
        sums[c] = total

    sums[c] = jnp.zeros((kinds, side), jnp.float32)
    own_terms.wait()
    gathered(me)
    with scope("terms"):
        @pl.loop(1, count)
        def _(shift):
            frame, dp = peer(count - shift)
            other = frame * dps + dp
            arrived(terms.at[other], t_recv.at[other])
            gathered(other)

    arrived(terms.at[pl.ds(0, count - 1)], t_send.at[0])
    swap = remote(sums.at[c], sums.at[c], g_send, g_recv, frame=other_core)
    swap.start()
    book_columns = book_ref[...].T

    def gradient(i):
        halves[i] = jnp.dot(book_columns, sums[i], precision=lax.Precision.HIGHEST,
                            preferred_element_type=jnp.float32)
        copy = pltpu.make_async_copy(
            halves.at[i], grad_ref.at[:, pl.ds(pl.multiple_of(i * side, HS), side)],
            out_sem.at[1 + i])
        copy.start()
        return copy

    first = gradient(c)
    arrived(sums.at[1 - c], g_recv)
    second = gradient(1 - c)
    swap.wait_send()
    first.wait()
    second.wait()
    result.wait()


def fused(dps, tokens, mask, embed, w_parts, w_out, cotangent, act_proj, codebook, action_idx, frames):
    clips, spots, width = tokens.shape
    parts, depth, heads_width = w_parts.shape
    groups = frames // clips
    per_group = heads_width // HS // groups
    count = frames * dps
    any_spec = pl.BlockSpec(memory_space=pl.ANY)
    vmem = pl.BlockSpec(memory_space=pltpu.VMEM)
    dma = pltpu.SemaphoreType.DMA
    return pl.pallas_call(
        functools.partial(fused_kernel, dps),
        in_specs=[any_spec, vmem, vmem] + [any_spec] * 4 + [vmem, pl.BlockSpec(memory_space=pltpu.SMEM)],
        out_specs=[any_spec] * 2,
        out_shape=[
            jax.ShapeDtypeStruct(tokens.shape, tokens.dtype),
            jax.ShapeDtypeStruct(act_proj.shape, jnp.float32),
        ],
        scratch_shapes=[
            pltpu.VMEM((2, frames, spots, width), jnp.bfloat16),
            pltpu.VMEM((per_group, parts, depth * frames, HS), jnp.bfloat16),
            pltpu.VMEM((1, frames, spots, parts * HS), jnp.float32),
            pltpu.VMEM((parts, frames, spots, HS), jnp.bfloat16),
            pltpu.VMEM((per_group, frames, spots, HS), jnp.bfloat16),
            pltpu.VMEM((2, per_group, clips * spots, groups * HS), jnp.bfloat16),
            pltpu.VMEM((2, heads_width, width), jnp.bfloat16),
            pltpu.VMEM((clips * spots, width), jnp.float32),
            pltpu.VMEM(tokens.shape, jnp.bfloat16),
            pltpu.VMEM(tokens.shape, jnp.bfloat16),
            pltpu.VMEM(act_proj.shape, jnp.float32),
            pltpu.VMEM((clips, width), jnp.float32),
            pltpu.VMEM((2, clips, width // 2 + HS), jnp.float32),
            pltpu.VMEM((count, clips, width // 2 + HS), jnp.float32),
            pltpu.VMEM((2, codebook.shape[0], width // 2), jnp.float32),
            pltpu.VMEM(tokens.shape, jnp.bfloat16),
            dma((2, frames, frames // 2)), dma((3,)),
            dma((per_group, frames, 2)), dma((4,)),
            dma((4, 4)), dma,
            dma((per_group, frames)), dma,
            dma((per_group,)), dma,
            dma((per_group + 1,)), dma((count,)), dma((2,)), dma((4,)),
            pltpu.VMEM((2, act_proj.shape[0], width // 2), jnp.float32), dma, dma,
        ],
        compiler_params=pltpu.CompilerParams(
            collective_id=2, has_side_effects=True, vmem_limit_bytes=60 << 20),
        name="fused",
    )(tokens, mask, embed, w_parts, w_out, cotangent, act_proj, codebook, action_idx)


def finish_kernel(next_ref, grad_ref, next_out, grad_out, rows, grads, load, store):
    copies = []
    for i, (source, middle, target) in enumerate(
            [(next_ref.at[r], rows.at[r], next_out.at[r]) for r in range(rows.shape[0])]
            + [(grad_ref, grads, grad_out)]):
        copies.append((pltpu.make_async_copy(source, middle, load.at[i]),
                       pltpu.make_async_copy(middle, target, store.at[i])))
    for first, _ in copies:
        first.start()
    for first, second in copies:
        first.wait()
        second.start()
    for _, second in copies:
        second.wait()


def finish(next_state, grad_proj):
    any_spec = pl.BlockSpec(memory_space=pl.ANY)
    count = next_state.shape[0] + 1
    return pl.pallas_call(
        finish_kernel,
        in_specs=[any_spec] * 2,
        out_specs=[any_spec] * 2,
        out_shape=[jax.ShapeDtypeStruct(a.shape, a.dtype) for a in (next_state, grad_proj)],
        scratch_shapes=[pltpu.VMEM(next_state.shape, next_state.dtype),
                        pltpu.VMEM(grad_proj.shape, grad_proj.dtype),
                        pltpu.SemaphoreType.DMA((count,)), pltpu.SemaphoreType.DMA((count,))],
        name="finish",
    )(next_state, grad_proj)


def gather_mp(block, size):
    if size != 2:
        return lax.all_gather(block, "mp", axis=block.ndim - 1, tiled=True)
    other = lax.ppermute(block, "mp", [(0, 1), (1, 0)])
    first = lax.axis_index("mp") == 0
    return jnp.concatenate(
        [jnp.where(first, block, other), jnp.where(first, other, block)], axis=-1
    )


def fits_fused(mps, dps, frames, clips, spots, width, depth, heads_width):
    groups = frames // clips
    return (mps == dps == clips == 2 and frames == groups * clips and groups == 2 * clips
            and heads_width == 3 * groups * HS
            and spots % 32 == 0 and depth % HS == 0
            and width * mps == depth * frames and heads_width % (16 * 16) == 0)


def body(mp_size, dp_size, tokens, token_mask, mask_embed, w_qkv, w_out, action_idx, codebook,
         act_proj, cotangent):
    clips, _, spots, width = tokens.shape
    heads_width = w_qkv.shape[2]
    depth = w_qkv.shape[0]
    xin = jnp.where(token_mask[..., None] == 1, mask_embed, tokens)
    frames = lax.axis_size("frame")
    if fits_fused(mp_size, dp_size, frames, clips, spots, width, depth, heads_width):
        next_state, grad_proj = fused(
            dp_size, tokens.reshape(clips, spots, width), token_mask, mask_embed, w_qkv.transpose(1, 0, 2), w_out,
            cotangent.reshape(clips, spots, width), act_proj, codebook,
            action_idx.reshape(clips), frames)
        next_state, grad_proj = finish(next_state.reshape(2 * clips, spots // 2, width), grad_proj)
        return (next_state.reshape(clips, 1, spots, width), grad_proj)
    else:
        share = depth // dp_size
        mine = lax.dynamic_slice_in_dim(
            w_qkv.reshape(depth, 3 * heads_width), lax.axis_index("dp") * share, share, axis=0
        )
        weights = lax.all_gather(mine, ("frame", "dp"), axis=0, tiled=True)
        if mp_size == 2:
            my_mp = lax.axis_index("mp")
            out_mine = lax.dynamic_slice_in_dim(w_out, my_mp * width, width, axis=1)
            out_other = lax.ppermute(
                lax.dynamic_slice_in_dim(w_out, (1 - my_mp) * width, width, axis=1),
                "mp", [(0, 1), (1, 0)])
        spread = lax.all_to_all(
            xin.reshape(clips, spots, width), "frame", split_axis=1, concat_axis=0, tiled=True
        )
        frames = spread.shape[0] // clips
        local = spread.shape[1]
        features = gather_mp(spread.reshape(frames * clips * local, width), mp_size)
        qkv = jnp.dot(features, weights, preferred_element_type=jnp.float32).astype(jnp.bfloat16)
        attn = attend(qkv.reshape(frames, clips * local, 3 * heads_width), frames, heads_width)
        back = lax.all_to_all(
            attn.reshape(frames * clips, local, heads_width), "frame", split_axis=0, concat_axis=1,
            tiled=True,
        )
        heads = back.reshape(clips * spots, heads_width)
        if mp_size == 2:
            other_heads = lax.ppermute(heads, "mp", [(0, 1), (1, 0)])
            mixed_rows = jnp.dot(heads, out_mine, preferred_element_type=jnp.float32) + jnp.dot(
                other_heads, out_other, preferred_element_type=jnp.float32)
        else:
            out_block = lax.all_to_all(w_out, "mp", split_axis=1, concat_axis=0, tiled=True)
            mixed_rows = jnp.dot(gather_mp(heads, mp_size), out_block,
                                 preferred_element_type=jnp.float32)
    mixed = mixed_rows.reshape(clips, 1, spots, width)
    onehot = (
        action_idx.reshape(clips)[:, None] == jnp.arange(codebook.shape[0])[None, :]
    ).astype(jnp.float32)
    codevec = jnp.dot(onehot, codebook, precision=lax.Precision.HIGHEST)
    gate = jnp.dot(codevec, act_proj, precision=lax.Precision.HIGHEST)
    next_state = (xin.astype(jnp.float32) + gate[:, None, None, :] * mixed).astype(jnp.bfloat16)
    dgate = jnp.sum(cotangent.astype(jnp.float32) * mixed, axis=2).reshape(clips, width)
    codes = codevec.shape[1]
    padded = jnp.pad(codevec, ((0, 0), (0, -codes % 128)))
    terms = spread_terms(jnp.concatenate([dgate, padded], axis=1), frames, dp_size)
    terms = terms.reshape(frames * dp_size * clips, -1)
    grad_proj = jnp.dot(
        terms[:, width : width + codes].T, terms[:, :width], precision=lax.Precision.HIGHEST)
    return (next_state, grad_proj)


def solution(mesh):
    in_specs = (
        P("dp", "frame", None, "mp"),
        P("dp", "frame", None),
        P("mp"),
        P("frame", None, "mp"),
        P("mp", None),
        P("dp", "frame"),
        P(),
        P(None, "mp"),
        P("dp", "frame", None, "mp"),
    )
    out_specs = (P("dp", "frame", None, "mp"), P(None, "mp"))
    return jax.shard_map(
        functools.partial(body, mesh.shape["mp"], mesh.shape["dp"]),
        mesh=mesh, in_specs=in_specs, out_specs=out_specs, check_vma=False,
    )
```

```python
import functools
import math

import jax
import jax.numpy as jnp
from jax import lax
from jax.experimental import pallas as pl
from jax.experimental.pallas import tpu as pltpu
from jax.sharding import PartitionSpec as P

HS = 128


def attend_kernel(frames, q_ref, k_ref, v_ref, o_ref):
    scale = 1.0 / math.sqrt(HS)
    for t in range(frames):
        q = q_ref[t].astype(jnp.float32) * scale
        scores = [
            jnp.sum(q * k_ref[u].astype(jnp.float32), axis=-1, keepdims=True) for u in range(t + 1)
        ]
        peak = functools.reduce(jnp.maximum, scores)
        weights = [jnp.exp(s - peak) for s in scores]
        total = functools.reduce(jnp.add, weights)
        accum = functools.reduce(
            jnp.add, [w * v_ref[u].astype(jnp.float32) for u, w in enumerate(weights)]
        )
        o_ref[t] = (accum / total).astype(o_ref.dtype)


def attend(qkv, frames, heads_width):
    rows = qkv.shape[1]
    heads = heads_width // HS
    spec = lambda part: pl.BlockSpec((frames, rows, HS), lambda h, part=part: (0, 0, part * heads + h))
    return pl.pallas_call(
        functools.partial(attend_kernel, frames),
        grid=(heads,),
        in_specs=[spec(0), spec(1), spec(2)],
        out_specs=spec(0),
        out_shape=jax.ShapeDtypeStruct((frames, rows, heads_width), jnp.bfloat16),
        cost_estimate=pl.CostEstimate(flops=4 * frames * frames * rows * heads_width,
                                      bytes_accessed=8 * frames * rows * heads_width,
                                      transcendentals=0),
        name="attend",
    )(qkv, qkv, qkv)


def spread_kernel(frames, dps, x_ref, o_ref, send_sem, recv_sem, own_sem):
    count = frames * dps
    me = lax.axis_index("frame") * dps + lax.axis_index("dp")
    barrier = pltpu.get_barrier_semaphore()

    def peer(shift):
        other = lax.rem(me + shift, count)
        return {"frame": other // dps, "dp": lax.rem(other, dps)}

    for shift in range(1, count):
        pl.semaphore_signal(barrier, inc=1, device_id=peer(shift),
                            device_id_type=pl.DeviceIdType.MESH)
    own = pltpu.make_async_copy(x_ref, o_ref.at[me], own_sem)
    own.start()
    pl.semaphore_wait(barrier, count - 1)
    copies = []
    for shift in range(1, count):
        copy = pltpu.make_async_remote_copy(
            src_ref=x_ref, dst_ref=o_ref.at[me], send_sem=send_sem.at[shift],
            recv_sem=recv_sem.at[shift], device_id=peer(shift),
            device_id_type=pl.DeviceIdType.MESH)
        copy.start()
        copies.append(copy)
    own.wait()
    for copy in copies:
        copy.wait()


def spread_terms(terms, frames, dps):
    count = frames * dps
    return pl.pallas_call(
        functools.partial(spread_kernel, frames, dps),
        in_specs=[pl.BlockSpec(memory_space=pltpu.VMEM)],
        out_specs=pl.BlockSpec(memory_space=pltpu.VMEM),
        out_shape=jax.ShapeDtypeStruct((count, *terms.shape), terms.dtype),
        scratch_shapes=[pltpu.SemaphoreType.DMA((count,)), pltpu.SemaphoreType.DMA((count,)),
                        pltpu.SemaphoreType.DMA],
        compiler_params=pltpu.CompilerParams(collective_id=1, has_side_effects=True),
        name="spread_terms",
    )(terms)


scope = jax.named_scope


def fused_kernel(dps, tokens_ref, mask_ref, embed_ref, w_ref, o_ref, cot_ref, act_ref, book_ref, idx_ref, next_ref, grad_ref,
                 xbuf, wbuf, acc, qkv, abuf, heads, wo, total, xin, cot, act, gate, mine_terms, terms, sums, after,
                 x_recv, x_send, w_recv, w_send, o_recv, o_send, a_recv, a_send, e_recv, e_send,
                 own_sem, t_recv, t_send, out_sem, halves, g_send, g_recv):
    mps, frames, spots, width = xbuf.shape
    per_group, _, _, _ = wbuf.shape
    depth = w_ref.shape[1]
    lines = frames // 2
    half = lines // 2
    part = depth // 2
    quarter = o_ref.shape[0] // 4
    f, m, d = lax.axis_index("frame"), lax.axis_index("mp"), lax.axis_index("dp")
    z, c = f // 2, f % 2
    hi, lo = z // 2, z % 2
    mine = hi * 2 + c
    inner = hi != lo
    pair, near, far = z + 1 - 2 * lo, half - hi, (lines - 1) * (1 - hi)
    other_core = 2 * z + 1 - c
    q0, q1 = d * 2 + c, (1 - d) * 2 + c

    def remote(source, target, send_sem, recv_sem, frame=f, mp=m, dp=d):
        return pltpu.make_async_remote_copy(
            src_ref=source, dst_ref=target, send_sem=send_sem, recv_sem=recv_sem,
            device_id={"frame": frame, "mp": mp, "dp": dp},
            device_id_type=pl.DeviceIdType.MESH)

    def arrived(target, recv_sem):
        pltpu.make_async_copy(target, target, recv_sem).wait()

    def rows_of(owner, which):
        return pl.ds(pl.multiple_of(owner * depth + which * part, part), part)

    def whole_rows(owner):
        return pl.ds(pl.multiple_of(owner * depth, depth), depth)

    def columns(group, head):
        return pl.ds(pl.multiple_of((group * per_group + head) * HS, HS), HS)

    def line(j):
        return jnp.where(j == 0, pair, jnp.where(j == 1, near, far))

    def source_of(j):
        return 2 * line(j // 2) + j % 2

    def w_direct(h, k):
        target = jnp.where(k < 2, pair, near)
        group = jnp.where(k < 2, hi, 1 - hi) * 2 + k % 2
        return remote(w_ref.at[:, pl.ds(pl.multiple_of(d * part, part), part), columns(group, h)],
                      wbuf.at[h, :, rows_of(f, d), :], w_send.at[0], w_recv.at[h, f, d],
                      frame=2 * target + k % 2)

    def w_partner(h):
        return remote(w_ref.at[:, :, columns(hi * 2 + 1 - c, h)], wbuf.at[h, :, whole_rows(f), :],
                      w_send.at[1], w_recv.at[h, f, 0], frame=other_core)

    def w_own(h):
        return pltpu.make_async_copy(w_ref.at[:, :, columns(mine, h)],
                                     wbuf.at[h, :, whole_rows(f), :], own_sem.at[h])

    def w_block(h, owner, which):
        return wbuf.at[h, :, rows_of(owner, which), :]

    def w_share(h, j):
        owner = source_of(j)
        block = w_block(h, owner, d)
        return remote(block, block, w_send.at[2], w_recv.at[h, owner, d], dp=1 - d)

    def w_relay(h, j):
        owner = source_of(j)
        block = w_block(h, owner, d)
        return remote(block, block, w_send.at[3], w_recv.at[h, owner, d],
                      frame=2 * pair + c)

    def forward_w(h, j):
        owner = source_of(j)
        with scope("fw"):
            arrived(w_block(h, owner, d), w_recv.at[h, owner, d])

        @pl.when(jnp.logical_and(inner, j >= 2))
        def _():
            w_relay(h, j).start()

        w_share(h, j).start()

    pieces = frames // mps

    def features(q):
        return pl.ds(pl.multiple_of(q * depth, depth), depth)

    def x_piece(which, owner, q):
        return xbuf.at[which, owner, :, features(q)]

    def x_direct(k, q):
        target = (z + k) % lines
        return remote(xin.at[target % 2, :, features(q)], x_piece(m, f, q), x_send.at[0],
                      x_recv.at[m, f, q], frame=2 * target + c)

    def x_across(owner, source, k, q):
        return remote(source, x_piece(m, owner, q), x_send.at[1], x_recv.at[m, owner, q],
                      mp=1 - m)

    def x_core(owner, source, which, k, q):
        return remote(source, x_piece(which, owner, q), x_send.at[2],
                      x_recv.at[which, owner, q], frame=other_core)

    def x_own(q):
        return xin.at[lo, :, features(q)]

    def x_owner(k):
        return f if k == 0 else 2 * line(k - 1) + c

    slices = o_recv.shape[1]
    share = quarter // slices

    def o_rows(which, i):
        return pl.ds(pl.multiple_of(which * quarter + i * share, share), share)

    def o_piece(which, i):
        return wo.at[1 - m, o_rows(which, i), :]

    def o_across(i):
        return remote(
            o_ref.at[o_rows(q0, i), pl.ds(pl.multiple_of((1 - m) * width, width), width)],
            wo.at[m, o_rows(q0, i), :], o_send, o_recv.at[q0, i], mp=1 - m)

    def o_share(i):
        return remote(o_piece(q0, i), o_piece(q0, i), o_send, o_recv.at[q0, i], dp=1 - d)

    def o_core(which, i, slot):
        return remote(o_piece(which, i), o_piece(which, i), o_send,
                      o_recv.at[which, i], frame=other_core)

    def forward_o(i):
        with scope("o_0"):
            arrived(o_piece(q0, i), o_recv.at[q0, i])
        o_share(i).start()
        o_core(q0, i, 2).start()

    def attn_block(which, owner, h):
        group = (owner // 4) * 2 + owner % 2
        clip = (owner // 2) % 2
        return heads.at[which, h, pl.ds(pl.multiple_of(clip * spots, spots), spots),
                        pl.ds(pl.multiple_of(group * HS, HS), HS)]

    def a_direct(h, k):
        target = (f + k) % frames
        return remote(abuf.at[h, target], attn_block(m, f, h), a_send, a_recv.at[h, f],
                      frame=target)

    def a_own(h):
        return pltpu.make_async_copy(abuf.at[h, f], attn_block(m, f, h), a_recv.at[h, f])

    def a_across(h, owner):
        block = attn_block(m, owner, h)
        return remote(block, block, e_send, e_recv.at[h], mp=1 - m)

    def forward_block(h, owner):
        arrived(attn_block(m, owner, h), a_recv.at[h, owner])
        a_across(h, owner).start()

    def forward_attn(h):
        @pl.loop(0, frames)
        def _(k):
            forward_block(h, (f + frames - k) % frames)

    def forward_from_inner(h):
        @pl.loop(frames // 4, frames - frames // 4)
        def _(owner):
            forward_block(h, owner)

    def forward_from_outer(h):
        @pl.loop(0, frames // 2)
        def _(i):
            forward_block(h, jnp.where(i < frames // 4, i, i + frames // 2))

    barrier = pltpu.get_barrier_semaphore()
    clips = xin.shape[0]
    tile = math.gcd(width, 512)

    def tile_of(n):
        return pl.ds(pl.multiple_of(n * tile, tile), tile)

    count = frames * dps
    me = f * dps + d

    def peer(shift):
        other = (me + shift) % count
        return other // dps, other % dps

    for shift in range(1, count):
        frame, dp = peer(shift)
        pl.semaphore_signal(barrier, inc=1, device_id={"frame": frame, "mp": m, "dp": dp},
                            device_id_type=pl.DeviceIdType.MESH)
    pl.semaphore_signal(barrier, inc=1, device_id={"frame": f, "mp": 1 - m, "dp": d},
                        device_id_type=pl.DeviceIdType.MESH)
    loads = [pltpu.make_async_copy(source, target, out_sem.at[i]) for i, (source, target) in enumerate((
        (tokens_ref, xin), (cot_ref, cot), (act_ref, act),
        (o_ref.at[:, pl.ds(pl.multiple_of(m * width, width), width)], wo.at[m])))]
    own_x = pltpu.make_async_copy(xin.at[lo], xbuf.at[m, f], own_sem.at[per_group])
    for h in range(per_group):
        w_own(h).start()
    loads[0].start()
    pl.semaphore_wait(barrier, count)

    last = per_group - 1
    outer = jnp.logical_not(inner)

    def send_tokens(q):
        for k in range(1, lines):
            x_direct(k, q).start()

    def send_weights(h):
        for k in range(4):
            w_direct(h, k).start()

    send_weights(0)

    @pl.loop(0, slices)
    def _(i):
        o_across(i).start()

    loads[0].wait()
    gate[0:1, :] = embed_ref[...].astype(jnp.float32)[None, :]
    same = (lax.broadcasted_iota(jnp.int32, (spots, spots), 0)
            == lax.broadcasted_iota(jnp.int32, (spots, spots), 1))
    for r in range(clips):
        row = jnp.broadcast_to(mask_ref[r].astype(jnp.float32), (spots, spots))
        masked = jnp.sum(jnp.where(same, row, 0.0), axis=1, keepdims=True) == 1.0

        @pl.loop(0, width // tile)
        def _(n):
            cols = tile_of(n)
            xin[r, :, cols] = jnp.where(masked, gate[0:1, cols],
                                        xin[r, :, cols].astype(jnp.float32)).astype(xin.dtype)

    own_x.start()
    send_tokens(0)

    w_partner(0).start()

    @pl.loop(0, pieces)
    def _(q):
        x_core(f, x_own(q), m, 0, q).start()

    @pl.loop(0, 2)
    def _(j):
        forward_w(0, j)

    for copy in loads[1:]:
        copy.start()

    send_tokens(1)

    @pl.when(inner)
    def _():
        @pl.loop(2, 6)
        def _(j):
            forward_w(0, j)

    forward_o(0)
    forward_o(1)

    @pl.when(outer)
    def _():
        forward_w(0, 2)
        forward_w(0, 3)

    forward_o(2)

    def matmul(slot, h, owner, first):
        side = owner // (frames // mps)
        col = pl.multiple_of((owner % (frames // mps)) * depth, depth)
        w = jnp.concatenate([wbuf[h, p, whole_rows(owner), :] for p in range(3)], axis=1)
        step = frames // 2

        @pl.loop(0, 2)
        def _(i):
            x = xbuf[side, pl.ds(i * step, step), :, pl.ds(col, depth)].reshape(step * spots, depth)
            y = jnp.dot(x, w, preferred_element_type=jnp.float32).reshape(step, spots, 3 * HS)

            @pl.when(first)
            def _():
                acc[slot, pl.ds(i * step, step)] = y

            @pl.when(jnp.logical_not(first))
            def _():
                acc[slot, pl.ds(i * step, step)] += y

    def attend_rows(h, i, rows):
        scale = 1.0 / math.sqrt(HS)
        at = pl.ds(pl.multiple_of(i * rows, rows), rows)
        for t in range(frames):
            q = qkv[0, t, at, :].astype(jnp.float32) * scale
            scores = [jnp.sum(q * qkv[1, u, at, :].astype(jnp.float32), axis=-1, keepdims=True)
                      for u in range(t + 1)]
            peak = functools.reduce(jnp.maximum, scores)
            weights = [jnp.exp(s - peak) for s in scores]
            total = functools.reduce(jnp.add, weights)
            accum = functools.reduce(
                jnp.add,
                [w * qkv[2, u, at, :].astype(jnp.float32) for u, w in enumerate(weights)])
            abuf[h, t, at, :] = (accum / total).astype(abuf.dtype)

    def attention(slot, h):
        @pl.loop(0, frames)
        def _(t):
            for p in range(3):
                qkv[p, t] = acc[slot, t, :, p * HS:(p + 1) * HS].astype(qkv.dtype)

        rows = math.gcd(spots, 32)

        @pl.loop(0, spots // rows)
        def _(i):
            with scope("att"):
                attend_rows(h, i, rows)

        a_own(h).start()

        @pl.loop(1, frames)
        def _(k):
            a_direct(h, k).start()

    def ready_w(h, j):
        owner = source_of(j)
        arrived(w_block(h, owner, 1 - d), w_recv.at[h, owner, 1 - d])

    def ready_chip(h):
        w_own(h).wait()
        arrived(wbuf.at[h, :, whole_rows(other_core), :], w_recv.at[h, other_core, 0])

    def ready_w(h, j):
        owner = source_of(j)
        arrived(w_block(h, owner, 1 - d), w_recv.at[h, owner, 1 - d])

    def ready_chip(h):
        w_own(h).wait()
        arrived(wbuf.at[h, :, whole_rows(other_core), :], w_recv.at[h, other_core, 0])

    for h in range(1, per_group):
        w_partner(h).start()

    @pl.loop(0, pieces + 3)
    def _(q):
        @pl.when(q < pieces)
        def _():
            x_across(f, x_own(q), 0, q).start()
            for k in range(1, lines):
                owner = x_owner(k)
                block = x_piece(m, owner, q)
                with scope("x_own"):
                    arrived(block, x_recv.at[m, owner, q])
                x_across(owner, block, k, q).start()
                x_core(owner, block, m, k, q).start()

        @pl.when(q < pieces - 2)
        def _():
            send_tokens(q + 2)

        @pl.when(q == pieces - 2 - jnp.where(outer, 1, 0))
        def _():
            send_weights(1)

        @pl.when(q == 0)
        def _():
            forward_o(3)

            @pl.when(outer)
            def _():
                forward_w(0, 4)
                forward_w(0, 5)

        @pl.when(jnp.logical_and(q >= 2, q < pieces + 2))
        def _():
            for k in range(lines):
                owner = x_owner(k)
                block = x_piece(1 - m, owner, q - 2)
                with scope("x_other"):
                    arrived(block, x_recv.at[1 - m, owner, q - 2])
                x_core(owner, block, 1 - m, k, q - 2).start()

        @pl.when(q == 4)
        def _():
            for h in range(2, per_group):
                send_weights(h)

        @pl.when(jnp.logical_and(q >= 4, q < 6))
        def _():
            forward_w(1, 3 * (q - 4))
            forward_w(1, 3 * (q - 4) + 1)
            forward_w(1, 3 * (q - 4) + 2)

        @pl.when(q == 6)
        def _():
            forward_w(2, 0)
            forward_w(2, 1)

        @pl.when(q == 3)
        def _():
            with scope("w_0"):
                own_x.wait()
                ready_chip(0)
                for j in range(6):
                    ready_w(0, j)

        @pl.when(q >= 3)
        def _():
            with scope("x_core"):
                for k in range(lines):
                    owner = x_owner(k) + 1 - 2 * c
                    for which in range(mps):
                        arrived(x_piece(which, owner, q - 3), x_recv.at[which, owner, q - 3])

            @pl.loop(0, mps)
            def _(side):
                with scope("mm0"):
                    matmul(0, 0, side * pieces + q - 3, jnp.logical_and(side == 0, q == 3))

    @pl.loop(0, slices)
    def _(i):
        with scope("o_1"):
            arrived(o_piece(q1, i), o_recv.at[q1, i])
        o_core(q1, i, 3).start()

    attention(0, 0)

    for copy in loads[1:]:
        copy.wait()
    groups = heads.shape[3] // HS
    codes = act.shape[0]
    kinds = book_ref.shape[0]
    index = jnp.concatenate([jnp.full((1, kinds), idx_ref[r], jnp.int32) for r in range(clips)], axis=0)
    onehot = (index == lax.broadcasted_iota(jnp.int32, (clips, kinds), 1)).astype(jnp.float32)
    codevec = jnp.dot(onehot, book_ref[...], precision=lax.Precision.HIGHEST,
                      preferred_element_type=jnp.float32)
    gate[...] = jnp.dot(codevec, act[...], precision=lax.Precision.HIGHEST,
                        preferred_element_type=jnp.float32)
    marks = jnp.concatenate(
        [jnp.full((1, HS), idx_ref[r], jnp.int32).astype(jnp.float32) for r in range(clips)], axis=0)
    side = width // 2
    for half_of in range(2):
        mine_terms[half_of, :, side:] = marks

    @pl.loop(0, last * frames)
    def _(i):
        h, jj = 1 + i // frames, i % frames

        @pl.when(jnp.logical_and(inner, jnp.logical_and(h < last, jj >= 4)))
        def _():
            forward_w(h + 1, jj - 2)

        @pl.when(jnp.logical_and(outer, jnp.logical_and(h < last, jj >= 6)))
        def _():
            forward_w(h + 1, jj - 4)

        @pl.when(jnp.logical_and(outer, jnp.logical_and(h > 1, jnp.logical_and(jj >= 4, jj < 6))))
        def _():
            forward_w(h, jj)

        @pl.when(jj == 0)
        def _():
            ready_chip(h)

        @pl.when(jj >= 2)
        def _():
            with scope("w_y"):
                ready_w(h, jnp.maximum(jj - 2, 0))

        owner = jnp.where(jj == 0, f, jnp.where(jj == 1, other_core, source_of(jnp.maximum(jj - 2, 0))))
        with scope("mm"):
            matmul(0, h, owner, jj == 0)

        @pl.when(jj == frames - 1)
        def _():
            attention(0, h)

        @pl.when(jnp.logical_and(h == last, jj == 5))
        def _():
            with scope("fa"):
                forward_attn(last - 1)

        @pl.when(jnp.logical_and(h == last, jj == 3))
        def _():
            for before in range(last - 1):
                with scope("fa"):
                    forward_attn(before)

    forward_from_inner(last)

    @pl.loop(0, slices)
    def _(i):
        for which in (d * 2 + 1 - c, (1 - d) * 2 + 1 - c):
            arrived(o_piece(which, i), o_recv.at[which, i])

    def partial(h, side, cols):
        w = jnp.concatenate(
            [wo[side, pl.ds(pl.multiple_of((g * per_group + h) * HS, HS), HS), cols]
             for g in range(groups)], axis=0)
        return jnp.dot(heads[side, h], w, preferred_element_type=jnp.float32)

    def exchanged(h):
        arrived(heads.at[1 - m, h], e_recv.at[h])

    @pl.loop(0, last)
    def _(h):
        with scope("exchanged"):
            exchanged(h)

        @pl.loop(0, width // tile)
        def _(n):
            cols = tile_of(n)
            y = partial(h, 0, cols) + partial(h, 1, cols)

            @pl.when(h == 0)
            def _():
                total[:, cols] = y

            @pl.when(h > 0)
            def _():
                total[:, cols] += y

    forward_from_outer(last)

    @pl.loop(0, width // tile)
    def _(n):
        cols = tile_of(n)
        total[:, cols] += partial(last, m, cols)

    with scope("exchanged"):
        exchanged(last)

    @pl.loop(0, width // tile)
    def _(n):
        cols = tile_of(n)
        y = total[:, cols] + partial(last, 1 - m, cols)
        for r in range(clips):
            mixed = y[r * spots:(r + 1) * spots]
            factor = gate[r:r + 1, cols]
            after[r, :, cols] = (
                xin[r, :, cols].astype(jnp.float32) + factor * mixed).astype(xin.dtype)
            weighed = jnp.sum(cot[r, :, cols].astype(jnp.float32) * mixed, axis=0, keepdims=True)
            piece = math.gcd(tile, side)
            for i in range(tile // piece):
                at = n * (tile // piece) + i
                mine_terms[at // (side // piece), r:r + 1,
                           pl.ds(pl.multiple_of(at % (side // piece) * piece, piece), piece)] = (
                    weighed[:, i * piece:(i + 1) * piece])

    def t_copy(shift):
        frame, dp = peer(shift)
        return remote(mine_terms.at[frame % 2], terms.at[me], t_send.at[0], t_recv.at[me],
                      frame=frame, dp=dp)

    for shift in range(1, count):
        t_copy(shift).start()
    own_terms = pltpu.make_async_copy(mine_terms.at[c], terms.at[me], t_send.at[1])
    own_terms.start()
    result = pltpu.make_async_copy(after, next_ref, out_sem.at[0])
    result.start()

    arrived(wo.at[0], o_send)
    arrived(xbuf.at[0, pl.ds(0, lines - 1)], x_send.at[0])
    arrived(xbuf.at[0, pl.ds(0, lines)], x_send.at[1])
    arrived(xbuf.at[0], x_send.at[2])
    arrived(wbuf.at[:, :, pl.ds(0, 4 * part), :], w_send.at[0])
    arrived(wbuf.at[:, :, pl.ds(0, depth), :], w_send.at[1])
    arrived(wbuf.at[:, :, pl.ds(0, 6 * part), :], w_send.at[2])

    @pl.when(inner)
    def _():
        arrived(wbuf.at[:, :, pl.ds(0, 4 * part), :], w_send.at[3])

    arrived(abuf.at[:, pl.ds(0, frames - 1)], a_send)
    arrived(abuf, e_send)
    kind = lax.broadcasted_iota(jnp.int32, (kinds, HS), 0).astype(jnp.float32)

    def gathered(other):
        total = sums[c]
        for r in range(clips):
            mask = jnp.tile(terms[other, r:r + 1, side:] == kind, (1, side // HS))
            total += jnp.where(mask, terms[other, r:r + 1, :side], 0.0)
        sums[c] = total

    sums[c] = jnp.zeros((kinds, side), jnp.float32)
    own_terms.wait()
    gathered(me)
    with scope("terms"):
        @pl.loop(1, count)
        def _(shift):
            frame, dp = peer(count - shift)
            other = frame * dps + dp
            arrived(terms.at[other], t_recv.at[other])
            gathered(other)

    arrived(terms.at[pl.ds(0, count - 1)], t_send.at[0])
    swap = remote(sums.at[c], sums.at[c], g_send, g_recv, frame=other_core)
    swap.start()
    book_columns = book_ref[...].T

    def gradient(i):
        halves[i] = jnp.dot(book_columns, sums[i], precision=lax.Precision.HIGHEST,
                            preferred_element_type=jnp.float32)
        copy = pltpu.make_async_copy(
            halves.at[i], grad_ref.at[:, pl.ds(pl.multiple_of(i * side, HS), side)],
            out_sem.at[1 + i])
        copy.start()
        return copy

    first = gradient(c)
    arrived(sums.at[1 - c], g_recv)
    second = gradient(1 - c)
    swap.wait_send()
    first.wait()
    second.wait()
    result.wait()


def fused(dps, tokens, mask, embed, w_parts, w_out, cotangent, act_proj, codebook, action_idx, frames):
    clips, spots, width = tokens.shape
    parts, depth, heads_width = w_parts.shape
    groups = frames // clips
    per_group = heads_width // HS // groups
    count = frames * dps
    any_spec = pl.BlockSpec(memory_space=pl.ANY)
    vmem = pl.BlockSpec(memory_space=pltpu.VMEM)
    dma = pltpu.SemaphoreType.DMA
    return pl.pallas_call(
        functools.partial(fused_kernel, dps),
        in_specs=[any_spec, vmem, vmem] + [any_spec] * 4 + [vmem, pl.BlockSpec(memory_space=pltpu.SMEM)],
        out_specs=[any_spec] * 2,
        out_shape=[
            jax.ShapeDtypeStruct(tokens.shape, tokens.dtype),
            jax.ShapeDtypeStruct(act_proj.shape, jnp.float32),
        ],
        scratch_shapes=[
            pltpu.VMEM((2, frames, spots, width), jnp.bfloat16),
            pltpu.VMEM((per_group, parts, depth * frames, HS), jnp.bfloat16),
            pltpu.VMEM((1, frames, spots, parts * HS), jnp.float32),
            pltpu.VMEM((parts, frames, spots, HS), jnp.bfloat16),
            pltpu.VMEM((per_group, frames, spots, HS), jnp.bfloat16),
            pltpu.VMEM((2, per_group, clips * spots, groups * HS), jnp.bfloat16),
            pltpu.VMEM((2, heads_width, width), jnp.bfloat16),
            pltpu.VMEM((clips * spots, width), jnp.float32),
            pltpu.VMEM(tokens.shape, jnp.bfloat16),
            pltpu.VMEM(tokens.shape, jnp.bfloat16),
            pltpu.VMEM(act_proj.shape, jnp.float32),
            pltpu.VMEM((clips, width), jnp.float32),
            pltpu.VMEM((2, clips, width // 2 + HS), jnp.float32),
            pltpu.VMEM((count, clips, width // 2 + HS), jnp.float32),
            pltpu.VMEM((2, codebook.shape[0], width // 2), jnp.float32),
            pltpu.VMEM(tokens.shape, jnp.bfloat16),
            dma((2, frames, frames // 2)), dma((3,)),
            dma((per_group, frames, 2)), dma((4,)),
            dma((4, 4)), dma,
            dma((per_group, frames)), dma,
            dma((per_group,)), dma,
            dma((per_group + 1,)), dma((count,)), dma((2,)), dma((4,)),
            pltpu.VMEM((2, act_proj.shape[0], width // 2), jnp.float32), dma, dma,
        ],
        compiler_params=pltpu.CompilerParams(
            collective_id=2, has_side_effects=True, vmem_limit_bytes=60 << 20),
        name="fused",
    )(tokens, mask, embed, w_parts, w_out, cotangent, act_proj, codebook, action_idx)


def finish_kernel(next_ref, grad_ref, next_out, grad_out, rows, grads, load, store):
    copies = []
    for i, (source, middle, target) in enumerate(
            [(next_ref.at[r], rows.at[r], next_out.at[r]) for r in range(rows.shape[0])]
            + [(grad_ref, grads, grad_out)]):
        copies.append((pltpu.make_async_copy(source, middle, load.at[i]),
                       pltpu.make_async_copy(middle, target, store.at[i])))
    for first, _ in copies:
        first.start()
    for first, second in copies:
        first.wait()
        second.start()
    for _, second in copies:
        second.wait()


def finish(next_state, grad_proj):
    any_spec = pl.BlockSpec(memory_space=pl.ANY)
    count = next_state.shape[0] + 1
    return pl.pallas_call(
        finish_kernel,
        in_specs=[any_spec] * 2,
        out_specs=[any_spec] * 2,
        out_shape=[jax.ShapeDtypeStruct(a.shape, a.dtype) for a in (next_state, grad_proj)],
        scratch_shapes=[pltpu.VMEM(next_state.shape, next_state.dtype),
                        pltpu.VMEM(grad_proj.shape, grad_proj.dtype),
                        pltpu.SemaphoreType.DMA((count,)), pltpu.SemaphoreType.DMA((count,))],
        name="finish",
    )(next_state, grad_proj)


def gather_mp(block, size):
    if size != 2:
        return lax.all_gather(block, "mp", axis=block.ndim - 1, tiled=True)
    other = lax.ppermute(block, "mp", [(0, 1), (1, 0)])
    first = lax.axis_index("mp") == 0
    return jnp.concatenate(
        [jnp.where(first, block, other), jnp.where(first, other, block)], axis=-1
    )


def fits_fused(mps, dps, frames, clips, spots, width, depth, heads_width):
    groups = frames // clips
    return (mps == dps == clips == 2 and frames == groups * clips and groups == 2 * clips
            and heads_width == 3 * groups * HS
            and spots % 32 == 0 and depth % HS == 0
            and width * mps == depth * frames and heads_width % (16 * 16) == 0)


def body(mp_size, dp_size, tokens, token_mask, mask_embed, w_qkv, w_out, action_idx, codebook,
         act_proj, cotangent):
    clips, _, spots, width = tokens.shape
    heads_width = w_qkv.shape[2]
    depth = w_qkv.shape[0]
    xin = jnp.where(token_mask[..., None] == 1, mask_embed, tokens)
    frames = lax.axis_size("frame")
    if fits_fused(mp_size, dp_size, frames, clips, spots, width, depth, heads_width):
        next_state, grad_proj = fused(
            dp_size, tokens.reshape(clips, spots, width), token_mask, mask_embed, w_qkv.transpose(1, 0, 2), w_out,
            cotangent.reshape(clips, spots, width), act_proj, codebook,
            action_idx.reshape(clips), frames)
        next_state, grad_proj = finish(next_state.reshape(2 * clips, spots // 2, width), grad_proj)
        return (next_state.reshape(clips, 1, spots, width), grad_proj)
    else:
        share = depth // dp_size
        mine = lax.dynamic_slice_in_dim(
            w_qkv.reshape(depth, 3 * heads_width), lax.axis_index("dp") * share, share, axis=0
        )
        weights = lax.all_gather(mine, ("frame", "dp"), axis=0, tiled=True)
        if mp_size == 2:
            my_mp = lax.axis_index("mp")
            out_mine = lax.dynamic_slice_in_dim(w_out, my_mp * width, width, axis=1)
            out_other = lax.ppermute(
                lax.dynamic_slice_in_dim(w_out, (1 - my_mp) * width, width, axis=1),
                "mp", [(0, 1), (1, 0)])
        spread = lax.all_to_all(
            xin.reshape(clips, spots, width), "frame", split_axis=1, concat_axis=0, tiled=True
        )
        frames = spread.shape[0] // clips
        local = spread.shape[1]
        features = gather_mp(spread.reshape(frames * clips * local, width), mp_size)
        qkv = jnp.dot(features, weights, preferred_element_type=jnp.float32).astype(jnp.bfloat16)
        attn = attend(qkv.reshape(frames, clips * local, 3 * heads_width), frames, heads_width)
        back = lax.all_to_all(
            attn.reshape(frames * clips, local, heads_width), "frame", split_axis=0, concat_axis=1,
            tiled=True,
        )
        heads = back.reshape(clips * spots, heads_width)
        if mp_size == 2:
            other_heads = lax.ppermute(heads, "mp", [(0, 1), (1, 0)])
            mixed_rows = jnp.dot(heads, out_mine, preferred_element_type=jnp.float32) + jnp.dot(
                other_heads, out_other, preferred_element_type=jnp.float32)
        else:
            out_block = lax.all_to_all(w_out, "mp", split_axis=1, concat_axis=0, tiled=True)
            mixed_rows = jnp.dot(gather_mp(heads, mp_size), out_block,
                                 preferred_element_type=jnp.float32)
    mixed = mixed_rows.reshape(clips, 1, spots, width)
    onehot = (
        action_idx.reshape(clips)[:, None] == jnp.arange(codebook.shape[0])[None, :]
    ).astype(jnp.float32)
    codevec = jnp.dot(onehot, codebook, precision=lax.Precision.HIGHEST)
    gate = jnp.dot(codevec, act_proj, precision=lax.Precision.HIGHEST)
    next_state = (xin.astype(jnp.float32) + gate[:, None, None, :] * mixed).astype(jnp.bfloat16)
    dgate = jnp.sum(cotangent.astype(jnp.float32) * mixed, axis=2).reshape(clips, width)
    codes = codevec.shape[1]
    padded = jnp.pad(codevec, ((0, 0), (0, -codes % 128)))
    terms = spread_terms(jnp.concatenate([dgate, padded], axis=1), frames, dp_size)
    terms = terms.reshape(frames * dp_size * clips, -1)
    grad_proj = jnp.dot(
        terms[:, width : width + codes].T, terms[:, :width], precision=lax.Precision.HIGHEST)
    return (next_state, grad_proj)


def solution(mesh):
    in_specs = (
        P("dp", "frame", None, "mp"),
        P("dp", "frame", None),
        P("mp"),
        P("frame", None, "mp"),
        P("mp", None),
        P("dp", "frame"),
        P(),
        P(None, "mp"),
        P("dp", "frame", None, "mp"),
    )
    out_specs = (P("dp", "frame", None, "mp"), P(None, "mp"))
    return jax.shard_map(
        functools.partial(body, mesh.shape["mp"], mesh.shape["dp"]),
        mesh=mesh, in_specs=in_specs, out_specs=out_specs, check_vma=False,
    )
```

```python
import functools
import math

import jax
import jax.numpy as jnp
from jax import lax
from jax.experimental import pallas as pl
from jax.experimental.pallas import tpu as pltpu
from jax.sharding import PartitionSpec as P

HS = 128


def attend_kernel(frames, q_ref, k_ref, v_ref, o_ref):
    scale = 1.0 / math.sqrt(HS)
    for t in range(frames):
        q = q_ref[t].astype(jnp.float32) * scale
        scores = [
            jnp.sum(q * k_ref[u].astype(jnp.float32), axis=-1, keepdims=True) for u in range(t + 1)
        ]
        peak = functools.reduce(jnp.maximum, scores)
        weights = [jnp.exp(s - peak) for s in scores]
        total = functools.reduce(jnp.add, weights)
        accum = functools.reduce(
            jnp.add, [w * v_ref[u].astype(jnp.float32) for u, w in enumerate(weights)]
        )
        o_ref[t] = (accum / total).astype(o_ref.dtype)


def attend(qkv, frames, heads_width):
    rows = qkv.shape[1]
    heads = heads_width // HS
    spec = lambda part: pl.BlockSpec((frames, rows, HS), lambda h, part=part: (0, 0, part * heads + h))
    return pl.pallas_call(
        functools.partial(attend_kernel, frames),
        grid=(heads,),
        in_specs=[spec(0), spec(1), spec(2)],
        out_specs=spec(0),
        out_shape=jax.ShapeDtypeStruct((frames, rows, heads_width), jnp.bfloat16),
        cost_estimate=pl.CostEstimate(flops=4 * frames * frames * rows * heads_width,
                                      bytes_accessed=8 * frames * rows * heads_width,
                                      transcendentals=0),
        name="attend",
    )(qkv, qkv, qkv)


def spread_kernel(frames, dps, x_ref, o_ref, send_sem, recv_sem, own_sem):
    count = frames * dps
    me = lax.axis_index("frame") * dps + lax.axis_index("dp")
    barrier = pltpu.get_barrier_semaphore()

    def peer(shift):
        other = lax.rem(me + shift, count)
        return {"frame": other // dps, "dp": lax.rem(other, dps)}

    for shift in range(1, count):
        pl.semaphore_signal(barrier, inc=1, device_id=peer(shift),
                            device_id_type=pl.DeviceIdType.MESH)
    own = pltpu.make_async_copy(x_ref, o_ref.at[me], own_sem)
    own.start()
    pl.semaphore_wait(barrier, count - 1)
    copies = []
    for shift in range(1, count):
        copy = pltpu.make_async_remote_copy(
            src_ref=x_ref, dst_ref=o_ref.at[me], send_sem=send_sem.at[shift],
            recv_sem=recv_sem.at[shift], device_id=peer(shift),
            device_id_type=pl.DeviceIdType.MESH)
        copy.start()
        copies.append(copy)
    own.wait()
    for copy in copies:
        copy.wait()


def spread_terms(terms, frames, dps):
    count = frames * dps
    return pl.pallas_call(
        functools.partial(spread_kernel, frames, dps),
        in_specs=[pl.BlockSpec(memory_space=pltpu.VMEM)],
        out_specs=pl.BlockSpec(memory_space=pltpu.VMEM),
        out_shape=jax.ShapeDtypeStruct((count, *terms.shape), terms.dtype),
        scratch_shapes=[pltpu.SemaphoreType.DMA((count,)), pltpu.SemaphoreType.DMA((count,)),
                        pltpu.SemaphoreType.DMA],
        compiler_params=pltpu.CompilerParams(collective_id=1, has_side_effects=True),
        name="spread_terms",
    )(terms)


scope = jax.named_scope


def fused_kernel(dps, tokens_ref, mask_ref, embed_ref, w_ref, o_ref, cot_ref, act_ref, book_ref, idx_ref, next_ref, grad_ref,
                 xbuf, wbuf, acc, qkv, abuf, heads, wo, total, xin, cot, act, gate, mine_terms, terms, sums, after,
                 x_recv, x_send, w_recv, w_send, o_recv, o_send, a_recv, a_send, e_recv, e_send,
                 own_sem, t_recv, t_send, out_sem, halves, g_send, g_recv):
    mps, frames, spots, width = xbuf.shape
    per_group, _, _, _ = wbuf.shape
    depth = w_ref.shape[1]
    lines = frames // 2
    half = lines // 2
    part = depth // 2
    quarter = o_ref.shape[0] // 4
    f, m, d = lax.axis_index("frame"), lax.axis_index("mp"), lax.axis_index("dp")
    z, c = f // 2, f % 2
    hi, lo = z // 2, z % 2
    mine = hi * 2 + c
    inner = hi != lo
    pair, near, far = z + 1 - 2 * lo, half - hi, (lines - 1) * (1 - hi)
    other_core = 2 * z + 1 - c
    q0, q1 = d * 2 + c, (1 - d) * 2 + c

    def remote(source, target, send_sem, recv_sem, frame=f, mp=m, dp=d):
        return pltpu.make_async_remote_copy(
            src_ref=source, dst_ref=target, send_sem=send_sem, recv_sem=recv_sem,
            device_id={"frame": frame, "mp": mp, "dp": dp},
            device_id_type=pl.DeviceIdType.MESH)

    def arrived(target, recv_sem):
        pltpu.make_async_copy(target, target, recv_sem).wait()

    def rows_of(owner, which):
        return pl.ds(pl.multiple_of(owner * depth + which * part, part), part)

    def whole_rows(owner):
        return pl.ds(pl.multiple_of(owner * depth, depth), depth)

    def columns(group, head):
        return pl.ds(pl.multiple_of((group * per_group + head) * HS, HS), HS)

    def line(j):
        return jnp.where(j == 0, pair, jnp.where(j == 1, near, far))

    def source_of(j):
        return 2 * line(j // 2) + j % 2

    def w_direct(h, k):
        target = jnp.where(k < 2, pair, near)
        group = jnp.where(k < 2, hi, 1 - hi) * 2 + k % 2
        return remote(w_ref.at[:, pl.ds(pl.multiple_of(d * part, part), part), columns(group, h)],
                      wbuf.at[h, :, rows_of(f, d), :], w_send.at[0], w_recv.at[h, f, d],
                      frame=2 * target + k % 2)

    def w_partner(h):
        return remote(w_ref.at[:, :, columns(hi * 2 + 1 - c, h)], wbuf.at[h, :, whole_rows(f), :],
                      w_send.at[1], w_recv.at[h, f, 0], frame=other_core)

    def w_own(h):
        return pltpu.make_async_copy(w_ref.at[:, :, columns(mine, h)],
                                     wbuf.at[h, :, whole_rows(f), :], own_sem.at[h])

    def w_block(h, owner, which):
        return wbuf.at[h, :, rows_of(owner, which), :]

    def w_share(h, j):
        owner = source_of(j)
        block = w_block(h, owner, d)
        return remote(block, block, w_send.at[2], w_recv.at[h, owner, d], dp=1 - d)

    def w_relay(h, j):
        owner = source_of(j)
        block = w_block(h, owner, d)
        return remote(block, block, w_send.at[3], w_recv.at[h, owner, d],
                      frame=2 * pair + c)

    def forward_w(h, j):
        owner = source_of(j)
        with scope("fw"):
            arrived(w_block(h, owner, d), w_recv.at[h, owner, d])

        @pl.when(jnp.logical_and(inner, j >= 2))
        def _():
            w_relay(h, j).start()

        w_share(h, j).start()

    pieces = frames // mps

    def features(q):
        return pl.ds(pl.multiple_of(q * depth, depth), depth)

    def x_piece(which, owner, q):
        return xbuf.at[which, owner, :, features(q)]

    def x_direct(k, q):
        target = (z + k) % lines
        return remote(xin.at[target % 2, :, features(q)], x_piece(m, f, q), x_send.at[0],
                      x_recv.at[m, f, q], frame=2 * target + c)

    def x_across(owner, source, k, q):
        return remote(source, x_piece(m, owner, q), x_send.at[1], x_recv.at[m, owner, q],
                      mp=1 - m)

    def x_core(owner, source, which, k, q):
        return remote(source, x_piece(which, owner, q), x_send.at[2],
                      x_recv.at[which, owner, q], frame=other_core)

    def x_own(q):
        return xin.at[lo, :, features(q)]

    def x_owner(k):
        return f if k == 0 else 2 * line(k - 1) + c

    slices = o_recv.shape[1]
    share = quarter // slices

    def o_rows(which, i):
        return pl.ds(pl.multiple_of(which * quarter + i * share, share), share)

    def o_piece(which, i):
        return wo.at[1 - m, o_rows(which, i), :]

    def o_across(i):
        return remote(
            o_ref.at[o_rows(q0, i), pl.ds(pl.multiple_of((1 - m) * width, width), width)],
            wo.at[m, o_rows(q0, i), :], o_send, o_recv.at[q0, i], mp=1 - m)

    def o_share(i):
        return remote(o_piece(q0, i), o_piece(q0, i), o_send, o_recv.at[q0, i], dp=1 - d)

    def o_core(which, i, slot):
        return remote(o_piece(which, i), o_piece(which, i), o_send,
                      o_recv.at[which, i], frame=other_core)

    def forward_o(i):
        with scope("o_0"):
            arrived(o_piece(q0, i), o_recv.at[q0, i])
        o_share(i).start()
        o_core(q0, i, 2).start()

    def attn_block(which, owner, h):
        group = (owner // 4) * 2 + owner % 2
        clip = (owner // 2) % 2
        return heads.at[which, h, pl.ds(pl.multiple_of(clip * spots, spots), spots),
                        pl.ds(pl.multiple_of(group * HS, HS), HS)]

    def a_direct(h, k):
        target = (f + k) % frames
        return remote(abuf.at[h, target], attn_block(m, f, h), a_send, a_recv.at[h, f],
                      frame=target)

    def a_own(h):
        return pltpu.make_async_copy(abuf.at[h, f], attn_block(m, f, h), a_recv.at[h, f])

    def a_across(h, owner):
        block = attn_block(m, owner, h)
        return remote(block, block, e_send, e_recv.at[h], mp=1 - m)

    def forward_block(h, owner):
        arrived(attn_block(m, owner, h), a_recv.at[h, owner])
        a_across(h, owner).start()

    def forward_attn(h):
        @pl.loop(0, frames)
        def _(k):
            forward_block(h, (f + frames - k) % frames)

    def forward_from_inner(h):
        @pl.loop(frames // 4, frames - frames // 4)
        def _(owner):
            forward_block(h, owner)

    def forward_from_outer(h):
        @pl.loop(0, frames // 2)
        def _(i):
            forward_block(h, jnp.where(i < frames // 4, i, i + frames // 2))

    barrier = pltpu.get_barrier_semaphore()
    clips = xin.shape[0]
    tile = math.gcd(width, 512)

    def tile_of(n):
        return pl.ds(pl.multiple_of(n * tile, tile), tile)

    count = frames * dps
    me = f * dps + d

    def peer(shift):
        other = (me + shift) % count
        return other // dps, other % dps

    for shift in range(1, count):
        frame, dp = peer(shift)
        pl.semaphore_signal(barrier, inc=1, device_id={"frame": frame, "mp": m, "dp": dp},
                            device_id_type=pl.DeviceIdType.MESH)
    pl.semaphore_signal(barrier, inc=1, device_id={"frame": f, "mp": 1 - m, "dp": d},
                        device_id_type=pl.DeviceIdType.MESH)
    loads = [pltpu.make_async_copy(source, target, out_sem.at[i]) for i, (source, target) in enumerate((
        (tokens_ref, xin), (cot_ref, cot), (act_ref, act),
        (o_ref.at[:, pl.ds(pl.multiple_of(m * width, width), width)], wo.at[m])))]
    own_x = pltpu.make_async_copy(xin.at[lo], xbuf.at[m, f], own_sem.at[per_group])
    for h in range(per_group):
        w_own(h).start()
    loads[0].start()
    pl.semaphore_wait(barrier, count)

    last = per_group - 1
    outer = jnp.logical_not(inner)

    def send_tokens(q):
        for k in range(1, lines):
            x_direct(k, q).start()

    def send_weights(h):
        for k in range(4):
            w_direct(h, k).start()

    send_weights(0)

    @pl.loop(0, slices)
    def _(i):
        o_across(i).start()

    loads[0].wait()
    gate[0:1, :] = embed_ref[...].astype(jnp.float32)[None, :]
    same = (lax.broadcasted_iota(jnp.int32, (spots, spots), 0)
            == lax.broadcasted_iota(jnp.int32, (spots, spots), 1))
    for r in range(clips):
        row = jnp.broadcast_to(mask_ref[r].astype(jnp.float32), (spots, spots))
        masked = jnp.sum(jnp.where(same, row, 0.0), axis=1, keepdims=True) == 1.0

        @pl.loop(0, width // tile)
        def _(n):
            cols = tile_of(n)
            xin[r, :, cols] = jnp.where(masked, gate[0:1, cols],
                                        xin[r, :, cols].astype(jnp.float32)).astype(xin.dtype)

    own_x.start()
    send_tokens(0)

    w_partner(0).start()

    @pl.loop(0, pieces)
    def _(q):
        x_core(f, x_own(q), m, 0, q).start()

    @pl.loop(0, 2)
    def _(j):
        forward_w(0, j)

    for copy in loads[1:]:
        copy.start()

    send_tokens(1)

    @pl.when(inner)
    def _():
        @pl.loop(2, 6)
        def _(j):
            forward_w(0, j)

    forward_o(0)
    forward_o(1)

    @pl.when(outer)
    def _():
        forward_w(0, 2)
        forward_w(0, 3)

    forward_o(2)

    def matmul(slot, h, owner, first):
        side = owner // (frames // mps)
        col = pl.multiple_of((owner % (frames // mps)) * depth, depth)
        w = jnp.concatenate([wbuf[h, p, whole_rows(owner), :] for p in range(3)], axis=1)
        step = frames // 2

        @pl.loop(0, 2)
        def _(i):
            x = xbuf[side, pl.ds(i * step, step), :, pl.ds(col, depth)].reshape(step * spots, depth)
            y = jnp.dot(x, w, preferred_element_type=jnp.float32).reshape(step, spots, 3 * HS)

            @pl.when(first)
            def _():
                acc[slot, pl.ds(i * step, step)] = y

            @pl.when(jnp.logical_not(first))
            def _():
                acc[slot, pl.ds(i * step, step)] += y

    def attend_rows(h, i, rows):
        scale = 1.0 / math.sqrt(HS)
        at = pl.ds(pl.multiple_of(i * rows, rows), rows)
        for t in range(frames):
            q = qkv[0, t, at, :].astype(jnp.float32) * scale
            scores = [jnp.sum(q * qkv[1, u, at, :].astype(jnp.float32), axis=-1, keepdims=True)
                      for u in range(t + 1)]
            peak = functools.reduce(jnp.maximum, scores)
            weights = [jnp.exp(s - peak) for s in scores]
            total = functools.reduce(jnp.add, weights)
            accum = functools.reduce(
                jnp.add,
                [w * qkv[2, u, at, :].astype(jnp.float32) for u, w in enumerate(weights)])
            abuf[h, t, at, :] = (accum / total).astype(abuf.dtype)

    def attention(slot, h):
        @pl.loop(0, frames)
        def _(t):
            for p in range(3):
                qkv[p, t] = acc[slot, t, :, p * HS:(p + 1) * HS].astype(qkv.dtype)

        rows = math.gcd(spots, 32)

        @pl.loop(0, spots // rows)
        def _(i):
            with scope("att"):
                attend_rows(h, i, rows)

        a_own(h).start()

        @pl.loop(1, frames)
        def _(k):
            a_direct(h, k).start()

    def ready_w(h, j):
        owner = source_of(j)
        arrived(w_block(h, owner, 1 - d), w_recv.at[h, owner, 1 - d])

    def ready_chip(h):
        w_own(h).wait()
        arrived(wbuf.at[h, :, whole_rows(other_core), :], w_recv.at[h, other_core, 0])

    def ready_w(h, j):
        owner = source_of(j)
        arrived(w_block(h, owner, 1 - d), w_recv.at[h, owner, 1 - d])

    def ready_chip(h):
        w_own(h).wait()
        arrived(wbuf.at[h, :, whole_rows(other_core), :], w_recv.at[h, other_core, 0])

    for h in range(1, per_group):
        w_partner(h).start()

    @pl.loop(0, pieces + 3)
    def _(q):
        @pl.when(q < pieces)
        def _():
            x_across(f, x_own(q), 0, q).start()
            for k in range(1, lines):
                owner = x_owner(k)
                block = x_piece(m, owner, q)
                with scope("x_own"):
                    arrived(block, x_recv.at[m, owner, q])
                x_across(owner, block, k, q).start()
                x_core(owner, block, m, k, q).start()

        @pl.when(q < pieces - 2)
        def _():
            send_tokens(q + 2)

        @pl.when(q == pieces - 2 - jnp.where(outer, 1, 0))
        def _():
            send_weights(1)

        @pl.when(q == 0)
        def _():
            forward_o(3)

            @pl.when(outer)
            def _():
                forward_w(0, 4)
                forward_w(0, 5)

        @pl.when(jnp.logical_and(q >= 2, q < pieces + 2))
        def _():
            for k in range(lines):
                owner = x_owner(k)
                block = x_piece(1 - m, owner, q - 2)
                with scope("x_other"):
                    arrived(block, x_recv.at[1 - m, owner, q - 2])
                x_core(owner, block, 1 - m, k, q - 2).start()

        @pl.when(q == 4)
        def _():
            for h in range(2, per_group):
                send_weights(h)

        @pl.when(jnp.logical_and(q >= 4, q < 6))
        def _():
            forward_w(1, 3 * (q - 4))
            forward_w(1, 3 * (q - 4) + 1)
            forward_w(1, 3 * (q - 4) + 2)

        @pl.when(q == 6)
        def _():
            forward_w(2, 0)
            forward_w(2, 1)

        @pl.when(q == 3)
        def _():
            with scope("w_0"):
                own_x.wait()
                ready_chip(0)
                for j in range(6):
                    ready_w(0, j)

        @pl.when(q >= 3)
        def _():
            with scope("x_core"):
                for k in range(lines):
                    owner = x_owner(k) + 1 - 2 * c
                    for which in range(mps):
                        arrived(x_piece(which, owner, q - 3), x_recv.at[which, owner, q - 3])

            @pl.loop(0, mps)
            def _(side):
                with scope("mm0"):
                    matmul(0, 0, side * pieces + q - 3, jnp.logical_and(side == 0, q == 3))

    @pl.loop(0, slices)
    def _(i):
        with scope("o_1"):
            arrived(o_piece(q1, i), o_recv.at[q1, i])
        o_core(q1, i, 3).start()

    attention(0, 0)

    for copy in loads[1:]:
        copy.wait()
    groups = heads.shape[3] // HS
    codes = act.shape[0]
    kinds = book_ref.shape[0]
    index = jnp.concatenate([jnp.full((1, kinds), idx_ref[r], jnp.int32) for r in range(clips)], axis=0)
    onehot = (index == lax.broadcasted_iota(jnp.int32, (clips, kinds), 1)).astype(jnp.float32)
    codevec = jnp.dot(onehot, book_ref[...], precision=lax.Precision.HIGHEST,
                      preferred_element_type=jnp.float32)
    gate[...] = jnp.dot(codevec, act[...], precision=lax.Precision.HIGHEST,
                        preferred_element_type=jnp.float32)
    marks = jnp.concatenate(
        [jnp.full((1, HS), idx_ref[r], jnp.int32).astype(jnp.float32) for r in range(clips)], axis=0)
    side = width // 2
    for half_of in range(2):
        mine_terms[half_of, :, side:] = marks

    @pl.loop(0, last * frames)
    def _(i):
        h, jj = 1 + i // frames, i % frames

        @pl.when(jnp.logical_and(inner, jnp.logical_and(h < last, jj >= 4)))
        def _():
            forward_w(h + 1, jj - 2)

        @pl.when(jnp.logical_and(outer, jnp.logical_and(h < last, jj >= 6)))
        def _():
            forward_w(h + 1, jj - 4)

        @pl.when(jnp.logical_and(outer, jnp.logical_and(h > 1, jnp.logical_and(jj >= 4, jj < 6))))
        def _():
            forward_w(h, jj)

        @pl.when(jj == 0)
        def _():
            ready_chip(h)

        @pl.when(jj >= 2)
        def _():
            with scope("w_y"):
                ready_w(h, jnp.maximum(jj - 2, 0))

        owner = jnp.where(jj == 0, f, jnp.where(jj == 1, other_core, source_of(jnp.maximum(jj - 2, 0))))
        with scope("mm"):
            matmul(0, h, owner, jj == 0)

        @pl.when(jj == frames - 1)
        def _():
            attention(0, h)

        @pl.when(jnp.logical_and(h == last, jj == 5))
        def _():
            with scope("fa"):
                forward_attn(last - 1)

        @pl.when(jnp.logical_and(h == last, jj == 1))
        def _():
            for before in range(last - 1):
                with scope("fa"):
                    forward_attn(before)

    forward_from_inner(last)

    @pl.loop(0, slices)
    def _(i):
        for which in (d * 2 + 1 - c, (1 - d) * 2 + 1 - c):
            arrived(o_piece(which, i), o_recv.at[which, i])

    def partial(h, side, cols):
        w = jnp.concatenate(
            [wo[side, pl.ds(pl.multiple_of((g * per_group + h) * HS, HS), HS), cols]
             for g in range(groups)], axis=0)
        return jnp.dot(heads[side, h], w, preferred_element_type=jnp.float32)

    def exchanged(h):
        arrived(heads.at[1 - m, h], e_recv.at[h])

    @pl.loop(0, last)
    def _(h):
        with scope("exchanged"):
            exchanged(h)

        @pl.loop(0, width // tile)
        def _(n):
            cols = tile_of(n)
            y = partial(h, 0, cols) + partial(h, 1, cols)

            @pl.when(h == 0)
            def _():
                total[:, cols] = y

            @pl.when(h > 0)
            def _():
                total[:, cols] += y

    forward_from_outer(last)

    @pl.loop(0, width // tile)
    def _(n):
        cols = tile_of(n)
        total[:, cols] += partial(last, m, cols)

    with scope("exchanged"):
        exchanged(last)

    @pl.loop(0, width // tile)
    def _(n):
        cols = tile_of(n)
        y = total[:, cols] + partial(last, 1 - m, cols)
        for r in range(clips):
            mixed = y[r * spots:(r + 1) * spots]
            factor = gate[r:r + 1, cols]
            after[r, :, cols] = (
                xin[r, :, cols].astype(jnp.float32) + factor * mixed).astype(xin.dtype)
            weighed = jnp.sum(cot[r, :, cols].astype(jnp.float32) * mixed, axis=0, keepdims=True)
            piece = math.gcd(tile, side)
            for i in range(tile // piece):
                at = n * (tile // piece) + i
                mine_terms[at // (side // piece), r:r + 1,
                           pl.ds(pl.multiple_of(at % (side // piece) * piece, piece), piece)] = (
                    weighed[:, i * piece:(i + 1) * piece])

    def t_copy(shift):
        frame, dp = peer(shift)
        return remote(mine_terms.at[frame % 2], terms.at[me], t_send.at[0], t_recv.at[me],
                      frame=frame, dp=dp)

    for shift in range(1, count):
        t_copy(shift).start()
    own_terms = pltpu.make_async_copy(mine_terms.at[c], terms.at[me], t_send.at[1])
    own_terms.start()
    result = pltpu.make_async_copy(after, next_ref, out_sem.at[0])
    result.start()

    arrived(wo.at[0], o_send)
    arrived(xbuf.at[0, pl.ds(0, lines - 1)], x_send.at[0])
    arrived(xbuf.at[0, pl.ds(0, lines)], x_send.at[1])
    arrived(xbuf.at[0], x_send.at[2])
    arrived(wbuf.at[:, :, pl.ds(0, 4 * part), :], w_send.at[0])
    arrived(wbuf.at[:, :, pl.ds(0, depth), :], w_send.at[1])
    arrived(wbuf.at[:, :, pl.ds(0, 6 * part), :], w_send.at[2])

    @pl.when(inner)
    def _():
        arrived(wbuf.at[:, :, pl.ds(0, 4 * part), :], w_send.at[3])

    arrived(abuf.at[:, pl.ds(0, frames - 1)], a_send)
    arrived(abuf, e_send)
    kind = lax.broadcasted_iota(jnp.int32, (kinds, HS), 0).astype(jnp.float32)

    def gathered(other):
        total = sums[c]
        for r in range(clips):
            mask = jnp.tile(terms[other, r:r + 1, side:] == kind, (1, side // HS))
            total += jnp.where(mask, terms[other, r:r + 1, :side], 0.0)
        sums[c] = total

    sums[c] = jnp.zeros((kinds, side), jnp.float32)
    own_terms.wait()
    gathered(me)
    with scope("terms"):
        @pl.loop(1, count)
        def _(shift):
            frame, dp = peer(count - shift)
            other = frame * dps + dp
            arrived(terms.at[other], t_recv.at[other])
            gathered(other)

    arrived(terms.at[pl.ds(0, count - 1)], t_send.at[0])
    swap = remote(sums.at[c], sums.at[c], g_send, g_recv, frame=other_core)
    swap.start()
    book_columns = book_ref[...].T

    def gradient(i):
        halves[i] = jnp.dot(book_columns, sums[i], precision=lax.Precision.HIGHEST,
                            preferred_element_type=jnp.float32)
        copy = pltpu.make_async_copy(
            halves.at[i], grad_ref.at[:, pl.ds(pl.multiple_of(i * side, HS), side)],
            out_sem.at[1 + i])
        copy.start()
        return copy

    first = gradient(c)
    arrived(sums.at[1 - c], g_recv)
    second = gradient(1 - c)
    swap.wait_send()
    first.wait()
    second.wait()
    result.wait()


def fused(dps, tokens, mask, embed, w_parts, w_out, cotangent, act_proj, codebook, action_idx, frames):
    clips, spots, width = tokens.shape
    parts, depth, heads_width = w_parts.shape
    groups = frames // clips
    per_group = heads_width // HS // groups
    count = frames * dps
    any_spec = pl.BlockSpec(memory_space=pl.ANY)
    vmem = pl.BlockSpec(memory_space=pltpu.VMEM)
    dma = pltpu.SemaphoreType.DMA
    return pl.pallas_call(
        functools.partial(fused_kernel, dps),
        in_specs=[any_spec, vmem, vmem] + [any_spec] * 4 + [vmem, pl.BlockSpec(memory_space=pltpu.SMEM)],
        out_specs=[any_spec] * 2,
        out_shape=[
            jax.ShapeDtypeStruct(tokens.shape, tokens.dtype),
            jax.ShapeDtypeStruct(act_proj.shape, jnp.float32),
        ],
        scratch_shapes=[
            pltpu.VMEM((2, frames, spots, width), jnp.bfloat16),
            pltpu.VMEM((per_group, parts, depth * frames, HS), jnp.bfloat16),
            pltpu.VMEM((1, frames, spots, parts * HS), jnp.float32),
            pltpu.VMEM((parts, frames, spots, HS), jnp.bfloat16),
            pltpu.VMEM((per_group, frames, spots, HS), jnp.bfloat16),
            pltpu.VMEM((2, per_group, clips * spots, groups * HS), jnp.bfloat16),
            pltpu.VMEM((2, heads_width, width), jnp.bfloat16),
            pltpu.VMEM((clips * spots, width), jnp.float32),
            pltpu.VMEM(tokens.shape, jnp.bfloat16),
            pltpu.VMEM(tokens.shape, jnp.bfloat16),
            pltpu.VMEM(act_proj.shape, jnp.float32),
            pltpu.VMEM((clips, width), jnp.float32),
            pltpu.VMEM((2, clips, width // 2 + HS), jnp.float32),
            pltpu.VMEM((count, clips, width // 2 + HS), jnp.float32),
            pltpu.VMEM((2, codebook.shape[0], width // 2), jnp.float32),
            pltpu.VMEM(tokens.shape, jnp.bfloat16),
            dma((2, frames, frames // 2)), dma((3,)),
            dma((per_group, frames, 2)), dma((4,)),
            dma((4, 4)), dma,
            dma((per_group, frames)), dma,
            dma((per_group,)), dma,
            dma((per_group + 1,)), dma((count,)), dma((2,)), dma((4,)),
            pltpu.VMEM((2, act_proj.shape[0], width // 2), jnp.float32), dma, dma,
        ],
        compiler_params=pltpu.CompilerParams(
            collective_id=2, has_side_effects=True, vmem_limit_bytes=60 << 20),
        name="fused",
    )(tokens, mask, embed, w_parts, w_out, cotangent, act_proj, codebook, action_idx)


def finish_kernel(next_ref, grad_ref, next_out, grad_out, rows, grads, load, store):
    copies = []
    for i, (source, middle, target) in enumerate(
            [(next_ref.at[r], rows.at[r], next_out.at[r]) for r in range(rows.shape[0])]
            + [(grad_ref, grads, grad_out)]):
        copies.append((pltpu.make_async_copy(source, middle, load.at[i]),
                       pltpu.make_async_copy(middle, target, store.at[i])))
    for first, _ in copies:
        first.start()
    for first, second in copies:
        first.wait()
        second.start()
    for _, second in copies:
        second.wait()


def finish(next_state, grad_proj):
    any_spec = pl.BlockSpec(memory_space=pl.ANY)
    count = next_state.shape[0] + 1
    return pl.pallas_call(
        finish_kernel,
        in_specs=[any_spec] * 2,
        out_specs=[any_spec] * 2,
        out_shape=[jax.ShapeDtypeStruct(a.shape, a.dtype) for a in (next_state, grad_proj)],
        scratch_shapes=[pltpu.VMEM(next_state.shape, next_state.dtype),
                        pltpu.VMEM(grad_proj.shape, grad_proj.dtype),
                        pltpu.SemaphoreType.DMA((count,)), pltpu.SemaphoreType.DMA((count,))],
        name="finish",
    )(next_state, grad_proj)


def gather_mp(block, size):
    if size != 2:
        return lax.all_gather(block, "mp", axis=block.ndim - 1, tiled=True)
    other = lax.ppermute(block, "mp", [(0, 1), (1, 0)])
    first = lax.axis_index("mp") == 0
    return jnp.concatenate(
        [jnp.where(first, block, other), jnp.where(first, other, block)], axis=-1
    )


def fits_fused(mps, dps, frames, clips, spots, width, depth, heads_width):
    groups = frames // clips
    return (mps == dps == clips == 2 and frames == groups * clips and groups == 2 * clips
            and heads_width == 3 * groups * HS
            and spots % 32 == 0 and depth % HS == 0
            and width * mps == depth * frames and heads_width % (16 * 16) == 0)


def body(mp_size, dp_size, tokens, token_mask, mask_embed, w_qkv, w_out, action_idx, codebook,
         act_proj, cotangent):
    clips, _, spots, width = tokens.shape
    heads_width = w_qkv.shape[2]
    depth = w_qkv.shape[0]
    xin = jnp.where(token_mask[..., None] == 1, mask_embed, tokens)
    frames = lax.axis_size("frame")
    if fits_fused(mp_size, dp_size, frames, clips, spots, width, depth, heads_width):
        next_state, grad_proj = fused(
            dp_size, tokens.reshape(clips, spots, width), token_mask, mask_embed, w_qkv.transpose(1, 0, 2), w_out,
            cotangent.reshape(clips, spots, width), act_proj, codebook,
            action_idx.reshape(clips), frames)
        next_state, grad_proj = finish(next_state.reshape(2 * clips, spots // 2, width), grad_proj)
        return (next_state.reshape(clips, 1, spots, width), grad_proj)
    else:
        share = depth // dp_size
        mine = lax.dynamic_slice_in_dim(
            w_qkv.reshape(depth, 3 * heads_width), lax.axis_index("dp") * share, share, axis=0
        )
        weights = lax.all_gather(mine, ("frame", "dp"), axis=0, tiled=True)
        if mp_size == 2:
            my_mp = lax.axis_index("mp")
            out_mine = lax.dynamic_slice_in_dim(w_out, my_mp * width, width, axis=1)
            out_other = lax.ppermute(
                lax.dynamic_slice_in_dim(w_out, (1 - my_mp) * width, width, axis=1),
                "mp", [(0, 1), (1, 0)])
        spread = lax.all_to_all(
            xin.reshape(clips, spots, width), "frame", split_axis=1, concat_axis=0, tiled=True
        )
        frames = spread.shape[0] // clips
        local = spread.shape[1]
        features = gather_mp(spread.reshape(frames * clips * local, width), mp_size)
        qkv = jnp.dot(features, weights, preferred_element_type=jnp.float32).astype(jnp.bfloat16)
        attn = attend(qkv.reshape(frames, clips * local, 3 * heads_width), frames, heads_width)
        back = lax.all_to_all(
            attn.reshape(frames * clips, local, heads_width), "frame", split_axis=0, concat_axis=1,
            tiled=True,
        )
        heads = back.reshape(clips * spots, heads_width)
        if mp_size == 2:
            other_heads = lax.ppermute(heads, "mp", [(0, 1), (1, 0)])
            mixed_rows = jnp.dot(heads, out_mine, preferred_element_type=jnp.float32) + jnp.dot(
                other_heads, out_other, preferred_element_type=jnp.float32)
        else:
            out_block = lax.all_to_all(w_out, "mp", split_axis=1, concat_axis=0, tiled=True)
            mixed_rows = jnp.dot(gather_mp(heads, mp_size), out_block,
                                 preferred_element_type=jnp.float32)
    mixed = mixed_rows.reshape(clips, 1, spots, width)
    onehot = (
        action_idx.reshape(clips)[:, None] == jnp.arange(codebook.shape[0])[None, :]
    ).astype(jnp.float32)
    codevec = jnp.dot(onehot, codebook, precision=lax.Precision.HIGHEST)
    gate = jnp.dot(codevec, act_proj, precision=lax.Precision.HIGHEST)
    next_state = (xin.astype(jnp.float32) + gate[:, None, None, :] * mixed).astype(jnp.bfloat16)
    dgate = jnp.sum(cotangent.astype(jnp.float32) * mixed, axis=2).reshape(clips, width)
    codes = codevec.shape[1]
    padded = jnp.pad(codevec, ((0, 0), (0, -codes % 128)))
    terms = spread_terms(jnp.concatenate([dgate, padded], axis=1), frames, dp_size)
    terms = terms.reshape(frames * dp_size * clips, -1)
    grad_proj = jnp.dot(
        terms[:, width : width + codes].T, terms[:, :width], precision=lax.Precision.HIGHEST)
    return (next_state, grad_proj)


def solution(mesh):
    in_specs = (
        P("dp", "frame", None, "mp"),
        P("dp", "frame", None),
        P("mp"),
        P("frame", None, "mp"),
        P("mp", None),
        P("dp", "frame"),
        P(),
        P(None, "mp"),
        P("dp", "frame", None, "mp"),
    )
    out_specs = (P("dp", "frame", None, "mp"), P(None, "mp"))
    return jax.shard_map(
        functools.partial(body, mesh.shape["mp"], mesh.shape["dp"]),
        mesh=mesh, in_specs=in_specs, out_specs=out_specs, check_vma=False,
    )
```
